16 devices in a mesh: data: 4 (over z, y), stage: 4 (over x, core).
Axes of the slice: x: 2, y: 2, z: 2, core: 2. Of those that a mesh axis runs over, the one named last changes fastest.
Arguments:
- master_up: float32 [4, 256, 1024], P('stage')
- master_down: float32 [4, 1024, 256], P('stage')
- mom1_up: float32 [4, 256, 1024], P('stage')
- mom1_down: float32 [4, 1024, 256], P('stage')
- mom2_up: float32 [4, 256, 1024], P('stage')
- mom2_down: float32 [4, 1024, 256], P('stage')
- grad_up: float32 [4, 4, 256, 1024], P('data', 'stage')
- grad_down: float32 [4, 4, 1024, 256], P('data', 'stage')
- stage_acts: bfloat16 [4, 4096, 256], P('stage', 'data')
- loss_grad: bfloat16 [4096, 256], P('data')
- next_batch: bfloat16 [16, 4096, 256], P(None, 'data')
- learn_rate: float32 [], replicated
- max_norm: float32 [], replicated
Outputs:
- output 1: float32 [4, 256, 1024], P('stage')
- output 2: float32 [4, 1024, 256], P('stage')
- output 3: float32 [4, 256, 1024], P('stage')
- output 4: float32 [4, 1024, 256], P('stage')
- output 5: float32 [4, 256, 1024], P('stage')
- output 6: float32 [4, 1024, 256], P('stage')
- output 7: bfloat16 [4, 16, 4096, 256], P('stage', None, 'data')
All inputs are finite; a program needn't handle non-finite values.
Results may differ from the reference program's by a relative error of at most 0.00850932.
Values are sent between devices in bfloat16 or wider.
A program may use at most 1 GiB of HBM per device.

```python
import jax
import jax.numpy as jnp
from jax import lax

STAGES = 4
REPLICAS = 4
D = 256
FF = 1024
TOKENS = 1024
MICROBATCHES = 16
ADAM_STEP = 8

ROWS = REPLICAS * TOKENS
BETA1 = 0.9
BETA2 = 0.95
ADAM_EPS = 1e-8
WEIGHT_DECAY = 0.1
NORM_EPS = 1e-6
SQRT_TWO_PI = 0.7978845608028654
GELU_CUBIC = 0.044715


def tanh_part(pre_act):
    return jnp.tanh(SQRT_TWO_PI * (pre_act + GELU_CUBIC * pre_act * pre_act * pre_act))


def gelu_tanh(pre_act):
    return 0.5 * pre_act * (1.0 + tanh_part(pre_act))


def gelu_pair(pre_act):
    tanh_val = tanh_part(pre_act)
    act_value = 0.5 * pre_act * (1.0 + tanh_val)
    act_slope = 0.5 * (1.0 + tanh_val) + 0.5 * pre_act * (1.0 - tanh_val * tanh_val) * SQRT_TWO_PI * (1.0 + 3.0 * GELU_CUBIC * pre_act * pre_act)
    return act_value, act_slope


def stage_backward(stage_in, master_up, master_down, loss_grad):
    up_bf = master_up.astype(jnp.bfloat16)
    down_bf = master_down.astype(jnp.bfloat16)

    def back_body(grad_in, stage_xs):
        rows_in, up_p, down_p = stage_xs
        pre_act = jnp.dot(rows_in, up_p, preferred_element_type=jnp.float32)
        act_value, act_slope = gelu_pair(pre_act)
        hidden = act_value.astype(jnp.bfloat16)
        d_hidden = jnp.dot(grad_in, down_p.T, preferred_element_type=jnp.float32)
        d_pre = (d_hidden * act_slope).astype(jnp.bfloat16)
        d_rows = (grad_in.astype(jnp.float32) + jnp.dot(d_pre, up_p.T, preferred_element_type=jnp.float32)).astype(jnp.bfloat16)
        dw_up = jnp.dot(rows_in.T, d_pre, preferred_element_type=jnp.float32)
        dw_down = jnp.dot(hidden.T, grad_in, preferred_element_type=jnp.float32)
        return d_rows, (dw_up, dw_down)

    _, (dw_up, dw_down) = lax.scan(back_body, loss_grad, (stage_in, up_bf, down_bf), reverse=True)
    return dw_up, dw_down


def mean_grads(grad_up, grad_down, stage_in, master_up, master_down, loss_grad):
    dw_up, dw_down = stage_backward(stage_in, master_up, master_down, loss_grad)
    gbar_up = (jnp.sum(grad_up, axis=0) + dw_up) / REPLICAS
    gbar_down = (jnp.sum(grad_down, axis=0) + dw_down) / REPLICAS
    return gbar_up, gbar_down


def adamw_update(master, first_mom, second_mom, grad_avg, clip_scale, learn_rate):
    scaled = clip_scale * grad_avg
    new_first = BETA1 * first_mom + (1.0 - BETA1) * scaled
    new_second = BETA2 * second_mom + (1.0 - BETA2) * scaled * scaled
    first_hat = new_first / (1.0 - BETA1 ** ADAM_STEP)
    second_hat = new_second / (1.0 - BETA2 ** ADAM_STEP)
    new_master = master - learn_rate * (first_hat / (jnp.sqrt(second_hat) + ADAM_EPS) + WEIGHT_DECAY * master)
    return new_master, new_first, new_second


def setup_inputs(seed: int = 0) -> dict:
    base_key = jax.random.key(seed)
    key_list = jax.random.split(base_key, 16)
    std_up = D ** -0.5
    std_down = 1.5 * (FF * STAGES) ** -0.5
    master_up = jax.random.normal(key_list[0], (STAGES, D, FF), jnp.float32) * std_up
    master_down = jax.random.normal(key_list[1], (STAGES, FF, D), jnp.float32) * std_down
    stage_acts = jax.random.normal(key_list[2], (STAGES, ROWS, D), jnp.float32).astype(jnp.bfloat16)
    loss_grad = jax.random.normal(key_list[3], (ROWS, D), jnp.float32).astype(jnp.bfloat16)
    next_batch = jax.random.normal(key_list[4], (MICROBATCHES, ROWS, D), jnp.float32).astype(jnp.bfloat16)
    grad_up = jax.random.normal(key_list[5], (REPLICAS, STAGES, D, FF), jnp.float32) * (0.4 * (TOKENS / STAGES) ** 0.5)
    grad_down = jax.random.normal(key_list[6], (REPLICAS, STAGES, FF, D), jnp.float32) * (0.6 * TOKENS ** 0.5)
    gbar_up, gbar_down = mean_grads(grad_up, grad_down, stage_acts, master_up, master_down, loss_grad)
    grad_norm = jnp.sqrt(jnp.sum(gbar_up * gbar_up) + jnp.sum(gbar_down * gbar_down))
    norm_frac = jax.random.uniform(key_list[7], (), jnp.float32, 0.35, 0.65)
    max_norm = norm_frac * grad_norm
    rms_up = norm_frac * jnp.sqrt(jnp.mean(gbar_up * gbar_up))
    rms_down = norm_frac * jnp.sqrt(jnp.mean(gbar_down * gbar_down))
    mom1_up = jax.random.normal(key_list[8], (STAGES, D, FF), jnp.float32) * (0.1 * rms_up)
    mom1_down = jax.random.normal(key_list[9], (STAGES, FF, D), jnp.float32) * (0.1 * rms_down)
    mom2_up = jax.random.uniform(key_list[10], (STAGES, D, FF), jnp.float32, 0.05, 0.15) * (rms_up * rms_up)
    mom2_down = jax.random.uniform(key_list[11], (STAGES, FF, D), jnp.float32, 0.05, 0.15) * (rms_down * rms_down)
    learn_rate = jax.random.uniform(key_list[12], (), jnp.float32, 0.1, 0.3) * std_down
    return dict(master_up=master_up, master_down=master_down, mom1_up=mom1_up, mom1_down=mom1_down, mom2_up=mom2_up, mom2_down=mom2_down, grad_up=grad_up, grad_down=grad_down, stage_acts=stage_acts, loss_grad=loss_grad, next_batch=next_batch, learn_rate=learn_rate, max_norm=max_norm)


def reference(master_up, master_down, mom1_up, mom1_down, mom2_up, mom2_down, grad_up, grad_down, stage_acts, loss_grad, next_batch, learn_rate, max_norm):
    gbar_up, gbar_down = mean_grads(grad_up, grad_down, stage_acts, master_up, master_down, loss_grad)
    grad_norm = jnp.sqrt(jnp.sum(gbar_up * gbar_up) + jnp.sum(gbar_down * gbar_down))
    clip_scale = jnp.minimum(1.0, max_norm / (grad_norm + NORM_EPS))
    new_up, new_mom1_up, new_mom2_up = adamw_update(master_up, mom1_up, mom2_up, gbar_up, clip_scale, learn_rate)
    new_down, new_mom1_down, new_mom2_down = adamw_update(master_down, mom1_down, mom2_down, gbar_down, clip_scale, learn_rate)
    up_bf = new_up.astype(jnp.bfloat16)
    down_bf = new_down.astype(jnp.bfloat16)

    def fwd_body(rows_in, weights):
        up_p, down_p = weights
        pre_act = jnp.dot(rows_in, up_p, preferred_element_type=jnp.float32)
        hidden = gelu_tanh(pre_act).astype(jnp.bfloat16)
        rows_out = (rows_in.astype(jnp.float32) + jnp.dot(hidden, down_p, preferred_element_type=jnp.float32)).astype(jnp.bfloat16)
        return rows_out, rows_out

    flat_batch = next_batch.reshape(MICROBATCHES * ROWS, D)
    _, stage_outs = lax.scan(fwd_body, flat_batch, (up_bf, down_bf))
    stage_outputs = stage_outs.reshape(STAGES, MICROBATCHES, ROWS, D)
    return (new_up, new_down, new_mom1_up, new_mom1_down, new_mom2_up, new_mom2_down, stage_outputs)
```

```python
import functools

import jax
import jax.numpy as jnp
from jax import lax
from jax.experimental import pallas as pl
from jax.experimental.pallas import tpu as pltpu
from jax.sharding import PartitionSpec as P

BETA1 = 0.9
BETA2 = 0.95
ADAM_EPS = 1e-8
WEIGHT_DECAY = 0.1
NORM_EPS = 1e-6
ADAM_STEP = 8
SQRT_TWO_PI = 0.7978845608028654
GELU_CUBIC = 0.044715

N_SENT = 6
MESH = pl.DeviceIdType.MESH
BF16 = jnp.bfloat16
F32 = jnp.float32


def tanh_part(pre_act):
    return jnp.tanh(SQRT_TWO_PI * (pre_act + GELU_CUBIC * pre_act * pre_act * pre_act))


def gelu_pair(pre_act):
    tanh_val = tanh_part(pre_act)
    act_value = 0.5 * pre_act * (1.0 + tanh_val)
    act_slope = 0.5 * (1.0 + tanh_val) + 0.5 * pre_act * (1.0 - tanh_val * tanh_val) * SQRT_TWO_PI * (1.0 + 3.0 * GELU_CUBIC * pre_act * pre_act)
    return act_value, act_slope


def mat_tn(left, right):
    return lax.dot_general(left, right, (((0,), (0,)), ((), ())), preferred_element_type=F32)


def mat_nt(left, right):
    return lax.dot_general(left, right, (((1,), (1,)), ((), ())), preferred_element_type=F32)


def adamw_update(master, first_mom, second_mom, grad_avg, clip_scale, learn_rate):
    scaled = clip_scale * grad_avg
    new_first = BETA1 * first_mom + (1.0 - BETA1) * scaled
    new_second = BETA2 * second_mom + (1.0 - BETA2) * scaled * scaled
    first_hat = new_first / (1.0 - BETA1 ** ADAM_STEP)
    second_hat = new_second / (1.0 - BETA2 ** ADAM_STEP)
    new_master = master - learn_rate * (first_hat / (jnp.sqrt(second_hat) + ADAM_EPS) + WEIGHT_DECAY * master)
    return new_master, new_first, new_second


def gelu_of_half(half):
    t = jnp.tanh(half * (2.0 * SQRT_TWO_PI + (8.0 * SQRT_TWO_PI * GELU_CUBIC) * (half * half)))
    return half + half * t


def stage_rows(src, up_half, down, dst):
    x = src[...]
    half = jnp.dot(x, up_half[...], preferred_element_type=F32)
    hidden = gelu_of_half(half).astype(BF16)
    y = jnp.dot(hidden, down[...], preferred_element_type=F32)
    dst[...] = (x.astype(F32) + y).astype(BF16)


def forward_part(stage, nb_hbm, up_own, down_own, up_aux, down_aux, out_hbm, nbuf, xin, yout, nb_sem, out_sem, send_sem, recv_sem):
    n_micro = nbuf.shape[0]
    n_kept = n_micro - N_SENT

    def load(i):
        return pltpu.make_async_copy(nb_hbm.at[i], nbuf.at[i], nb_sem.at[i])

    def store(i):
        return pltpu.make_async_copy(yout.at[i], out_hbm.at[i], out_sem.at[i])

    def push(src, i, peer):
        return pltpu.make_async_remote_copy(src_ref=src.at[i], dst_ref=xin.at[i], send_sem=send_sem.at[i], recv_sem=recv_sem.at[i], device_id={"stage": peer}, device_id_type=MESH)

    def arrived(i):
        push(yout, i, stage).wait_recv()

    def rotated(j):
        return lax.rem(j + n_kept, n_micro)

    def mixed(k):
        before = lax.div(k * N_SENT, n_micro)
        is_sent = lax.div((k + 1) * N_SENT, n_micro) - before
        return is_sent, is_sent * (n_kept + before) + (1 - is_sent) * (k - before)

    def finish_stores():
        def body(i, _):
            store(i).wait()
            return 0
        lax.fori_loop(0, n_micro, body, 0)

    def finish_sends(first, count):
        def body(i, _):
            push(yout, first + i, stage).wait_send()
            return 0
        lax.fori_loop(0, count, body, 0)

    @pl.when(stage == 0)
    def _():
        def start(j, _):
            load(rotated(j)).start()
            return 0
        lax.fori_loop(0, n_micro, start, 0)

        def body(j, _):
            i = rotated(j)
            load(i).wait()
            stage_rows(nbuf.at[i], up_own, down_own, yout.at[i])
            push(yout, i, 1).start()
            store(i).start()
            return 0
        lax.fori_loop(0, n_micro, body, 0)
        finish_sends(0, n_micro)
        finish_stores()

    @pl.when(stage == 1)
    def _():
        def body(j, _):
            i = rotated(j)
            arrived(i)
            stage_rows(xin.at[i], up_own, down_own, yout.at[i])

            @pl.when(j < N_SENT)
            def _():
                push(yout, i, 2).start()
            store(i).start()
            return 0
        lax.fori_loop(0, n_micro, body, 0)
        finish_sends(n_kept, N_SENT)
        finish_stores()

    @pl.when(stage == 2)
    def _():
        def body(k, _):
            is_sent, i = mixed(k)
            arrived(i)

            @pl.when(is_sent == 0)
            def _():
                stage_rows(xin.at[i], up_aux, down_aux, xin.at[i])
            stage_rows(xin.at[i], up_own, down_own, yout.at[i])
            push(yout, i, 3).start()
            store(i).start()
            return 0
        lax.fori_loop(0, n_micro, body, 0)
        finish_sends(0, n_micro)
        finish_stores()

    @pl.when(stage == 3)
    def _():
        def start(j, _):
            load(j).start()
            return 0
        lax.fori_loop(0, n_kept, start, 0)

        def first(j, _):
            load(j).wait()
            stage_rows(nbuf.at[j], up_aux, down_aux, nbuf.at[j])
            push(nbuf, j, 2).start()
            return 0
        lax.fori_loop(0, n_kept, first, 0)

        def body(k, _):
            _, i = mixed(k)
            arrived(i)
            stage_rows(xin.at[i], up_own, down_own, yout.at[i])
            store(i).start()
            return 0
        lax.fori_loop(0, n_micro, body, 0)
        finish_sends(0, n_kept)
        finish_stores()


def forward_kernel(nb_hbm, up_own, down_own, up_aux, down_aux, out_hbm, nbuf, xin, yout, nb_sem, out_sem, send_sem, recv_sem):
    stage = lax.axis_index("stage")
    barrier = pltpu.get_barrier_semaphore()

    @pl.when(stage > 0)
    def _():
        pl.semaphore_signal(barrier, inc=1, device_id={"stage": stage - 1}, device_id_type=MESH)

    @pl.when(stage < 3)
    def _():
        pl.semaphore_signal(barrier, inc=1, device_id={"stage": stage + 1}, device_id_type=MESH)

    pl.semaphore_wait(barrier, jnp.where((stage == 0) | (stage == 3), 1, 2))
    forward_part(stage, nb_hbm, up_own, down_own, up_aux, down_aux, out_hbm, nbuf, xin, yout, nb_sem, out_sem, send_sem, recv_sem)


def forward(next_batch, up_own, down_own, up_aux, down_aux):
    n_micro = next_batch.shape[0]
    vmem = pl.BlockSpec(memory_space=pltpu.VMEM)
    hbm = pl.BlockSpec(memory_space=pl.ANY)
    return pl.pallas_call(
        forward_kernel,
        name="forward_step",
        out_shape=jax.ShapeDtypeStruct(next_batch.shape, BF16),
        in_specs=[hbm, vmem, vmem, vmem, vmem],
        out_specs=hbm,
        scratch_shapes=[
            pltpu.VMEM(next_batch.shape, BF16),
            pltpu.VMEM(next_batch.shape, BF16),
            pltpu.VMEM(next_batch.shape, BF16),
            pltpu.SemaphoreType.DMA((n_micro,)),
            pltpu.SemaphoreType.DMA((n_micro,)),
            pltpu.SemaphoreType.DMA((n_micro,)),
            pltpu.SemaphoreType.DMA((n_micro,)),
        ],
        compiler_params=pltpu.CompilerParams(collective_id=1, has_side_effects=True, vmem_limit_bytes=60 * 1024 * 1024),
    )(next_batch, up_own, down_own, up_aux, down_aux)


def solution(mesh):
    n_stages = mesh.shape['stage']
    n_reps = mesh.shape['data']
    last_stage = n_stages - 1
    down_pairs = [(source, source - 1) for source in range(1, n_stages)]

    def local_step(master_up, master_down, mom1_up, mom1_down, mom2_up, mom2_down, grad_up, grad_down, stage_acts, loss_grad, next_batch, learn_rate, max_norm):
        stage_idx = lax.axis_index('stage')
        stage_in = stage_acts[0]
        up_bf = master_up[0].astype(BF16)
        down_bf = master_down[0].astype(BF16)

        pre_act = jnp.dot(stage_in, up_bf, preferred_element_type=F32)
        act_value, act_slope = gelu_pair(pre_act)
        hidden = act_value.astype(BF16)

        grad_in = loss_grad
        for step_idx in range(n_stages):
            d_pre = (mat_nt(grad_in, down_bf) * act_slope).astype(BF16)
            if step_idx < last_stage:
                d_rows = (grad_in.astype(F32) + mat_nt(d_pre, up_bf)).astype(BF16)
                received = lax.ppermute(d_rows, 'stage', down_pairs)
                grad_in = jnp.where(stage_idx == last_stage - 1 - step_idx, received, grad_in)

        gbar_up = lax.psum(grad_up[0, 0] + mat_tn(stage_in, d_pre), 'data') / n_reps
        gbar_down = lax.psum(grad_down[0, 0] + mat_tn(hidden, grad_in), 'data') / n_reps
        local_sq = jnp.sum(gbar_up * gbar_up) + jnp.sum(gbar_down * gbar_down)
        grad_norm = jnp.sqrt(lax.psum(local_sq, 'stage'))
        clip_scale = jnp.minimum(1.0, max_norm / (grad_norm + NORM_EPS))
        new_up, new_m1_up, new_m2_up = adamw_update(master_up[0], mom1_up[0], mom2_up[0], gbar_up, clip_scale, learn_rate)
        new_down, new_m1_down, new_m2_down = adamw_update(master_down[0], mom1_down[0], mom2_down[0], gbar_down, clip_scale, learn_rate)
        up_half = new_up.astype(BF16) * jnp.asarray(0.5, BF16)
        down_new = new_down.astype(BF16)
        up_aux = lax.ppermute(up_half, 'stage', [(0, 3), (1, 2)])
        down_aux = lax.ppermute(down_new, 'stage', [(0, 3), (1, 2)])
        stage_outs = forward(next_batch, up_half, down_new, up_aux, down_aux)
        return (new_up[None], new_down[None], new_m1_up[None], new_m1_down[None], new_m2_up[None], new_m2_down[None], stage_outs[None])

    w_spec = P('stage', None, None)
    g_spec = P('data', 'stage', None, None)
    in_specs = (w_spec, w_spec, w_spec, w_spec, w_spec, w_spec, g_spec, g_spec, P('stage', 'data', None), P('data', None), P(None, 'data', None), P(), P())
    out_specs = (w_spec, w_spec, w_spec, w_spec, w_spec, w_spec, P('stage', None, 'data', None))
    return jax.shard_map(local_step, mesh=mesh, in_specs=in_specs, out_specs=out_specs, check_vma=False)
```

```python
import jax
import jax.numpy as jnp
from jax import lax
from jax.experimental import pallas as pl
from jax.experimental.pallas import tpu as pltpu
from jax.sharding import PartitionSpec as P

BETA1 = 0.9
BETA2 = 0.95
ADAM_EPS = 1e-8
WEIGHT_DECAY = 0.1
NORM_EPS = 1e-6
ADAM_STEP = 8
SQRT_TWO_PI = 0.7978845608028654
GELU_CUBIC = 0.044715

N_SENT = 6
N_CHUNK = 4
MESH = pl.DeviceIdType.MESH
BF16 = jnp.bfloat16
F32 = jnp.float32


def mat_tn(left, right):
    return lax.dot_general(left, right, (((0,), (0,)), ((), ())), preferred_element_type=F32)


def mat_nt(left, right):
    return lax.dot_general(left, right, (((1,), (1,)), ((), ())), preferred_element_type=F32)


def adamw_update(master, first_mom, second_mom, grad_avg, clip_scale, learn_rate):
    scaled = clip_scale * grad_avg
    new_first = BETA1 * first_mom + (1.0 - BETA1) * scaled
    new_second = BETA2 * second_mom + (1.0 - BETA2) * scaled * scaled
    first_hat = new_first / (1.0 - BETA1 ** ADAM_STEP)
    second_hat = new_second / (1.0 - BETA2 ** ADAM_STEP)
    new_master = master - learn_rate * (first_hat / (jnp.sqrt(second_hat) + ADAM_EPS) + WEIGHT_DECAY * master)
    return new_master, new_first, new_second


def gelu_of_half(half):
    t = jnp.tanh(half * (2.0 * SQRT_TWO_PI + (8.0 * SQRT_TWO_PI * GELU_CUBIC) * (half * half)))
    return half + half * t


def stage_rows(src, up_half, down, dst):
    x = src[...]
    half = jnp.dot(x, up_half[...], preferred_element_type=F32)
    hidden = gelu_of_half(half).astype(BF16)
    y = jnp.dot(hidden, down[...], preferred_element_type=F32)
    dst[...] = (x.astype(F32) + y).astype(BF16)


def forward_part(stage, own_ready, aux_ready, relay_mean, nb_hbm, up_own, down_own, up_aux, down_aux, out_hbm, nbuf, xin, yout, nb_sem, out_sem, send_sem, recv_sem):
    n_micro = nbuf.shape[0]
    n_kept = n_micro - N_SENT

    def load(i):
        return pltpu.make_async_copy(nb_hbm.at[i], nbuf.at[i], nb_sem.at[i])

    def store(i):
        return pltpu.make_async_copy(yout.at[i], out_hbm.at[i], out_sem.at[i])

    def push(src, i, peer):
        return pltpu.make_async_remote_copy(src_ref=src.at[i], dst_ref=xin.at[i], send_sem=send_sem.at[i], recv_sem=recv_sem.at[i], device_id={"stage": peer}, device_id_type=MESH)

    def arrived(i):
        push(yout, i, stage).wait_recv()

    def rotated(j):
        return lax.rem(j + n_kept, n_micro)

    def mixed(k):
        before = lax.div(k * N_SENT, n_micro)
        is_sent = lax.div((k + 1) * N_SENT, n_micro) - before
        return is_sent, is_sent * (n_kept + before) + (1 - is_sent) * (k - before)

    def finish_stores():
        def body(i, _):
            store(i).wait()
            return 0
        lax.fori_loop(0, n_micro, body, 0)

    def finish_sends(first, count):
        def body(i, _):
            push(yout, first + i, stage).wait_send()
            return 0
        lax.fori_loop(0, count, body, 0)

    @pl.when(stage == 0)
    def _():
        own_ready()

        def body(j, _):
            i = rotated(j)
            load(i).wait()
            stage_rows(nbuf.at[i], up_own, down_own, yout.at[i])
            push(yout, i, 1).start()
            store(i).start()
            relay_mean(j == 7)
            return 0
        lax.fori_loop(0, n_micro, body, 0)
        finish_sends(0, n_micro)
        finish_stores()

    @pl.when(stage == 1)
    def _():
        own_ready()

        def body(j, _):
            i = rotated(j)
            arrived(i)
            stage_rows(xin.at[i], up_own, down_own, yout.at[i])

            @pl.when(j < N_SENT)
            def _():
                push(yout, i, 2).start()
            store(i).start()
            relay_mean(j == 7)
            return 0
        lax.fori_loop(0, n_micro, body, 0)
        finish_sends(n_kept, N_SENT)
        finish_stores()

    @pl.when(stage == 2)
    def _():
        aux_ready()
        own_ready()

        def body(k, _):
            is_sent, i = mixed(k)
            arrived(i)

            @pl.when(is_sent == 0)
            def _():
                stage_rows(xin.at[i], up_aux, down_aux, xin.at[i])
            stage_rows(xin.at[i], up_own, down_own, yout.at[i])
            push(yout, i, 3).start()
            store(i).start()
            relay_mean(k == 6)
            return 0
        lax.fori_loop(0, n_micro, body, 0)
        finish_sends(0, n_micro)
        finish_stores()

    @pl.when(stage == 3)
    def _():
        aux_ready()

        def first(j, _):
            load(j).wait()
            stage_rows(nbuf.at[j], up_aux, down_aux, nbuf.at[j])
            push(nbuf, j, 2).start()
            return 0
        lax.fori_loop(0, n_kept, first, 0)
        own_ready()

        def body(k, _):
            _, i = mixed(k)
            arrived(i)
            stage_rows(xin.at[i], up_own, down_own, yout.at[i])
            store(i).start()
            relay_mean(k == 1)
            return 0
        lax.fori_loop(0, n_micro, body, 0)
        finish_sends(0, n_kept)
        finish_stores()


def start_loads(stage, nb_hbm, nbuf, nb_sem):
    n_micro = nbuf.shape[0]
    n_kept = n_micro - N_SENT

    def body(j, _):
        i = lax.rem(j + n_kept, n_micro)
        pltpu.make_async_copy(nb_hbm.at[i], nbuf.at[i], nb_sem.at[i]).start()
        return 0

    @pl.when(stage == 0)
    def _():
        lax.fori_loop(0, n_micro, body, 0)

    @pl.when(stage == 3)
    def _():
        lax.fori_loop(N_SENT, n_micro, body, 0)


def step_kernel(up_hbm, down_hbm, m1_up_hbm, m1_down_hbm, m2_up_hbm, m2_down_hbm, gu_hbm, gv_hbm, acts_hbm, loss_hbm, nb_hbm, rate_ref, norm_ref,
                out_hbm, mean_up_hbm, mean_down_hbm, clip_out,
                up32, down32, gu, gv, mean_up, mean_down, acts, gbuf, dxbuf, hid, slope, dpre, up_bf, down_bf,
                ru1, rv1, ru2, rv2, mq_up, mq_down, up_own, down_own, up_aux, down_aux, sq_all, nbuf, xin, yout,
                in_sem, g_send, g_recv, rs_send, rs_recv, sq_send, sq_recv, ag_send, ag_recv, aux_send, aux_recv,
                nb_sem, out_sem, send_sem, recv_sem):
    stage = lax.axis_index("stage")
    data = lax.axis_index("data")
    z = lax.div(data, 2)
    y = lax.rem(data, 2)
    me = data * 4 + stage
    z_peer = 2 * (1 - z) + y
    y_peer = 2 * z + (1 - y)
    n_tok = acts.shape[0]
    chunk = n_tok // N_CHUNK

    def up_rows(zz, yy, first=0, count=64):
        return pl.ds(pl.multiple_of(128 * yy + 64 * zz + first, 32), count)

    def down_rows(zz, yy, first=0, count=256):
        return pl.ds(pl.multiple_of(512 * zz + 256 * yy + first, 128), count)

    own_up, own_down = up_rows(z, y), down_rows(z, y)
    loads = [
        pltpu.make_async_copy(acts_hbm, acts, in_sem.at[0]),
        pltpu.make_async_copy(up_hbm, up32, in_sem.at[1]),
        pltpu.make_async_copy(down_hbm, down32, in_sem.at[2]),
        pltpu.make_async_copy(gv_hbm, gv, in_sem.at[3]),
        pltpu.make_async_copy(gu_hbm, gu, in_sem.at[4]),
        pltpu.make_async_copy(m1_up_hbm.at[own_up], mq_up.at[0], in_sem.at[5]),
        pltpu.make_async_copy(m2_up_hbm.at[own_up], mq_up.at[1], in_sem.at[6]),
        pltpu.make_async_copy(m1_down_hbm.at[own_down], mq_down.at[0], in_sem.at[7]),
        pltpu.make_async_copy(m2_down_hbm.at[own_down], mq_down.at[1], in_sem.at[8]),
    ]
    load_loss = pltpu.make_async_copy(loss_hbm, gbuf, in_sem.at[9])
    loads[0].start()
    loads[1].start()

    @pl.when(stage == 3)
    def _():
        load_loss.start()
    for copy in loads[2:]:
        copy.start()
    start_loads(stage, nb_hbm, nbuf, nb_sem)

    barrier = pltpu.get_barrier_semaphore()

    def greet(d, _):
        other = lax.rem(me + d, 16)
        pl.semaphore_signal(barrier, inc=1, device_id={"data": lax.div(other, 4), "stage": lax.rem(other, 4)}, device_id_type=MESH)
        return 0
    lax.fori_loop(1, 16, greet, 0)

    loads[0].wait()
    loads[1].wait()
    up_bf[...] = up32[...].astype(BF16)
    loads[2].wait()
    down_bf[...] = down32[...].astype(BF16)
    pl.semaphore_wait(barrier, 15)

    @pl.when(stage == 3)
    def _():
        load_loss.wait()

    def chunk_rows(k):
        return pl.ds(pl.multiple_of(k * chunk, chunk), chunk)

    def pass_down(k):
        rows = chunk_rows(k)
        return pltpu.make_async_remote_copy(src_ref=dxbuf.at[rows], dst_ref=gbuf.at[rows], send_sem=g_send.at[k], recv_sem=g_recv.at[k],
                                            device_id={"stage": jnp.maximum(stage - 1, 0)}, device_id_type=MESH)

    def prepare(k):
        rows = chunk_rows(k)
        pre = jnp.dot(acts[rows, :], up_bf[...], preferred_element_type=F32)
        sq = pre * pre
        half_t = 0.5 * jnp.tanh(pre * (SQRT_TWO_PI + (SQRT_TWO_PI * GELU_CUBIC) * sq))
        prob = 0.5 + half_t
        rest = 0.5 - half_t
        hid[rows, :] = (pre * prob).astype(BF16)
        slope[rows, :] = prob + (prob * rest) * pre * (2.0 * SQRT_TWO_PI + (6.0 * SQRT_TWO_PI * GELU_CUBIC) * sq)

    def backward(k):
        rows = chunk_rows(k)

        @pl.when(stage < 3)
        def _():
            pass_down(k).wait_recv()
        grad = gbuf[rows, :]
        d_pre = (mat_nt(grad, down_bf[...]) * slope[rows, :]).astype(BF16)
        dpre[rows, :] = d_pre

        @pl.when(stage > 0)
        def _():
            dxbuf[rows, :] = (grad.astype(F32) + mat_nt(d_pre, up_bf[...])).astype(BF16)
            pass_down(k).start()

    def tick(t, _):
        upper = jnp.where(stage >= 2, 1, 0)
        is_prep = upper * (1 - lax.rem(t, 2)) + (1 - upper) * (1 - lax.div(t, N_CHUNK))
        k = upper * lax.div(t, 2) + (1 - upper) * lax.rem(t, N_CHUNK)

        @pl.when(is_prep == 1)
        def _():
            prepare(k)

        @pl.when(is_prep == 0)
        def _():
            backward(k)
        return 0
    lax.fori_loop(0, 2 * N_CHUNK, tick, 0)

    def rs_copy(src, dst, sem, peer):
        return pltpu.make_async_remote_copy(src_ref=src, dst_ref=dst, send_sem=rs_send.at[sem], recv_sem=rs_recv.at[sem], device_id={"data": peer}, device_id_type=MESH)

    def v_first(sub, c):
        yy = (1 - y) if sub == 0 else y
        return rs_copy(gv.at[down_rows(1 - z, yy, 128 * c, 128)], rv1.at[sub, pl.ds(128 * c, 128)], 2 * sub + c, z_peer)

    def u_first(sub, c):
        zz = (1 - z) if sub == 0 else z
        return rs_copy(gu.at[up_rows(zz, 1 - y, 32 * c, 32)], ru1.at[sub, pl.ds(32 * c, 32)], 4 + 2 * sub + c, y_peer)

    def v_second(c):
        return rs_copy(gv.at[down_rows(z, 1 - y, 128 * c, 128)], rv2.at[pl.ds(128 * c, 128)], 8 + c, y_peer)

    def u_second(c):
        return rs_copy(gu.at[up_rows(1 - z, y, 32 * c, 32)], ru2.at[pl.ds(32 * c, 32)], 10 + c, z_peer)

    loads[3].wait()
    gv[...] += mat_tn(hid[...], gbuf[...])
    for sub in range(2):
        for c in range(2):
            v_first(sub, c).start()
    loads[4].wait()
    gu[...] += mat_tn(acts[...], dpre[...])
    for sub in range(2):
        for c in range(2):
            u_first(sub, c).start()
    for c in range(2):
        v_first(0, c).wait_recv()
        rows = down_rows(z, 1 - y, 128 * c, 128)
        gv[rows, :] += rv1[0, 128 * c:128 * (c + 1), :]
        v_second(c).start()
        u_first(0, c).wait_recv()
        rows = up_rows(1 - z, y, 32 * c, 32)
        gu[rows, :] += ru1[0, 32 * c:32 * (c + 1), :]
        u_second(c).start()
    acc = jnp.zeros((8, 128), F32)

    def fold(tile, acc):
        sq = tile * tile
        sq = jnp.sum(sq.reshape(sq.shape[0] // 8, 8, sq.shape[1]), axis=0)
        for i in range(0, sq.shape[1], 128):
            acc = acc + sq[:, i:i + 128]
        return acc

    for c in range(2):
        v_first(1, c).wait_recv()
        v_second(c).wait_recv()
        rows = down_rows(z, y, 128 * c, 128)
        mean = (gv[rows, :] + rv1[1, 128 * c:128 * (c + 1), :] + rv2[128 * c:128 * (c + 1), :]) * 0.25
        mean_down[rows, :] = mean
        acc = fold(mean, acc)
        u_first(1, c).wait_recv()
        u_second(c).wait_recv()
        rows = up_rows(z, y, 32 * c, 32)
        mean = (gu[rows, :] + ru1[1, 32 * c:32 * (c + 1), :] + ru2[32 * c:32 * (c + 1), :]) * 0.25
        mean_up[rows, :] = mean
        acc = fold(mean, acc)

    def sq_copy(other, slot):
        return pltpu.make_async_remote_copy(src_ref=sq_all.at[slot], dst_ref=sq_all.at[slot], send_sem=sq_send.at[other], recv_sem=sq_recv.at[slot],
                                            device_id={"data": lax.div(other, 4), "stage": lax.rem(other, 4)}, device_id_type=MESH)

    sq_all[me] = acc

    def tell(d, _):
        sq_copy(lax.rem(me + d, 16), me).start()
        return 0
    lax.fori_loop(1, 16, tell, 0)
    for copy in loads[5:]:
        copy.wait()

    def hear(d, _):
        other = lax.rem(me + d, 16)
        sq_copy(other, other).wait_recv()
        return 0
    lax.fori_loop(1, 16, hear, 0)
    total = sq_all[0]
    for i in range(1, 16):
        total = total + sq_all[i]
    total = jnp.sum(jnp.sum(total, axis=0, keepdims=True), axis=1, keepdims=True)
    clip = jnp.minimum(1.0, norm_ref[0] / (jnp.sqrt(total) + NORM_EPS))
    clip_out[...] = jnp.broadcast_to(clip, clip_out.shape)

    rate = rate_ref[0]
    new_up, _, _ = adamw_update(up32[own_up, :], mq_up[0], mq_up[1], mean_up[own_up, :], clip, rate)
    up_own[own_up, :] = new_up.astype(BF16) * jnp.asarray(0.5, BF16)
    new_down, _, _ = adamw_update(down32[own_down, :], mq_down[0], mq_down[1], mean_down[own_down, :], clip, rate)
    down_own[own_down, :] = new_down.astype(BF16)

    def gather(which, up, down):
        def copy(ref, rows, sem, peer):
            return pltpu.make_async_remote_copy(src_ref=ref.at[rows], dst_ref=ref.at[rows], send_sem=ag_send.at[which * 6 + sem], recv_sem=ag_recv.at[which * 6 + sem],
                                                device_id={"data": peer}, device_id_type=MESH)

        sends = [copy(up, own_up, 0, z_peer), copy(down, own_down, 3, y_peer), copy(up, own_up, 1, y_peer), copy(down, own_down, 4, z_peer)]
        relays = [copy(up, up_rows(1 - z, y), 2, y_peer), copy(down, down_rows(z, 1 - y), 5, z_peer)]
        arrive_first = [copy(up, up_rows(1 - z, y), 0, z_peer), copy(down, down_rows(z, 1 - y), 3, y_peer)]
        arrive_rest = [copy(up, up_rows(z, 1 - y), 1, y_peer), copy(down, down_rows(1 - z, y), 4, z_peer),
                       copy(up, up_rows(1 - z, 1 - y), 2, y_peer), copy(down, down_rows(1 - z, 1 - y), 5, z_peer)]

        def begin():
            for c in sends:
                c.start()

        def relay():
            for a, c in zip(arrive_first, relays):
                a.wait_recv()
                c.start()

        def finish():
            for c in arrive_rest:
                c.wait_recv()

        def drain():
            for c in sends + relays:
                c.wait_send()
        return begin, relay, finish, drain

    own_begin, own_relay, own_finish, own_drain = gather(0, up_own, down_own)
    aux_begin, aux_relay, aux_finish, aux_drain = gather(1, up_aux, down_aux)
    mean_begin, mean_relay, mean_finish, mean_drain = gather(2, mean_up, mean_down)

    def feed():
        peer = 3 - stage
        return [pltpu.make_async_remote_copy(src_ref=own.at[rows], dst_ref=aux.at[rows], send_sem=aux_send.at[i], recv_sem=aux_recv.at[i], device_id={"stage": peer}, device_id_type=MESH)
                for i, (own, aux, rows) in enumerate([(up_own, up_aux, own_up), (down_own, down_aux, own_down)])]

    @pl.when(stage < 2)
    def _():
        for c in feed():
            c.start()
    own_begin()
    own_relay()

    @pl.when(stage >= 2)
    def _():
        for c in feed():
            c.wait_recv()
        aux_begin()
        aux_relay()
    mean_begin()

    def relay_mean(now):
        @pl.when(now)
        def _():
            mean_relay()

    forward_part(stage, own_finish, aux_finish, relay_mean, nb_hbm, up_own, down_own, up_aux, down_aux, out_hbm, nbuf, xin, yout, nb_sem, out_sem, send_sem, recv_sem)

    mean_finish()
    store_up = pltpu.make_async_copy(mean_up, mean_up_hbm, in_sem.at[0])
    store_down = pltpu.make_async_copy(mean_down, mean_down_hbm, in_sem.at[1])
    store_up.start()
    store_down.start()

    @pl.when(stage > 0)
    def _():
        for k in range(N_CHUNK):
            pass_down(k).wait_send()
    for c in range(2):
        for sub in range(2):
            v_first(sub, c).wait_send()
            u_first(sub, c).wait_send()
        v_second(c).wait_send()
        u_second(c).wait_send()

    def told(d, _):
        sq_copy(lax.rem(me + d, 16), me).wait_send()
        return 0
    lax.fori_loop(1, 16, told, 0)
    own_drain()
    mean_drain()

    @pl.when(stage < 2)
    def _():
        for c in feed():
            c.wait_send()

    @pl.when(stage >= 2)
    def _():
        aux_drain()
    store_up.wait()
    store_down.wait()


def fused_step(master_up, master_down, m1_up, m1_down, m2_up, m2_down, grad_up, grad_down, acts, loss_grad, next_batch, learn_rate, max_norm):
    n_micro = next_batch.shape[0]
    n_tok, width = acts.shape
    hidden = master_up.shape[1]
    hbm = pl.BlockSpec(memory_space=pl.ANY)
    smem = pl.BlockSpec(memory_space=pltpu.SMEM)
    vmem = pltpu.VMEM
    dma = pltpu.SemaphoreType.DMA
    return pl.pallas_call(
        step_kernel,
        name="pipeline_step",
        out_shape=[jax.ShapeDtypeStruct(next_batch.shape, BF16), jax.ShapeDtypeStruct((width, hidden), F32), jax.ShapeDtypeStruct((hidden, width), F32), jax.ShapeDtypeStruct((8, 128), F32)],
        in_specs=[hbm] * 11 + [smem] * 2,
        out_specs=[hbm, hbm, hbm, pl.BlockSpec(memory_space=pltpu.VMEM)],
        scratch_shapes=[
            vmem((width, hidden), F32), vmem((hidden, width), F32),
            vmem((width, hidden), F32), vmem((hidden, width), F32),
            vmem((width, hidden), F32), vmem((hidden, width), F32),
            vmem((n_tok, width), BF16), vmem((n_tok, width), BF16), vmem((n_tok, width), BF16),
            vmem((n_tok, hidden), BF16), vmem((n_tok, hidden), F32), vmem((n_tok, hidden), BF16),
            vmem((width, hidden), BF16), vmem((hidden, width), BF16),
            vmem((2, width // 4, hidden), F32), vmem((2, hidden // 4, width), F32),
            vmem((width // 4, hidden), F32), vmem((hidden // 4, width), F32),
            vmem((2, width // 4, hidden), F32), vmem((2, hidden // 4, width), F32),
            vmem((width, hidden), BF16), vmem((hidden, width), BF16),
            vmem((width, hidden), BF16), vmem((hidden, width), BF16),
            vmem((16, 8, 128), F32),
            vmem(next_batch.shape, BF16), vmem(next_batch.shape, BF16), vmem(next_batch.shape, BF16),
            dma((10,)), dma((N_CHUNK,)), dma((N_CHUNK,)), dma((12,)), dma((12,)), dma((16,)), dma((16,)), dma((18,)), dma((18,)), dma((2,)), dma((2,)),
            dma((n_micro,)), dma((n_micro,)), dma((n_micro,)), dma((n_micro,)),
        ],
        compiler_params=pltpu.CompilerParams(collective_id=1, has_side_effects=True, vmem_limit_bytes=63 * 1024 * 1024),
    )(master_up, master_down, m1_up, m1_down, m2_up, m2_down, grad_up, grad_down, acts, loss_grad, next_batch, learn_rate, max_norm)


def solution(mesh):
    def local_step(master_up, master_down, mom1_up, mom1_down, mom2_up, mom2_down, grad_up, grad_down, stage_acts, loss_grad, next_batch, learn_rate, max_norm):
        stage_outs, gbar_up, gbar_down, clip = fused_step(
            master_up[0], master_down[0], mom1_up[0], mom1_down[0], mom2_up[0], mom2_down[0], grad_up[0, 0], grad_down[0, 0],
            stage_acts[0], loss_grad, next_batch, learn_rate.reshape(1), max_norm.reshape(1))
        clip_scale = clip[0, 0]
        new_up, new_m1_up, new_m2_up = adamw_update(master_up[0], mom1_up[0], mom2_up[0], gbar_up, clip_scale, learn_rate)
        new_down, new_m1_down, new_m2_down = adamw_update(master_down[0], mom1_down[0], mom2_down[0], gbar_down, clip_scale, learn_rate)
        return (new_up[None], new_down[None], new_m1_up[None], new_m1_down[None], new_m2_up[None], new_m2_down[None], stage_outs[None])

    w_spec = P('stage', None, None)
    g_spec = P('data', 'stage', None, None)
    in_specs = (w_spec, w_spec, w_spec, w_spec, w_spec, w_spec, g_spec, g_spec, P('stage', 'data', None), P('data', None), P(None, 'data', None), P(), P())
    out_specs = (w_spec, w_spec, w_spec, w_spec, w_spec, w_spec, P('stage', None, 'data', None))
    return jax.shard_map(local_step, mesh=mesh, in_specs=in_specs, out_specs=out_specs, check_vma=False)
```

```python
import jax
import jax.numpy as jnp
from jax import lax
from jax.experimental import pallas as pl
from jax.experimental.pallas import tpu as pltpu
from jax.sharding import PartitionSpec as P

BETA1 = 0.9
BETA2 = 0.95
ADAM_EPS = 1e-8
WEIGHT_DECAY = 0.1
NORM_EPS = 1e-6
ADAM_STEP = 8
SQRT_TWO_PI = 0.7978845608028654
GELU_CUBIC = 0.044715

N_SENT = 6
N_CHUNK = 4
N_LATE = 5
N_TWICE = 2
MESH = pl.DeviceIdType.MESH
BF16 = jnp.bfloat16
F32 = jnp.float32


def mat_tn(left, right):
    return lax.dot_general(left, right, (((0,), (0,)), ((), ())), preferred_element_type=F32)


def mat_nt(left, right):
    return lax.dot_general(left, right, (((1,), (1,)), ((), ())), preferred_element_type=F32)


def adamw_update(master, first_mom, second_mom, grad_avg, clip_scale, learn_rate):
    scaled = clip_scale * grad_avg
    new_first = BETA1 * first_mom + (1.0 - BETA1) * scaled
    new_second = BETA2 * second_mom + (1.0 - BETA2) * scaled * scaled
    first_hat = new_first * (1.0 / (1.0 - BETA1 ** ADAM_STEP))
    second_hat = new_second * (1.0 / (1.0 - BETA2 ** ADAM_STEP))
    new_master = master - learn_rate * (first_hat / (jnp.sqrt(second_hat) + ADAM_EPS) + WEIGHT_DECAY * master)
    return new_master, new_first, new_second


def gelu_of_half(half):
    t = jnp.tanh(half * (2.0 * SQRT_TWO_PI + (8.0 * SQRT_TWO_PI * GELU_CUBIC) * (half * half)))
    return half + half * t


def stage_rows(src, up_half, down, dst):
    x = src[...]
    half = jnp.dot(x, up_half[...], preferred_element_type=F32)
    hidden = gelu_of_half(half).astype(BF16)
    y = jnp.dot(hidden, down[...], preferred_element_type=F32)
    dst[...] = (x.astype(F32) + y).astype(BF16)


def mixed(k, n_micro):
    before = lax.div(k * N_SENT, n_micro)
    is_sent = lax.div((k + 1) * N_SENT, n_micro) - before
    return is_sent, is_sent * (n_micro - N_SENT + before) + (1 - is_sent) * (k - before)


def forward_part(stage, own_ready, aux_ready, relay_mean, nb_hbm, up_own, down_own, up_aux, down_aux, up_two, down_two, out_hbm, late_hbm, nbuf, xin, yout, nb_sem, out_sem, send_sem, recv_sem, two_send, two_recv):
    n_micro = nbuf.shape[0]
    n_kept = n_micro - N_SENT

    def load(i):
        return pltpu.make_async_copy(nb_hbm.at[i], nbuf.at[i], nb_sem.at[i])

    def store(i):
        return pltpu.make_async_copy(yout.at[i], out_hbm.at[i], out_sem.at[i])

    def push(src, i, peer):
        return pltpu.make_async_remote_copy(src_ref=src.at[i], dst_ref=xin.at[i], send_sem=send_sem.at[i], recv_sem=recv_sem.at[i], device_id={"stage": peer}, device_id_type=MESH)

    def arrived(i):
        push(yout, i, stage).wait_recv()

    def rotated(j):
        return lax.rem(j + n_kept, n_micro)

    def finish_stores():
        def body(i, _):
            store(i).wait()
            return 0
        lax.fori_loop(0, n_micro, body, 0)

    def hand_over():
        return [pltpu.make_async_remote_copy(src_ref=aux, dst_ref=two, send_sem=two_send.at[i], recv_sem=two_recv.at[i], device_id={"stage": 3}, device_id_type=MESH)
                for i, (aux, two) in enumerate([(up_aux, up_two), (down_aux, down_two)])]

    def finish_sends(first, count):
        def body(i, _):
            push(yout, first + i, stage).wait_send()
            return 0
        lax.fori_loop(0, count, body, 0)

    @pl.when(stage == 0)
    def _():
        own_ready()

        def body(j, _):
            i = rotated(j)
            load(i).wait()
            stage_rows(nbuf.at[i], up_own, down_own, yout.at[i])
            push(yout, i, 1).start()
            store(i).start()
            relay_mean(j == 7)
            return 0
        lax.fori_loop(0, n_micro, body, 0)
        finish_sends(0, n_micro)
        finish_stores()

    @pl.when(stage == 1)
    def _():
        own_ready()

        def body(j, _):
            i = rotated(j)
            arrived(i)
            stage_rows(xin.at[i], up_own, down_own, yout.at[i])

            @pl.when(j < N_SENT)
            def _():
                push(yout, i, 2).start()
            store(i).start()
            relay_mean(j == 7)
            return 0
        lax.fori_loop(0, n_micro, body, 0)
        finish_sends(n_kept, N_SENT)
        finish_stores()

    @pl.when(stage == 2)
    def _():
        aux_ready()
        for copy in hand_over():
            copy.start()

        def body(k, _):
            _, i = mixed(k, n_micro)
            arrived(i)

            @pl.when(i < n_kept - N_TWICE)
            def _():
                stage_rows(xin.at[i], up_aux, down_aux, xin.at[i])
            stage_rows(xin.at[i], up_own, down_own, yout.at[i])
            push(yout, i, 3).start()
            store(i).start()
            return 0
        lax.fori_loop(0, n_micro, body, 0)
        finish_sends(0, n_micro)
        finish_stores()
        for copy in hand_over():
            copy.wait_send()

    @pl.when(stage == 3)
    def _():
        aux_ready()

        def first(j, _):
            load(j).wait()
            stage_rows(nbuf.at[j], up_aux, down_aux, nbuf.at[j])

            @pl.when(j == n_kept - N_TWICE)
            def _():
                for copy in hand_over():
                    copy.wait_recv()

            @pl.when(j >= n_kept - N_TWICE)
            def _():
                stage_rows(nbuf.at[j], up_two, down_two, nbuf.at[j])
            push(nbuf, j, 2).start()
            return 0
        lax.fori_loop(0, n_kept, first, 0)

        def body(k, _):
            _, i = mixed(k, n_micro)
            arrived(i)
            stage_rows(xin.at[i], up_own, down_own, yout.at[i])
            store(i).start()
            return 0
        lax.fori_loop(0, n_micro - N_LATE, body, 0)

        def late(k):
            _, i = mixed(k, n_micro)
            return i, pltpu.make_async_copy(xin.at[i], late_hbm.at[k - (n_micro - N_LATE)], out_sem.at[i])

        def save(k, _):
            i, copy = late(k)
            arrived(i)
            copy.start()
            return 0
        lax.fori_loop(n_micro - N_LATE, n_micro, save, 0)

        def stored(k, _):
            _, i = mixed(k, n_micro)
            store(i).wait()
            return 0
        lax.fori_loop(0, n_micro - N_LATE, stored, 0)

        def saved(k, _):
            late(k)[1].wait()
            return 0
        lax.fori_loop(n_micro - N_LATE, n_micro, saved, 0)
        finish_sends(0, n_kept)


def start_loads(stage, nb_hbm, nbuf, nb_sem):
    n_micro = nbuf.shape[0]
    n_kept = n_micro - N_SENT

    def body(j, _):
        i = lax.rem(j + n_kept, n_micro)
        pltpu.make_async_copy(nb_hbm.at[i], nbuf.at[i], nb_sem.at[i]).start()
        return 0

    @pl.when(stage == 0)
    def _():
        lax.fori_loop(0, n_micro, body, 0)

    @pl.when(stage == 3)
    def _():
        lax.fori_loop(N_SENT, n_micro, body, 0)


def step_kernel(up_hbm, down_hbm, m1_up_hbm, m1_down_hbm, m2_up_hbm, m2_down_hbm, gu_hbm, gv_hbm, acts_hbm, loss_hbm, nb_hbm, rate_ref, norm_ref,
                out_hbm, mean_up_hbm, mean_down_hbm, clip_out, late_hbm, w_up_hbm, w_down_hbm,
                up32, down32, gu, gv, mean_up, mean_down, acts, gbuf, dxbuf, hid, slope, dpre, up_bf, down_bf,
                ru1, rv1, ru2, rv2, m_up, m_down, up_own, down_own, up_aux, down_aux, up_two, down_two, sq_all, nbuf, xin, yout,
                in_sem, g_send, g_recv, rs_send, rs_recv, sq_send, sq_recv, ag_send, ag_recv, aux_send, aux_recv,
                nb_sem, out_sem, send_sem, recv_sem, two_send, two_recv):
    stage = lax.axis_index("stage")
    data = lax.axis_index("data")
    z = lax.div(data, 2)
    y = lax.rem(data, 2)
    me = data * 4 + stage
    z_peer = 2 * (1 - z) + y
    y_peer = 2 * z + (1 - y)
    n_tok = acts.shape[0]
    chunk = n_tok // N_CHUNK

    def up_rows(zz, yy, first=0, count=64):
        return pl.ds(pl.multiple_of(128 * yy + 64 * zz + first, 32), count)

    def down_rows(zz, yy, first=0, count=256):
        return pl.ds(pl.multiple_of(512 * zz + 256 * yy + first, 128), count)

    own_up, own_down = up_rows(z, y), down_rows(z, y)
    loads = [
        pltpu.make_async_copy(acts_hbm, acts, in_sem.at[0]),
        pltpu.make_async_copy(up_hbm, up32, in_sem.at[1]),
        pltpu.make_async_copy(down_hbm, down32, in_sem.at[2]),
        pltpu.make_async_copy(gv_hbm, gv, in_sem.at[3]),
        pltpu.make_async_copy(gu_hbm, gu, in_sem.at[4]),
        pltpu.make_async_copy(m1_up_hbm, m_up.at[0], in_sem.at[5]),
        pltpu.make_async_copy(m2_up_hbm, m_up.at[1], in_sem.at[6]),
        pltpu.make_async_copy(m1_down_hbm, m_down.at[0], in_sem.at[7]),
        pltpu.make_async_copy(m2_down_hbm, m_down.at[1], in_sem.at[8]),
    ]
    load_loss = pltpu.make_async_copy(loss_hbm, gbuf, in_sem.at[9])
    loads[0].start()
    loads[1].start()

    @pl.when(stage == 3)
    def _():
        load_loss.start()
    for copy in loads[2:]:
        copy.start()
    start_loads(stage, nb_hbm, nbuf, nb_sem)

    barrier = pltpu.get_barrier_semaphore()

    def greet(d, _):
        other = lax.rem(me + d, 16)
        pl.semaphore_signal(barrier, inc=1, device_id={"data": lax.div(other, 4), "stage": lax.rem(other, 4)}, device_id_type=MESH)
        return 0
    lax.fori_loop(1, 16, greet, 0)

    loads[0].wait()
    loads[1].wait()
    up_bf[...] = up32[...].astype(BF16)
    loads[2].wait()
    down_bf[...] = down32[...].astype(BF16)
    pl.semaphore_wait(barrier, 15)

    @pl.when(stage == 3)
    def _():
        load_loss.wait()

    def chunk_rows(k):
        return pl.ds(pl.multiple_of(k * chunk, chunk), chunk)

    def pass_down(k):
        rows = chunk_rows(k)
        return pltpu.make_async_remote_copy(src_ref=dxbuf.at[rows], dst_ref=gbuf.at[rows], send_sem=g_send.at[k], recv_sem=g_recv.at[k],
                                            device_id={"stage": jnp.maximum(stage - 1, 0)}, device_id_type=MESH)

    def prepare(k):
        rows = chunk_rows(k)
        pre = jnp.dot(acts[rows, :], up_bf[...], preferred_element_type=F32)
        sq = pre * pre
        half_t = 0.5 * jnp.tanh(pre * (SQRT_TWO_PI + (SQRT_TWO_PI * GELU_CUBIC) * sq))
        prob = 0.5 + half_t
        rest = 0.5 - half_t
        hid[rows, :] = (pre * prob).astype(BF16)
        slope[rows, :] = prob + (prob * rest) * pre * (2.0 * SQRT_TWO_PI + (6.0 * SQRT_TWO_PI * GELU_CUBIC) * sq)

    def backward(k):
        rows = chunk_rows(k)

        @pl.when(stage < 3)
        def _():
            pass_down(k).wait_recv()
        grad = gbuf[rows, :]
        d_pre = (mat_nt(grad, down_bf[...]) * slope[rows, :]).astype(BF16)
        dpre[rows, :] = d_pre

        @pl.when(stage > 0)
        def _():
            dxbuf[rows, :] = (grad.astype(F32) + mat_nt(d_pre, up_bf[...])).astype(BF16)
            pass_down(k).start()

    def tick(t, _):
        upper = jnp.where(stage >= 2, 1, 0)
        is_prep = upper * (1 - lax.rem(t, 2)) + (1 - upper) * (1 - lax.div(t, N_CHUNK))
        k = upper * lax.div(t, 2) + (1 - upper) * lax.rem(t, N_CHUNK)

        @pl.when(is_prep == 1)
        def _():
            prepare(k)

        @pl.when(is_prep == 0)
        def _():
            backward(k)
        return 0
    lax.fori_loop(0, 2 * N_CHUNK, tick, 0)

    def rs_copy(src, dst, sem, peer):
        return pltpu.make_async_remote_copy(src_ref=src, dst_ref=dst, send_sem=rs_send.at[sem], recv_sem=rs_recv.at[sem], device_id={"data": peer}, device_id_type=MESH)

    def v_first(sub, c):
        yy = (1 - y) if sub == 0 else y
        return rs_copy(gv.at[down_rows(1 - z, yy, 128 * c, 128)], rv1.at[sub, pl.ds(128 * c, 128)], 2 * sub + c, z_peer)

    def u_first(sub, c):
        zz = (1 - z) if sub == 0 else z
        return rs_copy(gu.at[up_rows(zz, 1 - y, 32 * c, 32)], ru1.at[sub, pl.ds(32 * c, 32)], 4 + 2 * sub + c, y_peer)

    def v_second(c):
        return rs_copy(gv.at[down_rows(z, 1 - y, 128 * c, 128)], rv2.at[pl.ds(128 * c, 128)], 8 + c, y_peer)

    def u_second(c):
        return rs_copy(gu.at[up_rows(1 - z, y, 32 * c, 32)], ru2.at[pl.ds(32 * c, 32)], 10 + c, z_peer)

    loads[3].wait()
    gv[...] += mat_tn(hid[...], gbuf[...])
    for sub in range(2):
        for c in range(2):
            v_first(sub, c).start()
    loads[4].wait()
    gu[...] += mat_tn(acts[...], dpre[...])
    for sub in range(2):
        for c in range(2):
            u_first(sub, c).start()
    for c in range(2):
        v_first(0, c).wait_recv()
        rows = down_rows(z, 1 - y, 128 * c, 128)
        gv[rows, :] += rv1[0, 128 * c:128 * (c + 1), :]
        v_second(c).start()
        u_first(0, c).wait_recv()
        rows = up_rows(1 - z, y, 32 * c, 32)
        gu[rows, :] += ru1[0, 32 * c:32 * (c + 1), :]
        u_second(c).start()
    acc = jnp.zeros((8, 128), F32)

    def fold(tile, acc):
        sq = tile * tile
        sq = jnp.sum(sq.reshape(sq.shape[0] // 8, 8, sq.shape[1]), axis=0)
        for i in range(0, sq.shape[1], 128):
            acc = acc + sq[:, i:i + 128]
        return acc

    for c in range(2):
        v_first(1, c).wait_recv()
        v_second(c).wait_recv()
        rows = down_rows(z, y, 128 * c, 128)
        mean = (gv[rows, :] + rv1[1, 128 * c:128 * (c + 1), :] + rv2[128 * c:128 * (c + 1), :]) * 0.25
        mean_down[rows, :] = mean
        acc = fold(mean, acc)
        u_first(1, c).wait_recv()
        u_second(c).wait_recv()
        rows = up_rows(z, y, 32 * c, 32)
        mean = (gu[rows, :] + ru1[1, 32 * c:32 * (c + 1), :] + ru2[32 * c:32 * (c + 1), :]) * 0.25
        mean_up[rows, :] = mean
        acc = fold(mean, acc)

    def gather(which, up, down):
        def copy(ref, rows, sem, peer):
            return pltpu.make_async_remote_copy(src_ref=ref.at[rows], dst_ref=ref.at[rows], send_sem=ag_send.at[which * 6 + sem], recv_sem=ag_recv.at[which * 6 + sem],
                                                device_id={"data": peer}, device_id_type=MESH)

        sends = [copy(up, own_up, 0, z_peer), copy(down, own_down, 3, y_peer), copy(up, own_up, 1, y_peer), copy(down, own_down, 4, z_peer)]
        relays = [copy(up, up_rows(1 - z, y), 2, y_peer), copy(down, down_rows(z, 1 - y), 5, z_peer)]
        arrive_first = [copy(up, up_rows(1 - z, y), 0, z_peer), copy(down, down_rows(z, 1 - y), 3, y_peer)]
        arrive_rest = [copy(up, up_rows(z, 1 - y), 1, y_peer), copy(down, down_rows(1 - z, y), 4, z_peer),
                       copy(up, up_rows(1 - z, 1 - y), 2, y_peer), copy(down, down_rows(1 - z, 1 - y), 5, z_peer)]

        def begin():
            for c in sends:
                c.start()

        def relay():
            for a, c in zip(arrive_first, relays):
                a.wait_recv()
                c.start()

        def finish():
            for c in arrive_rest:
                c.wait_recv()

        def drain():
            for c in sends + relays:
                c.wait_send()
        return begin, relay, finish, drain

    own_begin, own_relay, own_finish, own_drain = gather(0, up_own, down_own)
    aux_begin, aux_relay, aux_finish, aux_drain = gather(1, up_aux, down_aux)
    mean_begin, mean_relay, mean_finish, mean_drain = gather(2, mean_up, mean_down)

    def sq_copy(other, slot):
        return pltpu.make_async_remote_copy(src_ref=sq_all.at[slot], dst_ref=sq_all.at[slot], send_sem=sq_send.at[other], recv_sem=sq_recv.at[slot],
                                            device_id={"data": lax.div(other, 4), "stage": lax.rem(other, 4)}, device_id_type=MESH)

    sq_all[me] = acc

    def tell(d, _):
        sq_copy(lax.rem(me + d, 16), me).start()
        return 0
    lax.fori_loop(1, 16, tell, 0)
    for copy in loads[5:]:
        copy.wait()

    @pl.when(stage >= 2)
    def _():
        mean_begin()
        mean_relay()
        mean_finish()

    def hear(d, _):
        other = lax.rem(me + d, 16)
        sq_copy(other, other).wait_recv()
        return 0
    lax.fori_loop(1, 16, hear, 0)
    total = sq_all[0]
    for i in range(1, 16):
        total = total + sq_all[i]
    total = jnp.sum(jnp.sum(total, axis=0, keepdims=True), axis=1, keepdims=True)
    clip = jnp.minimum(1.0, norm_ref[0] / (jnp.sqrt(total) + NORM_EPS))
    clip_out[...] = jnp.broadcast_to(clip, clip_out.shape)

    rate = rate_ref[0]
    whole = jnp.where(stage >= 2, 1, 0)

    def renew(t, _):
        rows = pl.ds(pl.multiple_of(64 * (whole * t + (1 - whole) * (2 * y + z)), 64), 64)
        new_up, _, _ = adamw_update(up32[rows, :], m_up[0, rows, :], m_up[1, rows, :], mean_up[rows, :], clip, rate)
        up_own[rows, :] = new_up.astype(BF16) * jnp.asarray(0.5, BF16)
        rows = pl.ds(pl.multiple_of(256 * (whole * t + (1 - whole) * (2 * z + y)), 256), 256)
        new_down, _, _ = adamw_update(down32[rows, :], m_down[0, rows, :], m_down[1, rows, :], mean_down[rows, :], clip, rate)
        down_own[rows, :] = new_down.astype(BF16)
        return 0
    lax.fori_loop(0, 1 + 3 * whole, renew, 0)

    def feed():
        peer = 3 - stage
        return [pltpu.make_async_remote_copy(src_ref=own.at[rows], dst_ref=aux.at[rows], send_sem=aux_send.at[i], recv_sem=aux_recv.at[i], device_id={"stage": peer}, device_id_type=MESH)
                for i, (own, aux, rows) in enumerate([(up_own, up_aux, own_up), (down_own, down_aux, own_down)])]

    @pl.when(stage < 2)
    def _():
        for c in feed():
            c.start()
        own_begin()
        own_relay()
        mean_begin()

    @pl.when(stage >= 2)
    def _():
        for c in feed():
            c.wait_recv()
        aux_begin()
        aux_relay()

    def relay_mean(now):
        @pl.when(now)
        def _():
            mean_relay()

    forward_part(stage, own_finish, aux_finish, relay_mean, nb_hbm, up_own, down_own, up_aux, down_aux, up_two, down_two, out_hbm, late_hbm, nbuf, xin, yout, nb_sem, out_sem, send_sem, recv_sem, two_send, two_recv)

    @pl.when(stage < 2)
    def _():
        mean_finish()
    store_up = pltpu.make_async_copy(mean_up, mean_up_hbm, in_sem.at[0])
    store_down = pltpu.make_async_copy(mean_down, mean_down_hbm, in_sem.at[1])
    store_w_up = pltpu.make_async_copy(up_own, w_up_hbm, in_sem.at[2])
    store_w_down = pltpu.make_async_copy(down_own, w_down_hbm, in_sem.at[3])
    store_up.start()
    store_down.start()
    store_w_up.start()
    store_w_down.start()

    @pl.when(stage > 0)
    def _():
        for k in range(N_CHUNK):
            pass_down(k).wait_send()
    for c in range(2):
        for sub in range(2):
            v_first(sub, c).wait_send()
            u_first(sub, c).wait_send()
        v_second(c).wait_send()
        u_second(c).wait_send()

    def told(d, _):
        sq_copy(lax.rem(me + d, 16), me).wait_send()
        return 0
    lax.fori_loop(1, 16, told, 0)
    mean_drain()

    @pl.when(stage < 2)
    def _():
        own_drain()
        for c in feed():
            c.wait_send()

    @pl.when(stage >= 2)
    def _():
        aux_drain()
    store_up.wait()
    store_down.wait()
    store_w_up.wait()
    store_w_down.wait()


def fused_step(master_up, master_down, m1_up, m1_down, m2_up, m2_down, grad_up, grad_down, acts, loss_grad, next_batch, learn_rate, max_norm):
    n_micro = next_batch.shape[0]
    n_tok, width = acts.shape
    hidden = master_up.shape[1]
    hbm = pl.BlockSpec(memory_space=pl.ANY)
    smem = pl.BlockSpec(memory_space=pltpu.SMEM)
    vmem = pltpu.VMEM
    dma = pltpu.SemaphoreType.DMA
    return pl.pallas_call(
        step_kernel,
        name="pipeline_step",
        out_shape=[jax.ShapeDtypeStruct(next_batch.shape, BF16), jax.ShapeDtypeStruct((width, hidden), F32), jax.ShapeDtypeStruct((hidden, width), F32), jax.ShapeDtypeStruct((8, 128), F32),
                   jax.ShapeDtypeStruct((N_LATE,) + next_batch.shape[1:], BF16), jax.ShapeDtypeStruct((width, hidden), BF16), jax.ShapeDtypeStruct((hidden, width), BF16)],
        in_specs=[hbm] * 11 + [smem] * 2,
        out_specs=[hbm, hbm, hbm, pl.BlockSpec(memory_space=pltpu.VMEM), hbm, hbm, hbm],
        scratch_shapes=[
            vmem((width, hidden), F32), vmem((hidden, width), F32),
            vmem((width, hidden), F32), vmem((hidden, width), F32),
            vmem((width, hidden), F32), vmem((hidden, width), F32),
            vmem((n_tok, width), BF16), vmem((n_tok, width), BF16), vmem((n_tok, width), BF16),
            vmem((n_tok, hidden), BF16), vmem((n_tok, hidden), F32), vmem((n_tok, hidden), BF16),
            vmem((width, hidden), BF16), vmem((hidden, width), BF16),
            vmem((2, width // 4, hidden), F32), vmem((2, hidden // 4, width), F32),
            vmem((width // 4, hidden), F32), vmem((hidden // 4, width), F32),
            vmem((2, width, hidden), F32), vmem((2, hidden, width), F32),
            vmem((width, hidden), BF16), vmem((hidden, width), BF16),
            vmem((width, hidden), BF16), vmem((hidden, width), BF16),
            vmem((width, hidden), BF16), vmem((hidden, width), BF16),
            vmem((16, 8, 128), F32),
            vmem(next_batch.shape, BF16), vmem(next_batch.shape, BF16), vmem(next_batch.shape, BF16),
            dma((10,)), dma((N_CHUNK,)), dma((N_CHUNK,)), dma((12,)), dma((12,)), dma((16,)), dma((16,)), dma((18,)), dma((18,)), dma((2,)), dma((2,)),
            dma((n_micro,)), dma((n_micro,)), dma((n_micro,)), dma((n_micro,)), dma((2,)), dma((2,)),
        ],
        compiler_params=pltpu.CompilerParams(collective_id=1, has_side_effects=True, vmem_limit_bytes=63 * 1024 * 1024),
    )(master_up, master_down, m1_up, m1_down, m2_up, m2_down, grad_up, grad_down, acts, loss_grad, next_batch, learn_rate, max_norm)


def finish_kernel(outs_in, late_in, w_up_in, w_down_in, mean_up_in, mean_down_in, up_in, down_in, m1_up_in, m1_down_in, m2_up_in, m2_down_in, clip_ref, rate_ref,
                  outs, up_out, down_out, m1_up_out, m1_down_out, m2_up_out, m2_down_out,
                  obuf, late, w_up, w_down, upd_up, upd_down, load_sem, store_sem, micro_load, micro_store, late_load):
    stage = lax.axis_index("stage")
    n_micro = obuf.shape[0]
    last = stage == 3
    n_copied = jnp.where(last, n_micro - N_LATE, n_micro)
    up_loads = [pltpu.make_async_copy(src, upd_up.at[i], load_sem.at[i]) for i, src in enumerate((mean_up_in, up_in, m1_up_in, m2_up_in))]
    down_loads = [pltpu.make_async_copy(src, upd_down.at[i], load_sem.at[4 + i]) for i, src in enumerate((mean_down_in, down_in, m1_down_in, m2_down_in))]
    w_loads = [pltpu.make_async_copy(w_up_in, w_up, load_sem.at[8]), pltpu.make_async_copy(w_down_in, w_down, load_sem.at[9])]
    up_stores = [pltpu.make_async_copy(upd_up.at[1 + i], dst, store_sem.at[i]) for i, dst in enumerate((up_out, m1_up_out, m2_up_out))]
    down_stores = [pltpu.make_async_copy(upd_down.at[1 + i], dst, store_sem.at[3 + i]) for i, dst in enumerate((down_out, m1_down_out, m2_down_out))]

    def place(k):
        return mixed(k, n_micro)[1]

    def load_micro(k):
        i = place(k)
        return pltpu.make_async_copy(outs_in.at[i], obuf.at[i], micro_load.at[i])

    def store_micro(k):
        i = place(k)
        return pltpu.make_async_copy(obuf.at[i], outs.at[i], micro_store.at[i])

    def load_late(n):
        return pltpu.make_async_copy(late_in.at[n], late.at[n], late_load.at[n])

    for copy in up_loads:
        copy.start()

    def start_micro(k, _):
        load_micro(k).start()
        return 0

    def turn_micro(k, _):
        load_micro(k).wait()
        store_micro(k).start()
        return 0

    @pl.when(last)
    def _():
        for copy in w_loads:
            copy.start()
        for n in range(N_LATE):
            load_late(n).start()
    for copy in down_loads:
        copy.start()
    lax.fori_loop(0, n_copied, start_micro, 0)
    clip = clip_ref[0:1, 0:1]
    rate = rate_ref[0]

    def update(buf, n_rows):
        def body(t, _):
            rows = pl.ds(pl.multiple_of(t * n_rows, n_rows), n_rows)
            new = adamw_update(buf[1, rows, :], buf[2, rows, :], buf[3, rows, :], buf[0, rows, :], clip, rate)
            for i in range(3):
                buf[1 + i, rows, :] = new[i]
            return 0
        lax.fori_loop(0, buf.shape[1] // n_rows, body, 0)

    for copy in up_loads:
        copy.wait()
    update(upd_up, 32)
    for copy in up_stores:
        copy.start()
    for copy in down_loads:
        copy.wait()
    update(upd_down, 128)
    for copy in down_stores:
        copy.start()

    @pl.when(last)
    def _():
        for copy in w_loads:
            copy.wait()

        def body(n, _):
            for j in range(3):
                k = 3 * n + j

                @pl.when(k < n_micro - N_LATE)
                def _():
                    turn_micro(k, 0)
            load_late(n).wait()
            k = n_micro - N_LATE + n
            i = place(k)
            stage_rows(late.at[n], w_up, w_down, obuf.at[i])
            store_micro(k).start()
            return 0
        lax.fori_loop(0, N_LATE, body, 0)

    @pl.when(jnp.logical_not(last))
    def _():
        lax.fori_loop(0, n_micro, turn_micro, 0)

    def stored(k, _):
        store_micro(k).wait()
        return 0
    lax.fori_loop(0, n_micro, stored, 0)
    for copy in up_stores + down_stores:
        copy.wait()


def finish_step(outs, late, w_up, w_down, mean_up, mean_down, clip, master_up, master_down, m1_up, m1_down, m2_up, m2_down, learn_rate):
    n_micro = outs.shape[0]
    hbm = pl.BlockSpec(memory_space=pl.ANY)
    vmem = pltpu.VMEM
    dma = pltpu.SemaphoreType.DMA
    up, down = jax.ShapeDtypeStruct(master_up.shape, F32), jax.ShapeDtypeStruct(master_down.shape, F32)
    return pl.pallas_call(
        finish_kernel,
        name="finish_step",
        out_shape=[jax.ShapeDtypeStruct(outs.shape, BF16), up, down, up, down, up, down],
        in_specs=[hbm] * 12 + [pl.BlockSpec(memory_space=pltpu.VMEM), pl.BlockSpec(memory_space=pltpu.SMEM)],
        out_specs=[hbm] * 7,
        scratch_shapes=[
            vmem(outs.shape, BF16), vmem(late.shape, BF16), vmem(w_up.shape, BF16), vmem(w_down.shape, BF16),
            vmem((4,) + master_up.shape, F32), vmem((4,) + master_down.shape, F32),
            dma((10,)), dma((6,)), dma((n_micro,)), dma((n_micro,)), dma((N_LATE,)),
        ],
        compiler_params=pltpu.CompilerParams(vmem_limit_bytes=56 * 1024 * 1024),
    )(outs, late, w_up, w_down, mean_up, mean_down, master_up, master_down, m1_up, m1_down, m2_up, m2_down, clip, learn_rate)


def solution(mesh):
    def local_step(master_up, master_down, mom1_up, mom1_down, mom2_up, mom2_down, grad_up, grad_down, stage_acts, loss_grad, next_batch, learn_rate, max_norm):
        stage_outs, gbar_up, gbar_down, clip, late, w_up, w_down = fused_step(
            master_up[0], master_down[0], mom1_up[0], mom1_down[0], mom2_up[0], mom2_down[0], grad_up[0, 0], grad_down[0, 0],
            stage_acts[0], loss_grad, next_batch, learn_rate.reshape(1), max_norm.reshape(1))
        stage_outs, new_up, new_down, new_m1_up, new_m1_down, new_m2_up, new_m2_down = finish_step(
            stage_outs, late, w_up, w_down, gbar_up, gbar_down, clip, master_up[0], master_down[0], mom1_up[0], mom1_down[0], mom2_up[0], mom2_down[0], learn_rate.reshape(1))
        return (new_up[None], new_down[None], new_m1_up[None], new_m1_down[None], new_m2_up[None], new_m2_down[None], stage_outs[None])

    w_spec = P('stage', None, None)
    g_spec = P('data', 'stage', None, None)
    in_specs = (w_spec, w_spec, w_spec, w_spec, w_spec, w_spec, g_spec, g_spec, P('stage', 'data', None), P('data', None), P(None, 'data', None), P(), P())
    out_specs = (w_spec, w_spec, w_spec, w_spec, w_spec, w_spec, P('stage', None, 'data', None))
    return jax.shard_map(local_step, mesh=mesh, in_specs=in_specs, out_specs=out_specs, check_vma=False)
```

```python
import jax
import jax.numpy as jnp
from jax import lax
from jax.experimental import pallas as pl
from jax.experimental.pallas import tpu as pltpu
from jax.sharding import PartitionSpec as P

BETA1 = 0.9
BETA2 = 0.95
ADAM_EPS = 1e-8
WEIGHT_DECAY = 0.1
NORM_EPS = 1e-6
ADAM_STEP = 8
SQRT_TWO_PI = 0.7978845608028654
GELU_CUBIC = 0.044715

N_SENT = 6
N_CHUNK = 4
N_LATE = 3
N_TWICE = 1
N_PIECE = 2
MESH = pl.DeviceIdType.MESH
BF16 = jnp.bfloat16
F32 = jnp.float32


def mat_tn(left, right):
    return lax.dot_general(left, right, (((0,), (0,)), ((), ())), preferred_element_type=F32)


def mat_nt(left, right):
    return lax.dot_general(left, right, (((1,), (1,)), ((), ())), preferred_element_type=F32)


def adamw_update(master, first_mom, second_mom, grad_avg, clip_scale, learn_rate):
    scaled = clip_scale * grad_avg
    new_first = BETA1 * first_mom + (1.0 - BETA1) * scaled
    new_second = BETA2 * second_mom + (1.0 - BETA2) * scaled * scaled
    first_hat = new_first * (1.0 / (1.0 - BETA1 ** ADAM_STEP))
    second_hat = new_second * (1.0 / (1.0 - BETA2 ** ADAM_STEP))
    new_master = master - learn_rate * (first_hat / (jnp.sqrt(second_hat) + ADAM_EPS) + WEIGHT_DECAY * master)
    return new_master, new_first, new_second


def gelu_of_half(half):
    t = jnp.tanh(half * (2.0 * SQRT_TWO_PI + (8.0 * SQRT_TWO_PI * GELU_CUBIC) * (half * half)))
    return half + half * t


def stage_rows(src, up_half, down, dst):
    x = src[...]
    half = jnp.dot(x, up_half[...], preferred_element_type=F32)
    hidden = gelu_of_half(half).astype(BF16)
    y = jnp.dot(hidden, down[...], preferred_element_type=F32)
    dst[...] = (x.astype(F32) + y).astype(BF16)


def mixed(k, n_micro):
    before = lax.div(k * N_SENT, n_micro)
    is_sent = lax.div((k + 1) * N_SENT, n_micro) - before
    return is_sent, is_sent * (n_micro - N_SENT + before) + (1 - is_sent) * (k - before)


def forward_part(stage, own_ready, aux_ready, relay_mean, nb_hbm, up_own, down_own, up_aux, down_aux, up_two, down_two, out_hbm, late_hbm, nbuf, xin, yout, nb_sem, out_sem, send_sem, recv_sem, two_send, two_recv):
    n_micro = nbuf.shape[0]
    n_kept = n_micro - N_SENT

    def load(i):
        return pltpu.make_async_copy(nb_hbm.at[i], nbuf.at[i], nb_sem.at[i])

    def store(i):
        return pltpu.make_async_copy(yout.at[i], out_hbm.at[i], out_sem.at[i])

    def push(src, i, peer):
        return pltpu.make_async_remote_copy(src_ref=src.at[i], dst_ref=xin.at[i], send_sem=send_sem.at[i], recv_sem=recv_sem.at[i], device_id={"stage": peer}, device_id_type=MESH)

    def arrived(i):
        push(yout, i, stage).wait_recv()

    def rotated(j):
        return lax.rem(j + n_kept, n_micro)

    def finish_stores():
        def body(i, _):
            store(i).wait()
            return 0
        lax.fori_loop(0, n_micro, body, 0)

    def hand_over():
        return [pltpu.make_async_remote_copy(src_ref=aux, dst_ref=two, send_sem=two_send.at[i], recv_sem=two_recv.at[i], device_id={"stage": 3}, device_id_type=MESH)
                for i, (aux, two) in enumerate([(up_aux, up_two), (down_aux, down_two)])]

    def finish_sends(first, count):
        def body(i, _):
            push(yout, first + i, stage).wait_send()
            return 0
        lax.fori_loop(0, count, body, 0)

    @pl.when(stage == 0)
    def _():
        own_ready()

        def body(j, _):
            i = rotated(j)
            load(i).wait()
            stage_rows(nbuf.at[i], up_own, down_own, yout.at[i])
            push(yout, i, 1).start()
            store(i).start()
            relay_mean(j == 7)
            return 0
        lax.fori_loop(0, n_micro, body, 0)
        finish_sends(0, n_micro)
        finish_stores()

    @pl.when(stage == 1)
    def _():
        own_ready()

        def body(j, _):
            i = rotated(j)
            arrived(i)
            stage_rows(xin.at[i], up_own, down_own, yout.at[i])

            @pl.when(j < N_SENT)
            def _():
                push(yout, i, 2).start()
            store(i).start()
            relay_mean(j == 7)
            return 0
        lax.fori_loop(0, n_micro, body, 0)
        finish_sends(n_kept, N_SENT)
        finish_stores()

    @pl.when(stage == 2)
    def _():
        aux_ready()
        for copy in hand_over():
            copy.start()

        def body(k, _):
            _, i = mixed(k, n_micro)
            arrived(i)

            @pl.when(i < n_kept - N_TWICE)
            def _():
                stage_rows(xin.at[i], up_aux, down_aux, xin.at[i])
            stage_rows(xin.at[i], up_own, down_own, yout.at[i])
            push(yout, i, 3).start()
            store(i).start()
            return 0
        lax.fori_loop(0, n_micro, body, 0)
        finish_sends(0, n_micro)
        finish_stores()
        for copy in hand_over():
            copy.wait_send()

    @pl.when(stage == 3)
    def _():
        aux_ready()

        def first(j, _):
            load(j).wait()
            stage_rows(nbuf.at[j], up_aux, down_aux, nbuf.at[j])

            @pl.when(j == n_kept - N_TWICE)
            def _():
                for copy in hand_over():
                    copy.wait_recv()

            @pl.when(j >= n_kept - N_TWICE)
            def _():
                stage_rows(nbuf.at[j], up_two, down_two, nbuf.at[j])
            push(nbuf, j, 2).start()
            return 0
        lax.fori_loop(0, n_kept, first, 0)

        def body(k, _):
            _, i = mixed(k, n_micro)
            arrived(i)
            stage_rows(xin.at[i], up_own, down_own, yout.at[i])
            store(i).start()
            return 0
        lax.fori_loop(0, n_micro - N_LATE, body, 0)

        def late(k):
            _, i = mixed(k, n_micro)
            return i, pltpu.make_async_copy(xin.at[i], late_hbm.at[k - (n_micro - N_LATE)], out_sem.at[i])

        def save(k, _):
            i, copy = late(k)
            arrived(i)
            copy.start()
            return 0
        lax.fori_loop(n_micro - N_LATE, n_micro, save, 0)

        def stored(k, _):
            _, i = mixed(k, n_micro)
            store(i).wait()
            return 0
        lax.fori_loop(0, n_micro - N_LATE, stored, 0)

        def saved(k, _):
            late(k)[1].wait()
            return 0
        lax.fori_loop(n_micro - N_LATE, n_micro, saved, 0)
        finish_sends(0, n_kept)


def start_loads(stage, nb_hbm, nbuf, nb_sem):
    n_micro = nbuf.shape[0]
    n_kept = n_micro - N_SENT

    def body(j, _):
        i = lax.rem(j + n_kept, n_micro)
        pltpu.make_async_copy(nb_hbm.at[i], nbuf.at[i], nb_sem.at[i]).start()
        return 0

    @pl.when(stage == 0)
    def _():
        lax.fori_loop(0, n_micro, body, 0)

    @pl.when(stage == 3)
    def _():
        lax.fori_loop(N_SENT, n_micro, body, 0)


def step_kernel(up_hbm, down_hbm, m1_up_hbm, m1_down_hbm, m2_up_hbm, m2_down_hbm, gu_hbm, gv_hbm, acts_hbm, loss_hbm, nb_hbm, rate_ref, norm_ref,
                out_hbm, mean_up_hbm, mean_down_hbm, clip_out, late_hbm, w_up_hbm, w_down_hbm,
                up32, down32, gu, gv, mean_up, mean_down, acts, gbuf, dxbuf, hid, slope, dpre, up_bf, down_bf,
                ru1, rv1, ru2, rv2, m_up, m_down, up_own, down_own, up_aux, down_aux, up_two, down_two, sq_all, nbuf, xin, yout,
                in_sem, g_send, g_recv, rs_send, rs_recv, sq_send, sq_recv, ag_send, ag_recv, aux_send, aux_recv,
                nb_sem, out_sem, send_sem, recv_sem, two_send, two_recv):
    stage = lax.axis_index("stage")
    data = lax.axis_index("data")
    z = lax.div(data, 2)
    y = lax.rem(data, 2)
    me = data * 4 + stage
    z_peer = 2 * (1 - z) + y
    y_peer = 2 * z + (1 - y)
    n_tok = acts.shape[0]
    chunk = n_tok // N_CHUNK

    def up_rows(zz, yy, first=0, count=64):
        return pl.ds(pl.multiple_of(128 * yy + 64 * zz + first, 32), count)

    def down_rows(zz, yy, first=0, count=256):
        return pl.ds(pl.multiple_of(512 * zz + 256 * yy + first, 128), count)

    own_up, own_down = up_rows(z, y), down_rows(z, y)
    loads = [
        pltpu.make_async_copy(acts_hbm, acts, in_sem.at[0]),
        pltpu.make_async_copy(up_hbm, up32, in_sem.at[1]),
        pltpu.make_async_copy(down_hbm, down32, in_sem.at[2]),
        pltpu.make_async_copy(gv_hbm, gv, in_sem.at[3]),
        pltpu.make_async_copy(gu_hbm, gu, in_sem.at[4]),
        pltpu.make_async_copy(m1_up_hbm, m_up.at[0], in_sem.at[5]),
        pltpu.make_async_copy(m2_up_hbm, m_up.at[1], in_sem.at[6]),
        pltpu.make_async_copy(m1_down_hbm, m_down.at[0], in_sem.at[7]),
        pltpu.make_async_copy(m2_down_hbm, m_down.at[1], in_sem.at[8]),
    ]
    load_loss = pltpu.make_async_copy(loss_hbm, gbuf, in_sem.at[9])
    for copy in loads[:2]:
        copy.start()

    @pl.when(stage == 3)
    def _():
        load_loss.start()
    loads[2].start()

    barrier = pltpu.get_barrier_semaphore()

    def greet(d, _):
        other = lax.rem(me + d, 16)
        pl.semaphore_signal(barrier, inc=1, device_id={"data": lax.div(other, 4), "stage": lax.rem(other, 4)}, device_id_type=MESH)
        return 0
    lax.fori_loop(1, 16, greet, 0)

    def chunk_rows(k):
        return pl.ds(pl.multiple_of(k * chunk, chunk), chunk)

    def pass_down(k):
        rows = chunk_rows(k)
        return pltpu.make_async_remote_copy(src_ref=dxbuf.at[rows], dst_ref=gbuf.at[rows], send_sem=g_send.at[k], recv_sem=g_recv.at[k],
                                            device_id={"stage": jnp.maximum(stage - 1, 0)}, device_id_type=MESH)

    def prepare(k):
        rows = chunk_rows(k)
        pre = jnp.dot(acts[rows, :], up_bf[...], preferred_element_type=F32)
        sq = pre * pre
        half_t = 0.5 * jnp.tanh(pre * (SQRT_TWO_PI + (SQRT_TWO_PI * GELU_CUBIC) * sq))
        prob = 0.5 + half_t
        rest = 0.5 - half_t
        hid[rows, :] = (pre * prob).astype(BF16)
        slope[rows, :] = prob + (prob * rest) * pre * (2.0 * SQRT_TWO_PI + (6.0 * SQRT_TWO_PI * GELU_CUBIC) * sq)

    def backward(k):
        rows = chunk_rows(k)

        @pl.when(stage < 3)
        def _():
            pass_down(k).wait_recv()
        grad = gbuf[rows, :]
        d_pre = (mat_nt(grad, down_bf[...]) * slope[rows, :]).astype(BF16)
        dpre[rows, :] = d_pre

        @pl.when(stage > 0)
        def _():
            dxbuf[rows, :] = (grad.astype(F32) + mat_nt(d_pre, up_bf[...])).astype(BF16)
            pass_down(k).start()

    def rs_copy(src, dst, sem, peer):
        return pltpu.make_async_remote_copy(src_ref=src, dst_ref=dst, send_sem=rs_send.at[sem], recv_sem=rs_recv.at[sem], device_id={"data": peer}, device_id_type=MESH)

    def v_first(sub, c):
        yy = (1 - y) if sub == 0 else y
        return rs_copy(gv.at[down_rows(1 - z, yy, 128 * c, 128)], rv1.at[sub, pl.ds(128 * c, 128)], 2 * sub + c, z_peer)

    def u_first(sub, c):
        zz = (1 - z) if sub == 0 else z
        return rs_copy(gu.at[up_rows(zz, 1 - y, 32 * c, 32)], ru1.at[sub, pl.ds(32 * c, 32)], 4 + 2 * sub + c, y_peer)

    def v_second(c):
        return rs_copy(gv.at[down_rows(z, 1 - y, 128 * c, 128)], rv2.at[pl.ds(128 * c, 128)], 8 + c, y_peer)

    def u_second(c):
        return rs_copy(gu.at[up_rows(1 - z, y, 32 * c, 32)], ru2.at[pl.ds(32 * c, 32)], 10 + c, z_peer)

    def add_grads(k):
        rows = chunk_rows(k)

        @pl.when(k == 0)
        def _():
            loads[3].wait()
            loads[4].wait()

        def half(h, _):
            zz = h * z + (1 - h) * (1 - z)
            yy = h * y + (1 - h) * (1 - y)
            send = (k == N_CHUNK - 1) & (h == 0)
            out = pl.ds(pl.multiple_of(512 * zz, 512), 512)
            gv[out, :] += mat_tn(hid[rows, out], gbuf[rows, :])

            @pl.when(send)
            def _():
                for sub in range(2):
                    for c in range(2):
                        v_first(sub, c).start()
            out = pl.ds(pl.multiple_of(128 * yy, 128), 128)
            gu[out, :] += mat_tn(acts[rows, out], dpre[rows, :])

            @pl.when(send)
            def _():
                for sub in range(2):
                    for c in range(2):
                        u_first(sub, c).start()
            return 0
        lax.fori_loop(0, 2, half, 0)

    def tick(t, _):
        upper = jnp.where(stage >= 2, 1, 0)
        even = 1 - lax.rem(t, 2)
        early = jnp.where(t < N_CHUNK, 1, 0)
        late = jnp.where(t >= 2 * N_CHUNK, 1, 0)
        is_prep = upper * even * (1 - late) + (1 - upper) * early
        is_grad = upper * late + (1 - upper) * (1 - early) * (1 - even)
        k = upper * (late * (t - 2 * N_CHUNK) + (1 - late) * lax.div(t, 2)) + (1 - upper) * (early * t + (1 - early) * lax.div(t - N_CHUNK, 2))

        @pl.when(is_prep == 1)
        def _():
            prepare(k)

        @pl.when(is_prep + is_grad == 0)
        def _():
            backward(k)

        @pl.when(is_grad == 1)
        def _():
            add_grads(k)
        return 0

    loads[0].wait()
    loads[1].wait()
    up_bf[...] = up32[...].astype(BF16)
    prepare(0)
    loads[2].wait()
    for copy in loads[3:]:
        copy.start()
    start_loads(stage, nb_hbm, nbuf, nb_sem)
    down_bf[...] = down32[...].astype(BF16)
    pl.semaphore_wait(barrier, 15)

    @pl.when(stage == 3)
    def _():
        load_loss.wait()
    lax.fori_loop(1, 3 * N_CHUNK, tick, 0)

    for c in range(2):
        v_first(0, c).wait_recv()
        rows = down_rows(z, 1 - y, 128 * c, 128)
        gv[rows, :] += rv1[0, 128 * c:128 * (c + 1), :]
        v_second(c).start()
        u_first(0, c).wait_recv()
        rows = up_rows(1 - z, y, 32 * c, 32)
        gu[rows, :] += ru1[0, 32 * c:32 * (c + 1), :]
        u_second(c).start()
    acc = jnp.zeros((8, 128), F32)

    def fold(tile, acc):
        sq = tile * tile
        sq = jnp.sum(sq.reshape(sq.shape[0] // 8, 8, sq.shape[1]), axis=0)
        for i in range(0, sq.shape[1], 128):
            acc = acc + sq[:, i:i + 128]
        return acc

    for c in range(2):
        v_first(1, c).wait_recv()
        v_second(c).wait_recv()
        rows = down_rows(z, y, 128 * c, 128)
        mean = (gv[rows, :] + rv1[1, 128 * c:128 * (c + 1), :] + rv2[128 * c:128 * (c + 1), :]) * 0.25
        mean_down[rows, :] = mean
        acc = fold(mean, acc)
        u_first(1, c).wait_recv()
        u_second(c).wait_recv()
        rows = up_rows(z, y, 32 * c, 32)
        mean = (gu[rows, :] + ru1[1, 32 * c:32 * (c + 1), :] + ru2[32 * c:32 * (c + 1), :]) * 0.25
        mean_up[rows, :] = mean
        acc = fold(mean, acc)

    up_piece, down_piece = 64 // N_PIECE, 256 // N_PIECE

    def gather(which, up, down):
        def copy(ref, rows, sem, piece, peer):
            sem = (which * 6 + sem) * N_PIECE + piece
            return pltpu.make_async_remote_copy(src_ref=ref.at[rows], dst_ref=ref.at[rows], send_sem=ag_send.at[sem], recv_sem=ag_recv.at[sem],
                                                device_id={"data": peer}, device_id_type=MESH)

        def up_copy(zz, yy, sem, p, peer):
            return copy(up, up_rows(zz, yy, up_piece * p, up_piece), sem, p, peer)

        def down_copy(zz, yy, sem, p, peer):
            return copy(down, down_rows(zz, yy, down_piece * p, down_piece), sem, p, peer)

        def up_sends(p):
            return [up_copy(z, y, 0, p, z_peer), up_copy(z, y, 1, p, y_peer)]

        def down_sends(p):
            return [down_copy(z, y, 3, p, y_peer), down_copy(z, y, 4, p, z_peer)]

        def relays(p):
            return [(up_copy(1 - z, y, 0, p, z_peer), up_copy(1 - z, y, 2, p, y_peer)), (down_copy(z, 1 - y, 3, p, y_peer), down_copy(z, 1 - y, 5, p, z_peer))]

        def begin(fed=None):
            for p in range(N_PIECE):
                for i, sends in enumerate((up_sends(p), down_sends(p))):
                    if fed is not None:
                        fed(p)[i].wait_recv()
                    for c in sends:
                        c.start()

        def relay():
            for p in range(N_PIECE):
                for arrived, onward in relays(p):
                    arrived.wait_recv()
                    onward.start()

        def finish():
            for p in range(N_PIECE):
                for c in (up_copy(z, 1 - y, 1, p, y_peer), down_copy(1 - z, y, 4, p, z_peer), up_copy(1 - z, 1 - y, 2, p, y_peer), down_copy(1 - z, 1 - y, 5, p, z_peer)):
                    c.wait_recv()

        def drain():
            for p in range(N_PIECE):
                for c in up_sends(p) + down_sends(p) + [onward for _, onward in relays(p)]:
                    c.wait_send()
        return begin, relay, finish, drain

    own_begin, own_relay, own_finish, own_drain = gather(0, up_own, down_own)
    aux_begin, aux_relay, aux_finish, aux_drain = gather(1, up_aux, down_aux)
    mean_begin, mean_relay, mean_finish, mean_drain = gather(2, mean_up, mean_down)

    def sq_copy(other, slot):
        return pltpu.make_async_remote_copy(src_ref=sq_all.at[slot], dst_ref=sq_all.at[slot], send_sem=sq_send.at[other], recv_sem=sq_recv.at[slot],
                                            device_id={"data": lax.div(other, 4), "stage": lax.rem(other, 4)}, device_id_type=MESH)

    sq_all[me] = acc

    def tell(d, _):
        sq_copy(lax.rem(me + d, 16), me).start()
        return 0
    lax.fori_loop(1, 16, tell, 0)
    for copy in loads[5:]:
        copy.wait()

    @pl.when(stage >= 2)
    def _():
        mean_begin()
        mean_relay()
        mean_finish()

    def hear(d, _):
        other = lax.rem(me + d, 16)
        sq_copy(other, other).wait_recv()
        return 0
    lax.fori_loop(1, 16, hear, 0)
    total = sq_all[0]
    for i in range(1, 16):
        total = total + sq_all[i]
    total = jnp.sum(jnp.sum(total, axis=0, keepdims=True), axis=1, keepdims=True)
    clip = jnp.minimum(1.0, norm_ref[0] / (jnp.sqrt(total) + NORM_EPS))
    clip_out[...] = jnp.broadcast_to(clip, clip_out.shape)

    rate = rate_ref[0]
    whole = jnp.where(stage >= 2, 1, 0)

    def renew(t, _):
        rows = pl.ds(pl.multiple_of(64 * (whole * t + (1 - whole) * (2 * y + z)), 64), 64)
        new_up, _, _ = adamw_update(up32[rows, :], m_up[0, rows, :], m_up[1, rows, :], mean_up[rows, :], clip, rate)
        up_own[rows, :] = new_up.astype(BF16) * jnp.asarray(0.5, BF16)
        rows = pl.ds(pl.multiple_of(256 * (whole * t + (1 - whole) * (2 * z + y)), 256), 256)
        new_down, _, _ = adamw_update(down32[rows, :], m_down[0, rows, :], m_down[1, rows, :], mean_down[rows, :], clip, rate)
        down_own[rows, :] = new_down.astype(BF16)
        return 0
    lax.fori_loop(0, 1 + 3 * whole, renew, 0)

    def feed(p):
        parts = [(up_own, up_aux, up_rows(z, y, up_piece * p, up_piece)), (down_own, down_aux, down_rows(z, y, down_piece * p, down_piece))]
        return [pltpu.make_async_remote_copy(src_ref=own.at[rows], dst_ref=aux.at[rows], send_sem=aux_send.at[2 * p + i], recv_sem=aux_recv.at[2 * p + i], device_id={"stage": 3 - stage}, device_id_type=MESH)
                for i, (own, aux, rows) in enumerate(parts)]

    @pl.when(stage < 2)
    def _():
        for p in range(N_PIECE):
            for c in feed(p):
                c.start()
        own_begin()
        own_relay()
        mean_begin()

    @pl.when(stage >= 2)
    def _():
        aux_begin(feed)
        aux_relay()

    def relay_mean(now):
        @pl.when(now)
        def _():
            mean_relay()

    forward_part(stage, own_finish, aux_finish, relay_mean, nb_hbm, up_own, down_own, up_aux, down_aux, up_two, down_two, out_hbm, late_hbm, nbuf, xin, yout, nb_sem, out_sem, send_sem, recv_sem, two_send, two_recv)

    @pl.when(stage < 2)
    def _():
        mean_finish()
    store_up = pltpu.make_async_copy(mean_up, mean_up_hbm, in_sem.at[0])
    store_down = pltpu.make_async_copy(mean_down, mean_down_hbm, in_sem.at[1])
    store_w_up = pltpu.make_async_copy(up_own, w_up_hbm, in_sem.at[2])
    store_w_down = pltpu.make_async_copy(down_own, w_down_hbm, in_sem.at[3])
    store_up.start()
    store_down.start()
    store_w_up.start()
    store_w_down.start()

    @pl.when(stage > 0)
    def _():
        for k in range(N_CHUNK):
            pass_down(k).wait_send()
    for c in range(2):
        for sub in range(2):
            v_first(sub, c).wait_send()
            u_first(sub, c).wait_send()
        v_second(c).wait_send()
        u_second(c).wait_send()

    def told(d, _):
        sq_copy(lax.rem(me + d, 16), me).wait_send()
        return 0
    lax.fori_loop(1, 16, told, 0)
    mean_drain()

    @pl.when(stage < 2)
    def _():
        own_drain()
        for p in range(N_PIECE):
            for c in feed(p):
                c.wait_send()

    @pl.when(stage >= 2)
    def _():
        aux_drain()
    store_up.wait()
    store_down.wait()
    store_w_up.wait()
    store_w_down.wait()


def fused_step(master_up, master_down, m1_up, m1_down, m2_up, m2_down, grad_up, grad_down, acts, loss_grad, next_batch, learn_rate, max_norm):
    n_micro = next_batch.shape[0]
    n_tok, width = acts.shape
    hidden = master_up.shape[1]
    hbm = pl.BlockSpec(memory_space=pl.ANY)
    smem = pl.BlockSpec(memory_space=pltpu.SMEM)
    vmem = pltpu.VMEM
    dma = pltpu.SemaphoreType.DMA
    return pl.pallas_call(
        step_kernel,
        name="pipeline_step",
        out_shape=[jax.ShapeDtypeStruct(next_batch.shape, BF16), jax.ShapeDtypeStruct((width, hidden), F32), jax.ShapeDtypeStruct((hidden, width), F32), jax.ShapeDtypeStruct((8, 128), F32),
                   jax.ShapeDtypeStruct((N_LATE,) + next_batch.shape[1:], BF16), jax.ShapeDtypeStruct((width, hidden), BF16), jax.ShapeDtypeStruct((hidden, width), BF16)],
        in_specs=[hbm] * 11 + [smem] * 2,
        out_specs=[hbm, hbm, hbm, pl.BlockSpec(memory_space=pltpu.VMEM), hbm, hbm, hbm],
        scratch_shapes=[
            vmem((width, hidden), F32), vmem((hidden, width), F32),
            vmem((width, hidden), F32), vmem((hidden, width), F32),
            vmem((width, hidden), F32), vmem((hidden, width), F32),
            vmem((n_tok, width), BF16), vmem((n_tok, width), BF16), vmem((n_tok, width), BF16),
            vmem((n_tok, hidden), BF16), vmem((n_tok, hidden), F32), vmem((n_tok, hidden), BF16),
            vmem((width, hidden), BF16), vmem((hidden, width), BF16),
            vmem((2, width // 4, hidden), F32), vmem((2, hidden // 4, width), F32),
            vmem((width // 4, hidden), F32), vmem((hidden // 4, width), F32),
            vmem((2, width, hidden), F32), vmem((2, hidden, width), F32),
            vmem((width, hidden), BF16), vmem((hidden, width), BF16),
            vmem((width, hidden), BF16), vmem((hidden, width), BF16),
            vmem((width, hidden), BF16), vmem((hidden, width), BF16),
            vmem((16, 8, 128), F32),
            vmem(next_batch.shape, BF16), vmem(next_batch.shape, BF16), vmem(next_batch.shape, BF16),
            dma((10,)), dma((N_CHUNK,)), dma((N_CHUNK,)), dma((12,)), dma((12,)), dma((16,)), dma((16,)), dma((18 * N_PIECE,)), dma((18 * N_PIECE,)), dma((2 * N_PIECE,)), dma((2 * N_PIECE,)),
            dma((n_micro,)), dma((n_micro,)), dma((n_micro,)), dma((n_micro,)), dma((2,)), dma((2,)),
        ],
        compiler_params=pltpu.CompilerParams(collective_id=1, has_side_effects=True, vmem_limit_bytes=63 * 1024 * 1024),
    )(master_up, master_down, m1_up, m1_down, m2_up, m2_down, grad_up, grad_down, acts, loss_grad, next_batch, learn_rate, max_norm)


def finish_kernel(outs_in, late_in, w_up_in, w_down_in, mean_up_in, mean_down_in, up_in, down_in, m1_up_in, m1_down_in, m2_up_in, m2_down_in, clip_ref, rate_ref,
                  outs, up_out, down_out, m1_up_out, m1_down_out, m2_up_out, m2_down_out,
                  obuf, late, w_up, w_down, upd_up, upd_down, load_sem, store_sem, micro_load, micro_store, late_load):
    stage = lax.axis_index("stage")
    n_micro = obuf.shape[0]
    last = stage == 3
    n_copied = jnp.where(last, n_micro - N_LATE, n_micro)
    per_late = -(-(n_micro - N_LATE) // N_LATE)
    up_loads = [pltpu.make_async_copy(src, upd_up.at[i], load_sem.at[i]) for i, src in enumerate((mean_up_in, up_in, m1_up_in, m2_up_in))]
    down_loads = [pltpu.make_async_copy(src, upd_down.at[i], load_sem.at[4 + i]) for i, src in enumerate((mean_down_in, down_in, m1_down_in, m2_down_in))]
    w_loads = [pltpu.make_async_copy(w_up_in, w_up, load_sem.at[8]), pltpu.make_async_copy(w_down_in, w_down, load_sem.at[9])]
    up_stores = [pltpu.make_async_copy(upd_up.at[1 + i], dst, store_sem.at[i]) for i, dst in enumerate((up_out, m1_up_out, m2_up_out))]
    down_stores = [pltpu.make_async_copy(upd_down.at[1 + i], dst, store_sem.at[3 + i]) for i, dst in enumerate((down_out, m1_down_out, m2_down_out))]

    def place(k):
        return mixed(k, n_micro)[1]

    def load_micro(k):
        i = place(k)
        return pltpu.make_async_copy(outs_in.at[i], obuf.at[i], micro_load.at[i])

    def store_micro(k):
        i = place(k)
        return pltpu.make_async_copy(obuf.at[i], outs.at[i], micro_store.at[i])

    def load_late(n):
        return pltpu.make_async_copy(late_in.at[n], late.at[n], late_load.at[n])

    for copy in up_loads:
        copy.start()

    def start_micro(k, _):
        load_micro(k).start()
        return 0

    def turn_micro(k, _):
        load_micro(k).wait()
        store_micro(k).start()
        return 0

    @pl.when(last)
    def _():
        for copy in w_loads:
            copy.start()
        for n in range(N_LATE):
            load_late(n).start()
    for copy in down_loads:
        copy.start()
    lax.fori_loop(0, n_copied, start_micro, 0)
    clip = clip_ref[0:1, 0:1]
    rate = rate_ref[0]

    def update(buf, n_rows):
        def body(t, _):
            rows = pl.ds(pl.multiple_of(t * n_rows, n_rows), n_rows)
            new = adamw_update(buf[1, rows, :], buf[2, rows, :], buf[3, rows, :], buf[0, rows, :], clip, rate)
            for i in range(3):
                buf[1 + i, rows, :] = new[i]
            return 0
        lax.fori_loop(0, buf.shape[1] // n_rows, body, 0)

    for copy in up_loads:
        copy.wait()
    update(upd_up, 32)
    for copy in up_stores:
        copy.start()
    for copy in down_loads:
        copy.wait()
    update(upd_down, 128)
    for copy in down_stores:
        copy.start()

    @pl.when(last)
    def _():
        for copy in w_loads:
            copy.wait()

        def body(n, _):
            for j in range(per_late):
                k = per_late * n + j

                @pl.when(k < n_micro - N_LATE)
                def _():
                    turn_micro(k, 0)
            load_late(n).wait()
            k = n_micro - N_LATE + n
            i = place(k)
            stage_rows(late.at[n], w_up, w_down, obuf.at[i])
            store_micro(k).start()
            return 0
        lax.fori_loop(0, N_LATE, body, 0)

    @pl.when(jnp.logical_not(last))
    def _():
        lax.fori_loop(0, n_micro, turn_micro, 0)

    def stored(k, _):
        store_micro(k).wait()
        return 0
    lax.fori_loop(0, n_micro, stored, 0)
    for copy in up_stores + down_stores:
        copy.wait()


def finish_step(outs, late, w_up, w_down, mean_up, mean_down, clip, master_up, master_down, m1_up, m1_down, m2_up, m2_down, learn_rate):
    n_micro = outs.shape[0]
    hbm = pl.BlockSpec(memory_space=pl.ANY)
    vmem = pltpu.VMEM
    dma = pltpu.SemaphoreType.DMA
    up, down = jax.ShapeDtypeStruct(master_up.shape, F32), jax.ShapeDtypeStruct(master_down.shape, F32)
    return pl.pallas_call(
        finish_kernel,
        name="finish_step",
        out_shape=[jax.ShapeDtypeStruct(outs.shape, BF16), up, down, up, down, up, down],
        in_specs=[hbm] * 12 + [pl.BlockSpec(memory_space=pltpu.VMEM), pl.BlockSpec(memory_space=pltpu.SMEM)],
        out_specs=[hbm] * 7,
        scratch_shapes=[
            vmem(outs.shape, BF16), vmem(late.shape, BF16), vmem(w_up.shape, BF16), vmem(w_down.shape, BF16),
            vmem((4,) + master_up.shape, F32), vmem((4,) + master_down.shape, F32),
            dma((10,)), dma((6,)), dma((n_micro,)), dma((n_micro,)), dma((N_LATE,)),
        ],
        compiler_params=pltpu.CompilerParams(vmem_limit_bytes=56 * 1024 * 1024),
    )(outs, late, w_up, w_down, mean_up, mean_down, master_up, master_down, m1_up, m1_down, m2_up, m2_down, clip, learn_rate)


def solution(mesh):
    def local_step(master_up, master_down, mom1_up, mom1_down, mom2_up, mom2_down, grad_up, grad_down, stage_acts, loss_grad, next_batch, learn_rate, max_norm):
        stage_outs, gbar_up, gbar_down, clip, late, w_up, w_down = fused_step(
            master_up[0], master_down[0], mom1_up[0], mom1_down[0], mom2_up[0], mom2_down[0], grad_up[0, 0], grad_down[0, 0],
            stage_acts[0], loss_grad, next_batch, learn_rate.reshape(1), max_norm.reshape(1))
        stage_outs, new_up, new_down, new_m1_up, new_m1_down, new_m2_up, new_m2_down = finish_step(
            stage_outs, late, w_up, w_down, gbar_up, gbar_down, clip, master_up[0], master_down[0], mom1_up[0], mom1_down[0], mom2_up[0], mom2_down[0], learn_rate.reshape(1))
        return (new_up[None], new_down[None], new_m1_up[None], new_m1_down[None], new_m2_up[None], new_m2_down[None], stage_outs[None])

    w_spec = P('stage', None, None)
    g_spec = P('data', 'stage', None, None)
    in_specs = (w_spec, w_spec, w_spec, w_spec, w_spec, w_spec, g_spec, g_spec, P('stage', 'data', None), P('data', None), P(None, 'data', None), P(), P())
    out_specs = (w_spec, w_spec, w_spec, w_spec, w_spec, w_spec, P('stage', None, 'data', None))
    return jax.shard_map(local_step, mesh=mesh, in_specs=in_specs, out_specs=out_specs, check_vma=False)
```

```python
import jax
import jax.numpy as jnp
from jax import lax
from jax.experimental import pallas as pl
from jax.experimental.pallas import tpu as pltpu
from jax.sharding import PartitionSpec as P

BETA1 = 0.9
BETA2 = 0.95
ADAM_EPS = 1e-8
WEIGHT_DECAY = 0.1
NORM_EPS = 1e-6
ADAM_STEP = 8
SQRT_TWO_PI = 0.7978845608028654
GELU_CUBIC = 0.044715

N_SENT = 6
N_CHUNK = 4
N_LATE = 6
N_TWICE = 3
N_PIECE = 1
MESH = pl.DeviceIdType.MESH
BF16 = jnp.bfloat16
F32 = jnp.float32


def mat_tn(left, right):
    return lax.dot_general(left, right, (((0,), (0,)), ((), ())), preferred_element_type=F32)


def mat_nt(left, right):
    return lax.dot_general(left, right, (((1,), (1,)), ((), ())), preferred_element_type=F32)


def adamw_update(master, first_mom, second_mom, grad_avg, clip_scale, learn_rate):
    scaled = clip_scale * grad_avg
    new_first = BETA1 * first_mom + (1.0 - BETA1) * scaled
    new_second = BETA2 * second_mom + (1.0 - BETA2) * scaled * scaled
    first_hat = new_first * (1.0 / (1.0 - BETA1 ** ADAM_STEP))
    second_hat = new_second * (1.0 / (1.0 - BETA2 ** ADAM_STEP))
    new_master = master - learn_rate * (first_hat / (jnp.sqrt(second_hat) + ADAM_EPS) + WEIGHT_DECAY * master)
    return new_master, new_first, new_second


def gelu_of_half(half):
    t = jnp.tanh(half * (2.0 * SQRT_TWO_PI + (8.0 * SQRT_TWO_PI * GELU_CUBIC) * (half * half)))
    return half + half * t


def stage_rows(src, up_half, down, dst):
    x = src[...]
    half = jnp.dot(x, up_half[...], preferred_element_type=F32)
    hidden = gelu_of_half(half).astype(BF16)
    y = jnp.dot(hidden, down[...], preferred_element_type=F32)
    dst[...] = (x.astype(F32) + y).astype(BF16)


def mixed(k, n_micro):
    before = lax.div(k * N_SENT, n_micro)
    is_sent = lax.div((k + 1) * N_SENT, n_micro) - before
    return is_sent, is_sent * (n_micro - N_SENT + before) + (1 - is_sent) * (k - before)


def forward_part(stage, own_ready, aux_ready, relay_mean, nb_hbm, up_own, down_own, up_aux, down_aux, up_two, down_two, out_hbm, late_hbm, nbuf, xin, yout, nb_sem, out_sem, send_sem, recv_sem, two_send, two_recv):
    n_micro = nbuf.shape[0]
    n_kept = n_micro - N_SENT

    def load(i):
        return pltpu.make_async_copy(nb_hbm.at[i], nbuf.at[i], nb_sem.at[i])

    def store(i):
        return pltpu.make_async_copy(yout.at[i], out_hbm.at[i], out_sem.at[i])

    def push(src, i, peer):
        return pltpu.make_async_remote_copy(src_ref=src.at[i], dst_ref=xin.at[i], send_sem=send_sem.at[i], recv_sem=recv_sem.at[i], device_id={"stage": peer}, device_id_type=MESH)

    def arrived(i):
        push(yout, i, stage).wait_recv()

    def rotated(j):
        return lax.rem(j + n_kept, n_micro)

    def finish_stores():
        def body(i, _):
            store(i).wait()
            return 0
        lax.fori_loop(0, n_micro, body, 0)

    def hand_over():
        return [pltpu.make_async_remote_copy(src_ref=aux, dst_ref=two, send_sem=two_send.at[i], recv_sem=two_recv.at[i], device_id={"stage": 3}, device_id_type=MESH)
                for i, (aux, two) in enumerate([(up_aux, up_two), (down_aux, down_two)])]

    def finish_sends(first, count):
        def body(i, _):
            push(yout, first + i, stage).wait_send()
            return 0
        lax.fori_loop(0, count, body, 0)

    @pl.when(stage == 0)
    def _():
        own_ready()

        def body(j, _):
            i = rotated(j)
            load(i).wait()
            stage_rows(nbuf.at[i], up_own, down_own, yout.at[i])
            push(yout, i, 1).start()
            store(i).start()
            relay_mean(j == 7)
            return 0
        lax.fori_loop(0, n_micro, body, 0)
        finish_sends(0, n_micro)
        finish_stores()

    @pl.when(stage == 1)
    def _():
        own_ready()

        def body(j, _):
            i = rotated(j)
            arrived(i)
            stage_rows(xin.at[i], up_own, down_own, yout.at[i])

            @pl.when(j < N_SENT)
            def _():
                push(yout, i, 2).start()
            store(i).start()
            relay_mean(j == 7)
            return 0
        lax.fori_loop(0, n_micro, body, 0)
        finish_sends(n_kept, N_SENT)
        finish_stores()

    @pl.when(stage == 2)
    def _():
        aux_ready()
        for copy in hand_over():
            copy.start()

        def body(k, _):
            _, i = mixed(k, n_micro)
            arrived(i)

            @pl.when(i < n_kept - N_TWICE)
            def _():
                stage_rows(xin.at[i], up_aux, down_aux, xin.at[i])
            stage_rows(xin.at[i], up_own, down_own, yout.at[i])
            push(yout, i, 3).start()
            store(i).start()
            return 0
        lax.fori_loop(0, n_micro, body, 0)
        finish_sends(0, n_micro)
        finish_stores()
        for copy in hand_over():
            copy.wait_send()

    @pl.when(stage == 3)
    def _():
        aux_ready()

        def first(j, _):
            load(j).wait()
            stage_rows(nbuf.at[j], up_aux, down_aux, nbuf.at[j])

            @pl.when(j == n_kept - N_TWICE)
            def _():
                for copy in hand_over():
                    copy.wait_recv()

            @pl.when(j >= n_kept - N_TWICE)
            def _():
                stage_rows(nbuf.at[j], up_two, down_two, nbuf.at[j])
            push(nbuf, j, 2).start()
            return 0
        lax.fori_loop(0, n_kept, first, 0)

        def body(k, _):
            _, i = mixed(k, n_micro)
            arrived(i)
            stage_rows(xin.at[i], up_own, down_own, yout.at[i])
            store(i).start()
            return 0
        lax.fori_loop(0, n_micro - N_LATE, body, 0)

        def late(k):
            _, i = mixed(k, n_micro)
            return i, pltpu.make_async_copy(xin.at[i], late_hbm.at[k - (n_micro - N_LATE)], out_sem.at[i])

        def save(k, _):
            i, copy = late(k)
            arrived(i)
            copy.start()
            return 0
        lax.fori_loop(n_micro - N_LATE, n_micro, save, 0)

        def stored(k, _):
            _, i = mixed(k, n_micro)
            store(i).wait()
            return 0
        lax.fori_loop(0, n_micro - N_LATE, stored, 0)

        def saved(k, _):
            late(k)[1].wait()
            return 0
        lax.fori_loop(n_micro - N_LATE, n_micro, saved, 0)
        finish_sends(0, n_kept)


def start_loads(stage, nb_hbm, nbuf, nb_sem):
    n_micro = nbuf.shape[0]
    n_kept = n_micro - N_SENT

    def body(j, _):
        i = lax.rem(j + n_kept, n_micro)
        pltpu.make_async_copy(nb_hbm.at[i], nbuf.at[i], nb_sem.at[i]).start()
        return 0

    @pl.when(stage == 0)
    def _():
        lax.fori_loop(0, n_micro, body, 0)

    @pl.when(stage == 3)
    def _():
        lax.fori_loop(N_SENT, n_micro, body, 0)


def step_kernel(up_hbm, down_hbm, m1_up_hbm, m1_down_hbm, m2_up_hbm, m2_down_hbm, gu_hbm, gv_hbm, acts_hbm, loss_hbm, nb_hbm, rate_ref, norm_ref,
                out_hbm, new_up_hbm, new_down_hbm, new_m1_up_hbm, new_m1_down_hbm, new_m2_up_hbm, new_m2_down_hbm, late_hbm, w_up_hbm, w_down_hbm,
                up32, down32, gu, gv, mean_up, mean_down, acts, gbuf, dxbuf, hid, slope, dpre, up_bf, down_bf,
                ru1, rv1, ru2, rv2, m_up, m_down, up_own, down_own, up_aux, down_aux, up_two, down_two, sq_all, nbuf, xin, yout,
                in_sem, g_send, g_recv, rs_send, rs_recv, sq_send, sq_recv, ag_send, ag_recv, aux_send, aux_recv,
                nb_sem, out_sem, send_sem, recv_sem, two_send, two_recv):
    stage = lax.axis_index("stage")
    data = lax.axis_index("data")
    z = lax.div(data, 2)
    y = lax.rem(data, 2)
    me = data * 4 + stage
    z_peer = 2 * (1 - z) + y
    y_peer = 2 * z + (1 - y)
    n_tok = acts.shape[0]
    chunk = n_tok // N_CHUNK

    def up_rows(zz, yy, first=0, count=64):
        return pl.ds(pl.multiple_of(128 * yy + 64 * zz + first, 32), count)

    def down_rows(zz, yy, first=0, count=256):
        return pl.ds(pl.multiple_of(512 * zz + 256 * yy + first, 128), count)

    own_up, own_down = up_rows(z, y), down_rows(z, y)
    loads = [
        pltpu.make_async_copy(acts_hbm, acts, in_sem.at[0]),
        pltpu.make_async_copy(up_hbm, up32, in_sem.at[1]),
        pltpu.make_async_copy(down_hbm, down32, in_sem.at[2]),
        pltpu.make_async_copy(gv_hbm, gv, in_sem.at[3]),
        pltpu.make_async_copy(gu_hbm, gu, in_sem.at[4]),
        pltpu.make_async_copy(m1_up_hbm, m_up.at[0], in_sem.at[5]),
        pltpu.make_async_copy(m2_up_hbm, m_up.at[1], in_sem.at[6]),
        pltpu.make_async_copy(m1_down_hbm, m_down.at[0], in_sem.at[7]),
        pltpu.make_async_copy(m2_down_hbm, m_down.at[1], in_sem.at[8]),
    ]
    load_loss = pltpu.make_async_copy(loss_hbm, gbuf, in_sem.at[9])
    for copy in loads[:2]:
        copy.start()

    @pl.when(stage == 3)
    def _():
        load_loss.start()
    loads[2].start()

    barrier = pltpu.get_barrier_semaphore()

    def greet(d, _):
        other = lax.rem(me + d, 16)
        pl.semaphore_signal(barrier, inc=1, device_id={"data": lax.div(other, 4), "stage": lax.rem(other, 4)}, device_id_type=MESH)
        return 0
    lax.fori_loop(1, 16, greet, 0)

    def chunk_rows(k):
        return pl.ds(pl.multiple_of(k * chunk, chunk), chunk)

    def pass_down(k):
        rows = chunk_rows(k)
        return pltpu.make_async_remote_copy(src_ref=dxbuf.at[rows], dst_ref=gbuf.at[rows], send_sem=g_send.at[k], recv_sem=g_recv.at[k],
                                            device_id={"stage": jnp.maximum(stage - 1, 0)}, device_id_type=MESH)

    def prepare(k):
        rows = chunk_rows(k)
        pre = jnp.dot(acts[rows, :], up_bf[...], preferred_element_type=F32)
        sq = pre * pre
        half_t = 0.5 * jnp.tanh(pre * (SQRT_TWO_PI + (SQRT_TWO_PI * GELU_CUBIC) * sq))
        prob = 0.5 + half_t
        rest = 0.5 - half_t
        hid[rows, :] = (pre * prob).astype(BF16)
        slope[rows, :] = prob + (prob * rest) * pre * (2.0 * SQRT_TWO_PI + (6.0 * SQRT_TWO_PI * GELU_CUBIC) * sq)

    def backward(k):
        rows = chunk_rows(k)

        @pl.when(stage < 3)
        def _():
            pass_down(k).wait_recv()
        grad = gbuf[rows, :]
        d_pre = (mat_nt(grad, down_bf[...]) * slope[rows, :]).astype(BF16)
        dpre[rows, :] = d_pre

        @pl.when(stage > 0)
        def _():
            dxbuf[rows, :] = (grad.astype(F32) + mat_nt(d_pre, up_bf[...])).astype(BF16)
            pass_down(k).start()

    def rs_copy(src, dst, sem, peer):
        return pltpu.make_async_remote_copy(src_ref=src, dst_ref=dst, send_sem=rs_send.at[sem], recv_sem=rs_recv.at[sem], device_id={"data": peer}, device_id_type=MESH)

    def v_first(sub, c):
        yy = (1 - y) if sub == 0 else y
        return rs_copy(gv.at[down_rows(1 - z, yy, 128 * c, 128)], rv1.at[sub, pl.ds(128 * c, 128)], 2 * sub + c, z_peer)

    def u_first(sub, c):
        zz = (1 - z) if sub == 0 else z
        return rs_copy(gu.at[up_rows(zz, 1 - y, 32 * c, 32)], ru1.at[sub, pl.ds(32 * c, 32)], 4 + 2 * sub + c, y_peer)

    def v_second(c):
        return rs_copy(gv.at[down_rows(z, 1 - y, 128 * c, 128)], rv2.at[pl.ds(128 * c, 128)], 8 + c, y_peer)

    def u_second(c):
        return rs_copy(gu.at[up_rows(1 - z, y, 32 * c, 32)], ru2.at[pl.ds(32 * c, 32)], 10 + c, z_peer)

    def add_grads(k):
        rows = chunk_rows(k)

        @pl.when(k == 0)
        def _():
            loads[3].wait()
            loads[4].wait()

        def half(h, _):
            zz = h * z + (1 - h) * (1 - z)
            yy = h * y + (1 - h) * (1 - y)
            send = (k == N_CHUNK - 1) & (h == 0)
            out = pl.ds(pl.multiple_of(512 * zz, 512), 512)
            gv[out, :] += mat_tn(hid[rows, out], gbuf[rows, :])

            @pl.when(send)
            def _():
                for sub in range(2):
                    for c in range(2):
                        v_first(sub, c).start()
            out = pl.ds(pl.multiple_of(128 * yy, 128), 128)
            gu[out, :] += mat_tn(acts[rows, out], dpre[rows, :])

            @pl.when(send)
            def _():
                for sub in range(2):
                    for c in range(2):
                        u_first(sub, c).start()
            return 0
        lax.fori_loop(0, 2, half, 0)

    def tick(t, _):
        upper = jnp.where(stage >= 2, 1, 0)
        even = 1 - lax.rem(t, 2)
        early = jnp.where(t < N_CHUNK, 1, 0)
        late = jnp.where(t >= 2 * N_CHUNK, 1, 0)
        is_prep = upper * even * (1 - late) + (1 - upper) * early
        is_grad = upper * late + (1 - upper) * (1 - early) * (1 - even)
        k = upper * (late * (t - 2 * N_CHUNK) + (1 - late) * lax.div(t, 2)) + (1 - upper) * (early * t + (1 - early) * lax.div(t - N_CHUNK, 2))

        @pl.when(is_prep == 1)
        def _():
            prepare(k)

        @pl.when(is_prep + is_grad == 0)
        def _():
            backward(k)

        @pl.when(is_grad == 1)
        def _():
            add_grads(k)
        return 0

    loads[0].wait()
    loads[1].wait()
    up_bf[...] = up32[...].astype(BF16)
    prepare(0)
    loads[2].wait()
    for copy in loads[3:]:
        copy.start()
    start_loads(stage, nb_hbm, nbuf, nb_sem)
    down_bf[...] = down32[...].astype(BF16)
    pl.semaphore_wait(barrier, 15)

    @pl.when(stage == 3)
    def _():
        load_loss.wait()
    lax.fori_loop(1, 3 * N_CHUNK, tick, 0)

    for c in range(2):
        v_first(0, c).wait_recv()
        rows = down_rows(z, 1 - y, 128 * c, 128)
        gv[rows, :] += rv1[0, 128 * c:128 * (c + 1), :]
        v_second(c).start()
        u_first(0, c).wait_recv()
        rows = up_rows(1 - z, y, 32 * c, 32)
        gu[rows, :] += ru1[0, 32 * c:32 * (c + 1), :]
        u_second(c).start()
    acc = jnp.zeros((8, 128), F32)

    def fold(tile, acc):
        sq = tile * tile
        sq = jnp.sum(sq.reshape(sq.shape[0] // 8, 8, sq.shape[1]), axis=0)
        for i in range(0, sq.shape[1], 128):
            acc = acc + sq[:, i:i + 128]
        return acc

    for c in range(2):
        v_first(1, c).wait_recv()
        v_second(c).wait_recv()
        rows = down_rows(z, y, 128 * c, 128)
        mean = (gv[rows, :] + rv1[1, 128 * c:128 * (c + 1), :] + rv2[128 * c:128 * (c + 1), :]) * 0.25
        mean_down[rows, :] = mean
        acc = fold(mean, acc)
        u_first(1, c).wait_recv()
        u_second(c).wait_recv()
        rows = up_rows(z, y, 32 * c, 32)
        mean = (gu[rows, :] + ru1[1, 32 * c:32 * (c + 1), :] + ru2[32 * c:32 * (c + 1), :]) * 0.25
        mean_up[rows, :] = mean
        acc = fold(mean, acc)

    up_piece, down_piece = 64 // N_PIECE, 256 // N_PIECE

    def gather(which, up, down):
        def copy(ref, rows, sem, piece, peer):
            sem = (which * 6 + sem) * N_PIECE + piece
            return pltpu.make_async_remote_copy(src_ref=ref.at[rows], dst_ref=ref.at[rows], send_sem=ag_send.at[sem], recv_sem=ag_recv.at[sem],
                                                device_id={"data": peer}, device_id_type=MESH)

        def up_copy(zz, yy, sem, p, peer):
            return copy(up, up_rows(zz, yy, up_piece * p, up_piece), sem, p, peer)

        def down_copy(zz, yy, sem, p, peer):
            return copy(down, down_rows(zz, yy, down_piece * p, down_piece), sem, p, peer)

        def up_sends(p):
            return [up_copy(z, y, 0, p, z_peer), up_copy(z, y, 1, p, y_peer)]

        def down_sends(p):
            return [down_copy(z, y, 3, p, y_peer), down_copy(z, y, 4, p, z_peer)]

        def relays(p):
            return [(up_copy(1 - z, y, 0, p, z_peer), up_copy(1 - z, y, 2, p, y_peer)), (down_copy(z, 1 - y, 3, p, y_peer), down_copy(z, 1 - y, 5, p, z_peer))]

        def begin(fed=None):
            for p in range(N_PIECE):
                for i, sends in enumerate((up_sends(p), down_sends(p))):
                    if fed is not None:
                        fed(p)[i].wait_recv()
                    for c in sends:
                        c.start()

        def relay():
            for p in range(N_PIECE):
                for arrived, onward in relays(p):
                    arrived.wait_recv()
                    onward.start()

        def finish():
            for p in range(N_PIECE):
                for c in (up_copy(z, 1 - y, 1, p, y_peer), down_copy(1 - z, y, 4, p, z_peer), up_copy(1 - z, 1 - y, 2, p, y_peer), down_copy(1 - z, 1 - y, 5, p, z_peer)):
                    c.wait_recv()

        def drain():
            for p in range(N_PIECE):
                for c in up_sends(p) + down_sends(p) + [onward for _, onward in relays(p)]:
                    c.wait_send()
        return begin, relay, finish, drain

    own_begin, own_relay, own_finish, own_drain = gather(0, up_own, down_own)
    aux_begin, aux_relay, aux_finish, aux_drain = gather(1, up_aux, down_aux)
    mean_begin, mean_relay, mean_finish, mean_drain = gather(2, mean_up, mean_down)

    def sq_copy(other, slot):
        return pltpu.make_async_remote_copy(src_ref=sq_all.at[slot], dst_ref=sq_all.at[slot], send_sem=sq_send.at[other], recv_sem=sq_recv.at[slot],
                                            device_id={"data": lax.div(other, 4), "stage": lax.rem(other, 4)}, device_id_type=MESH)

    sq_all[me] = acc

    def tell(d, _):
        sq_copy(lax.rem(me + d, 16), me).start()
        return 0
    lax.fori_loop(1, 16, tell, 0)
    for copy in loads[5:]:
        copy.wait()

    @pl.when(stage >= 2)
    def _():
        mean_begin()
        mean_relay()
        mean_finish()

    def hear(d, _):
        other = lax.rem(me + d, 16)
        sq_copy(other, other).wait_recv()
        return 0
    lax.fori_loop(1, 16, hear, 0)
    total = sq_all[0]
    for i in range(1, 16):
        total = total + sq_all[i]
    total = jnp.sum(jnp.sum(total, axis=0, keepdims=True), axis=1, keepdims=True)
    clip = jnp.minimum(1.0, norm_ref[0] / (jnp.sqrt(total) + NORM_EPS))

    rate = rate_ref[0]
    whole = jnp.where(stage >= 2, 1, 0)

    def renew(rows, master, moments, mean, weights, scale, first, full):
        new = adamw_update(master[rows, :], moments[0, rows, :], moments[1, rows, :], mean[rows, :], clip, rate)
        if first:
            weights[rows, :] = new[0].astype(BF16) * jnp.asarray(scale, BF16)

        @pl.when(full)
        def _():
            master[rows, :] = new[0]
            moments[0, rows, :] = new[1]
            moments[1, rows, :] = new[2]

    def renew_block(up_block, down_block, first, full):
        renew(pl.ds(pl.multiple_of(64 * up_block, 64), 64), up32, m_up, mean_up, up_own, 0.5, first, full)
        renew(pl.ds(pl.multiple_of(256 * down_block, 256), 256), down32, m_down, mean_down, down_own, 1.0, first, full)

    def renew_first(t, _):
        renew_block(whole * t + (1 - whole) * (2 * y + z), whole * t + (1 - whole) * (2 * z + y), True, whole == 1)
        return 0

    def renew_rest(t, _):
        renew_block(t, t, False, t >= 0)
        return 0

    new_stores = [pltpu.make_async_copy(src, dst, in_sem.at[i]) for i, (src, dst) in enumerate((
        (up32, new_up_hbm), (down32, new_down_hbm), (m_up.at[0], new_m1_up_hbm), (m_down.at[0], new_m1_down_hbm), (m_up.at[1], new_m2_up_hbm), (m_down.at[1], new_m2_down_hbm)))]
    lax.fori_loop(0, 1 + 3 * whole, renew_first, 0)

    def feed(p):
        parts = [(up_own, up_aux, up_rows(z, y, up_piece * p, up_piece)), (down_own, down_aux, down_rows(z, y, down_piece * p, down_piece))]
        return [pltpu.make_async_remote_copy(src_ref=own.at[rows], dst_ref=aux.at[rows], send_sem=aux_send.at[2 * p + i], recv_sem=aux_recv.at[2 * p + i], device_id={"stage": 3 - stage}, device_id_type=MESH)
                for i, (own, aux, rows) in enumerate(parts)]

    @pl.when(stage < 2)
    def _():
        for p in range(N_PIECE):
            for c in feed(p):
                c.start()
        own_begin()
        own_relay()
        mean_begin()

    @pl.when(stage >= 2)
    def _():
        for copy in new_stores:
            copy.start()
        aux_begin(feed)
        aux_relay()

    def relay_mean(now):
        @pl.when(now)
        def _():
            mean_relay()

    forward_part(stage, own_finish, aux_finish, relay_mean, nb_hbm, up_own, down_own, up_aux, down_aux, up_two, down_two, out_hbm, late_hbm, nbuf, xin, yout, nb_sem, out_sem, send_sem, recv_sem, two_send, two_recv)

    @pl.when(stage < 2)
    def _():
        mean_finish()
        lax.fori_loop(0, 4, renew_rest, 0)
        for copy in new_stores:
            copy.start()
    store_w_up = pltpu.make_async_copy(up_own, w_up_hbm, in_sem.at[6])
    store_w_down = pltpu.make_async_copy(down_own, w_down_hbm, in_sem.at[7])
    store_w_up.start()
    store_w_down.start()

    @pl.when(stage > 0)
    def _():
        for k in range(N_CHUNK):
            pass_down(k).wait_send()
    for c in range(2):
        for sub in range(2):
            v_first(sub, c).wait_send()
            u_first(sub, c).wait_send()
        v_second(c).wait_send()
        u_second(c).wait_send()

    def told(d, _):
        sq_copy(lax.rem(me + d, 16), me).wait_send()
        return 0
    lax.fori_loop(1, 16, told, 0)
    mean_drain()

    @pl.when(stage < 2)
    def _():
        own_drain()
        for p in range(N_PIECE):
            for c in feed(p):
                c.wait_send()

    @pl.when(stage >= 2)
    def _():
        aux_drain()
    for copy in new_stores:
        copy.wait()
    store_w_up.wait()
    store_w_down.wait()


def fused_step(master_up, master_down, m1_up, m1_down, m2_up, m2_down, grad_up, grad_down, acts, loss_grad, next_batch, learn_rate, max_norm):
    n_micro = next_batch.shape[0]
    n_tok, width = acts.shape
    hidden = master_up.shape[1]
    hbm = pl.BlockSpec(memory_space=pl.ANY)
    smem = pl.BlockSpec(memory_space=pltpu.SMEM)
    vmem = pltpu.VMEM
    dma = pltpu.SemaphoreType.DMA
    return pl.pallas_call(
        step_kernel,
        name="pipeline_step",
        out_shape=[jax.ShapeDtypeStruct(next_batch.shape, BF16)] + [jax.ShapeDtypeStruct((width, hidden), F32), jax.ShapeDtypeStruct((hidden, width), F32)] * 3 + [
            jax.ShapeDtypeStruct((N_LATE,) + next_batch.shape[1:], BF16), jax.ShapeDtypeStruct((width, hidden), BF16), jax.ShapeDtypeStruct((hidden, width), BF16)],
        in_specs=[hbm] * 11 + [smem] * 2,
        out_specs=[hbm] * 10,
        scratch_shapes=[
            vmem((width, hidden), F32), vmem((hidden, width), F32),
            vmem((width, hidden), F32), vmem((hidden, width), F32),
            vmem((width, hidden), F32), vmem((hidden, width), F32),
            vmem((n_tok, width), BF16), vmem((n_tok, width), BF16), vmem((n_tok, width), BF16),
            vmem((n_tok, hidden), BF16), vmem((n_tok, hidden), F32), vmem((n_tok, hidden), BF16),
            vmem((width, hidden), BF16), vmem((hidden, width), BF16),
            vmem((2, width // 4, hidden), F32), vmem((2, hidden // 4, width), F32),
            vmem((width // 4, hidden), F32), vmem((hidden // 4, width), F32),
            vmem((2, width, hidden), F32), vmem((2, hidden, width), F32),
            vmem((width, hidden), BF16), vmem((hidden, width), BF16),
            vmem((width, hidden), BF16), vmem((hidden, width), BF16),
            vmem((width, hidden), BF16), vmem((hidden, width), BF16),
            vmem((16, 8, 128), F32),
            vmem(next_batch.shape, BF16), vmem(next_batch.shape, BF16), vmem(next_batch.shape, BF16),
            dma((10,)), dma((N_CHUNK,)), dma((N_CHUNK,)), dma((12,)), dma((12,)), dma((16,)), dma((16,)), dma((18 * N_PIECE,)), dma((18 * N_PIECE,)), dma((2 * N_PIECE,)), dma((2 * N_PIECE,)),
            dma((n_micro,)), dma((n_micro,)), dma((n_micro,)), dma((n_micro,)), dma((2,)), dma((2,)),
        ],
        compiler_params=pltpu.CompilerParams(collective_id=1, has_side_effects=True, vmem_limit_bytes=63 * 1024 * 1024),
    )(master_up, master_down, m1_up, m1_down, m2_up, m2_down, grad_up, grad_down, acts, loss_grad, next_batch, learn_rate, max_norm)


def finish_kernel(outs_in, late_in, w_up_in, w_down_in, *refs):
    news_in, outs, news_out = refs[:6], refs[6], refs[7:13]
    obuf, late, w_up, w_down, upd_up, upd_down, load_sem, store_sem, micro_load, micro_store, late_load = refs[13:]
    stage = lax.axis_index("stage")
    n_micro = obuf.shape[0]
    last = stage == 3
    n_copied = jnp.where(last, n_micro - N_LATE, n_micro)
    per_late = -(-(n_micro - N_LATE) // N_LATE)
    slots = [buf.at[i] for i in range(3) for buf in (upd_up, upd_down)]
    loads = [pltpu.make_async_copy(src, slot, load_sem.at[i]) for i, (src, slot) in enumerate(zip(news_in, slots))]
    stores = [pltpu.make_async_copy(slot, dst, store_sem.at[i]) for i, (slot, dst) in enumerate(zip(slots, news_out))]
    w_loads = [pltpu.make_async_copy(w_up_in, w_up, load_sem.at[6]), pltpu.make_async_copy(w_down_in, w_down, load_sem.at[7])]

    def place(k):
        return mixed(k, n_micro)[1]

    def load_micro(k):
        i = place(k)
        return pltpu.make_async_copy(outs_in.at[i], obuf.at[i], micro_load.at[i])

    def store_micro(k):
        i = place(k)
        return pltpu.make_async_copy(obuf.at[i], outs.at[i], micro_store.at[i])

    def load_late(n):
        return pltpu.make_async_copy(late_in.at[n], late.at[n], late_load.at[n])

    def start_micro(k, _):
        load_micro(k).start()
        return 0

    def turn_micro(k, _):
        load_micro(k).wait()
        store_micro(k).start()
        return 0

    def start_late(n, _):
        load_late(n).start()
        return 0

    @pl.when(last)
    def _():
        for copy in w_loads:
            copy.start()
        lax.fori_loop(0, N_LATE, start_late, 0)
    for copy in loads:
        copy.start()
    lax.fori_loop(0, n_copied, start_micro, 0)

    @pl.when(last)
    def _():
        for copy in w_loads:
            copy.wait()

        def body(n, _):
            load_late(n).wait()
            k = n_micro - N_LATE + n
            stage_rows(late.at[n], w_up, w_down, obuf.at[place(k)])
            store_micro(k).start()

            @pl.when(n == 0)
            def _():
                for load, store in zip(loads, stores):
                    load.wait()
                    store.start()
            for j in range(per_late):
                k = per_late * n + j

                @pl.when(k < n_micro - N_LATE)
                def _():
                    turn_micro(k, 0)
            return 0
        lax.fori_loop(0, N_LATE, body, 0)

    @pl.when(jnp.logical_not(last))
    def _():
        for load, store in zip(loads, stores):
            load.wait()
            store.start()
        lax.fori_loop(0, n_micro, turn_micro, 0)

    def stored(k, _):
        store_micro(k).wait()
        return 0
    lax.fori_loop(0, n_micro, stored, 0)
    for copy in stores:
        copy.wait()


def finish_step(outs, late, w_up, w_down, *news):
    n_micro = outs.shape[0]
    hbm = pl.BlockSpec(memory_space=pl.ANY)
    vmem = pltpu.VMEM
    dma = pltpu.SemaphoreType.DMA
    return pl.pallas_call(
        finish_kernel,
        name="finish_step",
        out_shape=[jax.ShapeDtypeStruct(outs.shape, BF16)] + [jax.ShapeDtypeStruct(new.shape, F32) for new in news],
        in_specs=[hbm] * 10,
        out_specs=[hbm] * 7,
        scratch_shapes=[
            vmem(outs.shape, BF16), vmem(late.shape, BF16), vmem(w_up.shape, BF16), vmem(w_down.shape, BF16),
            vmem((3,) + news[0].shape, F32), vmem((3,) + news[1].shape, F32),
            dma((8,)), dma((6,)), dma((n_micro,)), dma((n_micro,)), dma((N_LATE,)),
        ],
        compiler_params=pltpu.CompilerParams(vmem_limit_bytes=56 * 1024 * 1024),
    )(outs, late, w_up, w_down, *news)


def solution(mesh):
    def local_step(master_up, master_down, mom1_up, mom1_down, mom2_up, mom2_down, grad_up, grad_down, stage_acts, loss_grad, next_batch, learn_rate, max_norm):
        stage_outs, *news, late, w_up, w_down = fused_step(
            master_up[0], master_down[0], mom1_up[0], mom1_down[0], mom2_up[0], mom2_down[0], grad_up[0, 0], grad_down[0, 0],
            stage_acts[0], loss_grad, next_batch, learn_rate.reshape(1), max_norm.reshape(1))
        stage_outs, new_up, new_down, new_m1_up, new_m1_down, new_m2_up, new_m2_down = finish_step(stage_outs, late, w_up, w_down, *news)
        return (new_up[None], new_down[None], new_m1_up[None], new_m1_down[None], new_m2_up[None], new_m2_down[None], stage_outs[None])

    w_spec = P('stage', None, None)
    g_spec = P('data', 'stage', None, None)
    in_specs = (w_spec, w_spec, w_spec, w_spec, w_spec, w_spec, g_spec, g_spec, P('stage', 'data', None), P('data', None), P(None, 'data', None), P(), P())
    out_specs = (w_spec, w_spec, w_spec, w_spec, w_spec, w_spec, P('stage', None, 'data', None))
    return jax.shard_map(local_step, mesh=mesh, in_specs=in_specs, out_specs=out_specs, check_vma=False)
```

```python
import jax
import jax.numpy as jnp
from jax import lax
from jax.experimental import pallas as pl
from jax.experimental.pallas import tpu as pltpu
from jax.sharding import PartitionSpec as P

BETA1 = 0.9
BETA2 = 0.95
ADAM_EPS = 1e-8
WEIGHT_DECAY = 0.1
NORM_EPS = 1e-6
ADAM_STEP = 8
SQRT_TWO_PI = 0.7978845608028654
GELU_CUBIC = 0.044715

N_SENT = 5
N_CHUNK = 4
N_LATE = 6
N_TWICE = 3
N_PIECE = 1
MESH = pl.DeviceIdType.MESH
BF16 = jnp.bfloat16
F32 = jnp.float32


def mat_tn(left, right):
    return lax.dot_general(left, right, (((0,), (0,)), ((), ())), preferred_element_type=F32)


def mat_nt(left, right):
    return lax.dot_general(left, right, (((1,), (1,)), ((), ())), preferred_element_type=F32)


def adamw_update(master, first_mom, second_mom, grad_avg, clip_scale, learn_rate):
    scaled = clip_scale * grad_avg
    new_first = BETA1 * first_mom + (1.0 - BETA1) * scaled
    new_second = BETA2 * second_mom + (1.0 - BETA2) * scaled * scaled
    first_hat = new_first * (1.0 / (1.0 - BETA1 ** ADAM_STEP))
    second_hat = new_second * (1.0 / (1.0 - BETA2 ** ADAM_STEP))
    new_master = master - learn_rate * (first_hat / (jnp.sqrt(second_hat) + ADAM_EPS) + WEIGHT_DECAY * master)
    return new_master, new_first, new_second


def gelu_of_half(half):
    t = jnp.tanh(half * (2.0 * SQRT_TWO_PI + (8.0 * SQRT_TWO_PI * GELU_CUBIC) * (half * half)))
    return half + half * t


def stage_rows(src, up_half, down, dst):
    x = src[...]
    half = jnp.dot(x, up_half[...], preferred_element_type=F32)
    hidden = gelu_of_half(half).astype(BF16)
    y = jnp.dot(hidden, down[...], preferred_element_type=F32)
    dst[...] = (x.astype(F32) + y).astype(BF16)


def mixed(k, n_micro):
    before = lax.div(k * N_SENT, n_micro)
    is_sent = lax.div((k + 1) * N_SENT, n_micro) - before
    return is_sent, is_sent * (n_micro - N_SENT + before) + (1 - is_sent) * (k - before)


def forward_part(stage, own_ready, aux_ready, relay_mean, nb_hbm, up_own, down_own, up_aux, down_aux, up_two, down_two, out_hbm, late_hbm, nbuf, xin, yout, nb_sem, out_sem, send_sem, recv_sem, two_send, two_recv):
    n_micro = nbuf.shape[0]
    n_kept = n_micro - N_SENT

    def load(i):
        return pltpu.make_async_copy(nb_hbm.at[i], nbuf.at[i], nb_sem.at[i])

    def store(i):
        return pltpu.make_async_copy(yout.at[i], out_hbm.at[i], out_sem.at[i])

    def push(src, i, peer):
        return pltpu.make_async_remote_copy(src_ref=src.at[i], dst_ref=xin.at[i], send_sem=send_sem.at[i], recv_sem=recv_sem.at[i], device_id={"stage": peer}, device_id_type=MESH)

    def arrived(i):
        push(yout, i, stage).wait_recv()

    def rotated(j):
        return lax.rem(j + n_kept, n_micro)

    def finish_stores():
        def body(i, _):
            store(i).wait()
            return 0
        lax.fori_loop(0, n_micro, body, 0)

    def hand_over():
        return [pltpu.make_async_remote_copy(src_ref=aux, dst_ref=two, send_sem=two_send.at[i], recv_sem=two_recv.at[i], device_id={"stage": 3}, device_id_type=MESH)
                for i, (aux, two) in enumerate([(up_aux, up_two), (down_aux, down_two)])]

    def finish_sends(first, count):
        def body(i, _):
            push(yout, first + i, stage).wait_send()
            return 0
        lax.fori_loop(0, count, body, 0)

    @pl.when(stage == 0)
    def _():
        own_ready()

        def body(j, _):
            i = rotated(j)
            load(i).wait()
            stage_rows(nbuf.at[i], up_own, down_own, yout.at[i])
            push(yout, i, 1).start()
            store(i).start()
            relay_mean(j == 7)
            return 0
        lax.fori_loop(0, n_micro, body, 0)
        finish_sends(0, n_micro)
        finish_stores()

    @pl.when(stage == 1)
    def _():
        own_ready()

        def body(j, _):
            i = rotated(j)
            arrived(i)
            stage_rows(xin.at[i], up_own, down_own, yout.at[i])

            @pl.when(j < N_SENT)
            def _():
                push(yout, i, 2).start()
            store(i).start()
            relay_mean(j == 7)
            return 0
        lax.fori_loop(0, n_micro, body, 0)
        finish_stores()

    @pl.when(stage == 2)
    def _():
        aux_ready()
        for copy in hand_over():
            copy.start()

        def body(k, _):
            _, i = mixed(k, n_micro)
            arrived(i)

            @pl.when(i < n_kept - N_TWICE)
            def _():
                stage_rows(xin.at[i], up_aux, down_aux, xin.at[i])
            stage_rows(xin.at[i], up_own, down_own, yout.at[i])
            push(yout, i, 3).start()
            store(i).start()
            return 0
        lax.fori_loop(0, n_micro, body, 0)
        finish_sends(0, n_micro)
        finish_stores()
        for copy in hand_over():
            copy.wait_send()

    @pl.when(stage == 3)
    def _():
        aux_ready()

        def first(j, _):
            load(j).wait()
            stage_rows(nbuf.at[j], up_aux, down_aux, nbuf.at[j])

            @pl.when(j == n_kept - N_TWICE)
            def _():
                for copy in hand_over():
                    copy.wait_recv()

            @pl.when(j >= n_kept - N_TWICE)
            def _():
                stage_rows(nbuf.at[j], up_two, down_two, nbuf.at[j])
            push(nbuf, j, 2).start()
            return 0
        lax.fori_loop(0, n_kept, first, 0)

        def body(k, _):
            _, i = mixed(k, n_micro)
            arrived(i)
            stage_rows(xin.at[i], up_own, down_own, yout.at[i])
            store(i).start()
            return 0
        lax.fori_loop(0, n_micro - N_LATE, body, 0)

        def late(k):
            _, i = mixed(k, n_micro)
            return i, pltpu.make_async_copy(xin.at[i], late_hbm.at[k - (n_micro - N_LATE)], out_sem.at[i])

        def save(k, _):
            i, copy = late(k)
            arrived(i)
            copy.start()
            return 0
        lax.fori_loop(n_micro - N_LATE, n_micro, save, 0)

        def stored(k, _):
            _, i = mixed(k, n_micro)
            store(i).wait()
            return 0
        lax.fori_loop(0, n_micro - N_LATE, stored, 0)

        def saved(k, _):
            late(k)[1].wait()
            return 0
        lax.fori_loop(n_micro - N_LATE, n_micro, saved, 0)
        finish_sends(0, n_kept)


def start_loads(stage, nb_hbm, nbuf, nb_sem):
    n_micro = nbuf.shape[0]
    n_kept = n_micro - N_SENT

    def body(j, _):
        i = lax.rem(j + n_kept, n_micro)
        pltpu.make_async_copy(nb_hbm.at[i], nbuf.at[i], nb_sem.at[i]).start()
        return 0

    @pl.when(stage == 0)
    def _():
        lax.fori_loop(0, n_micro, body, 0)

    @pl.when(stage == 3)
    def _():
        lax.fori_loop(N_SENT, n_micro, body, 0)


def step_kernel(up_hbm, down_hbm, m1_up_hbm, m1_down_hbm, m2_up_hbm, m2_down_hbm, gu_hbm, gv_hbm, acts_hbm, loss_hbm, nb_hbm, rate_ref, norm_ref,
                out_hbm, new_up_hbm, new_down_hbm, new_m1_up_hbm, new_m1_down_hbm, new_m2_up_hbm, new_m2_down_hbm, late_hbm, w_up_hbm, w_down_hbm,
                up32, down32, gu, gv, mean_up, mean_down, acts, gbuf, dxbuf, hid, slope, dpre, up_bf, down_bf,
                ru1, rv1, ru2, rv2, m_up, m_down, up_own, down_own, up_aux, down_aux, up_two, down_two, sq_all, nbuf, xin, yout,
                in_sem, g_send, g_recv, rs_send, rs_recv, sq_send, sq_recv, ag_send, ag_recv, aux_send, aux_recv,
                nb_sem, out_sem, send_sem, recv_sem, two_send, two_recv):
    stage = lax.axis_index("stage")
    data = lax.axis_index("data")
    z = lax.div(data, 2)
    y = lax.rem(data, 2)
    me = data * 4 + stage
    z_peer = 2 * (1 - z) + y
    y_peer = 2 * z + (1 - y)
    n_tok = acts.shape[0]
    chunk = n_tok // N_CHUNK

    def up_rows(zz, yy, first=0, count=64):
        return pl.ds(pl.multiple_of(128 * yy + 64 * zz + first, 32), count)

    def down_rows(zz, yy, first=0, count=256):
        return pl.ds(pl.multiple_of(512 * zz + 256 * yy + first, 128), count)

    own_up, own_down = up_rows(z, y), down_rows(z, y)
    loads = [
        pltpu.make_async_copy(acts_hbm, acts, in_sem.at[0]),
        pltpu.make_async_copy(up_hbm, up32, in_sem.at[1]),
        pltpu.make_async_copy(down_hbm, down32, in_sem.at[2]),
        pltpu.make_async_copy(gv_hbm, gv, in_sem.at[3]),
        pltpu.make_async_copy(gu_hbm, gu, in_sem.at[4]),
        pltpu.make_async_copy(m1_up_hbm, m_up.at[0], in_sem.at[5]),
        pltpu.make_async_copy(m2_up_hbm, m_up.at[1], in_sem.at[6]),
        pltpu.make_async_copy(m1_down_hbm, m_down.at[0], in_sem.at[7]),
        pltpu.make_async_copy(m2_down_hbm, m_down.at[1], in_sem.at[8]),
    ]
    load_loss = pltpu.make_async_copy(loss_hbm, gbuf, in_sem.at[9])
    for copy in loads[:2]:
        copy.start()

    @pl.when(stage == 3)
    def _():
        load_loss.start()
    loads[2].start()

    barrier = pltpu.get_barrier_semaphore()

    def greet(d, _):
        other = lax.rem(me + d, 16)
        pl.semaphore_signal(barrier, inc=1, device_id={"data": lax.div(other, 4), "stage": lax.rem(other, 4)}, device_id_type=MESH)
        return 0
    lax.fori_loop(1, 16, greet, 0)

    def chunk_rows(k):
        return pl.ds(pl.multiple_of(k * chunk, chunk), chunk)

    def pass_down(k):
        rows = chunk_rows(k)
        return pltpu.make_async_remote_copy(src_ref=dxbuf.at[rows], dst_ref=gbuf.at[rows], send_sem=g_send.at[k], recv_sem=g_recv.at[k],
                                            device_id={"stage": jnp.maximum(stage - 1, 0)}, device_id_type=MESH)

    def prepare(k):
        rows = chunk_rows(k)
        pre = jnp.dot(acts[rows, :], up_bf[...], preferred_element_type=F32)
        sq = pre * pre
        half_t = 0.5 * jnp.tanh(pre * (SQRT_TWO_PI + (SQRT_TWO_PI * GELU_CUBIC) * sq))
        prob = 0.5 + half_t
        rest = 0.5 - half_t
        hid[rows, :] = (pre * prob).astype(BF16)
        slope[rows, :] = prob + (prob * rest) * pre * (2.0 * SQRT_TWO_PI + (6.0 * SQRT_TWO_PI * GELU_CUBIC) * sq)

    def backward(k):
        rows = chunk_rows(k)

        @pl.when(stage < 3)
        def _():
            pass_down(k).wait_recv()
        grad = gbuf[rows, :]
        d_pre = (mat_nt(grad, down_bf[...]) * slope[rows, :]).astype(BF16)
        dpre[rows, :] = d_pre

        @pl.when(stage > 0)
        def _():
            dxbuf[rows, :] = (grad.astype(F32) + mat_nt(d_pre, up_bf[...])).astype(BF16)
            pass_down(k).start()

    def rs_copy(src, dst, sem, peer):
        return pltpu.make_async_remote_copy(src_ref=src, dst_ref=dst, send_sem=rs_send.at[sem], recv_sem=rs_recv.at[sem], device_id={"data": peer}, device_id_type=MESH)

    def v_first(sub, c):
        yy = (1 - y) if sub == 0 else y
        return rs_copy(gv.at[down_rows(1 - z, yy, 128 * c, 128)], rv1.at[sub, pl.ds(128 * c, 128)], 2 * sub + c, z_peer)

    def u_first(sub, c):
        zz = (1 - z) if sub == 0 else z
        return rs_copy(gu.at[up_rows(zz, 1 - y, 32 * c, 32)], ru1.at[sub, pl.ds(32 * c, 32)], 4 + 2 * sub + c, y_peer)

    def v_second(c):
        return rs_copy(gv.at[down_rows(z, 1 - y, 128 * c, 128)], rv2.at[pl.ds(128 * c, 128)], 8 + c, y_peer)

    def u_second(c):
        return rs_copy(gu.at[up_rows(1 - z, y, 32 * c, 32)], ru2.at[pl.ds(32 * c, 32)], 10 + c, z_peer)

    def add_grads(k):
        rows = chunk_rows(k)

        @pl.when(k == 0)
        def _():
            loads[3].wait()
            loads[4].wait()

        def half(h, _):
            zz = h * z + (1 - h) * (1 - z)
            yy = h * y + (1 - h) * (1 - y)
            send = (k == N_CHUNK - 1) & (h == 0)
            out = pl.ds(pl.multiple_of(512 * zz, 512), 512)
            gv[out, :] += mat_tn(hid[rows, out], gbuf[rows, :])

            @pl.when(send)
            def _():
                for sub in range(2):
                    for c in range(2):
                        v_first(sub, c).start()
            out = pl.ds(pl.multiple_of(128 * yy, 128), 128)
            gu[out, :] += mat_tn(acts[rows, out], dpre[rows, :])

            @pl.when(send)
            def _():
                for sub in range(2):
                    for c in range(2):
                        u_first(sub, c).start()
            return 0
        lax.fori_loop(0, 2, half, 0)

    def tick(t, _):
        upper = jnp.where(stage >= 2, 1, 0)
        even = 1 - lax.rem(t, 2)
        early = jnp.where(t < N_CHUNK, 1, 0)
        late = jnp.where(t >= 2 * N_CHUNK, 1, 0)
        is_prep = upper * even * (1 - late) + (1 - upper) * early
        is_grad = upper * late + (1 - upper) * (1 - early) * (1 - even)
        k = upper * (late * (t - 2 * N_CHUNK) + (1 - late) * lax.div(t, 2)) + (1 - upper) * (early * t + (1 - early) * lax.div(t - N_CHUNK, 2))

        @pl.when(is_prep == 1)
        def _():
            prepare(k)

        @pl.when(is_prep + is_grad == 0)
        def _():
            backward(k)

        @pl.when(is_grad == 1)
        def _():
            add_grads(k)
        return 0

    loads[0].wait()
    loads[1].wait()
    up_bf[...] = up32[...].astype(BF16)
    prepare(0)
    loads[2].wait()
    for copy in loads[3:]:
        copy.start()
    start_loads(stage, nb_hbm, nbuf, nb_sem)
    down_bf[...] = down32[...].astype(BF16)
    pl.semaphore_wait(barrier, 15)

    @pl.when(stage == 3)
    def _():
        load_loss.wait()
    lax.fori_loop(1, 3 * N_CHUNK, tick, 0)

    for c in range(2):
        v_first(0, c).wait_recv()
        rows = down_rows(z, 1 - y, 128 * c, 128)
        gv[rows, :] += rv1[0, 128 * c:128 * (c + 1), :]
        v_second(c).start()
        u_first(0, c).wait_recv()
        rows = up_rows(1 - z, y, 32 * c, 32)
        gu[rows, :] += ru1[0, 32 * c:32 * (c + 1), :]
        u_second(c).start()
    acc = jnp.zeros((8, 128), F32)

    def fold(tile, acc):
        sq = tile * tile
        sq = jnp.sum(sq.reshape(sq.shape[0] // 8, 8, sq.shape[1]), axis=0)
        for i in range(0, sq.shape[1], 128):
            acc = acc + sq[:, i:i + 128]
        return acc

    for c in range(2):
        v_first(1, c).wait_recv()
        v_second(c).wait_recv()
        rows = down_rows(z, y, 128 * c, 128)
        mean = (gv[rows, :] + rv1[1, 128 * c:128 * (c + 1), :] + rv2[128 * c:128 * (c + 1), :]) * 0.25
        mean_down[rows, :] = mean
        acc = fold(mean, acc)
        u_first(1, c).wait_recv()
        u_second(c).wait_recv()
        rows = up_rows(z, y, 32 * c, 32)
        mean = (gu[rows, :] + ru1[1, 32 * c:32 * (c + 1), :] + ru2[32 * c:32 * (c + 1), :]) * 0.25
        mean_up[rows, :] = mean
        acc = fold(mean, acc)

    up_piece, down_piece = 64 // N_PIECE, 256 // N_PIECE

    def gather(which, up, down):
        def copy(ref, rows, sem, piece, peer):
            sem = (which * 6 + sem) * N_PIECE + piece
            return pltpu.make_async_remote_copy(src_ref=ref.at[rows], dst_ref=ref.at[rows], send_sem=ag_send.at[sem], recv_sem=ag_recv.at[sem],
                                                device_id={"data": peer}, device_id_type=MESH)

        def up_copy(zz, yy, sem, p, peer):
            return copy(up, up_rows(zz, yy, up_piece * p, up_piece), sem, p, peer)

        def down_copy(zz, yy, sem, p, peer):
            return copy(down, down_rows(zz, yy, down_piece * p, down_piece), sem, p, peer)

        def up_sends(p):
            return [up_copy(z, y, 0, p, z_peer), up_copy(z, y, 1, p, y_peer)]

        def down_sends(p):
            return [down_copy(z, y, 3, p, y_peer), down_copy(z, y, 4, p, z_peer)]

        def relays(p):
            return [(up_copy(1 - z, y, 0, p, z_peer), up_copy(1 - z, y, 2, p, y_peer)), (down_copy(z, 1 - y, 3, p, y_peer), down_copy(z, 1 - y, 5, p, z_peer))]

        def begin(fed=None):
            for p in range(N_PIECE):
                for i, sends in enumerate((up_sends(p), down_sends(p))):
                    if fed is not None:
                        fed(p)[i].wait_recv()
                    for c in sends:
                        c.start()

        def relay():
            for p in range(N_PIECE):
                for arrived, onward in relays(p):
                    arrived.wait_recv()
                    onward.start()

        def finish():
            for p in range(N_PIECE):
                for c in (up_copy(z, 1 - y, 1, p, y_peer), down_copy(1 - z, y, 4, p, z_peer), up_copy(1 - z, 1 - y, 2, p, y_peer), down_copy(1 - z, 1 - y, 5, p, z_peer)):
                    c.wait_recv()

        def drain():
            for p in range(N_PIECE):
                for c in up_sends(p) + down_sends(p) + [onward for _, onward in relays(p)]:
                    c.wait_send()
        return begin, relay, finish, drain

    own_begin, own_relay, own_finish, own_drain = gather(0, up_own, down_own)
    aux_begin, aux_relay, aux_finish, aux_drain = gather(1, up_aux, down_aux)
    mean_begin, mean_relay, mean_finish, mean_drain = gather(2, mean_up, mean_down)

    def sq_copy(other, slot):
        return pltpu.make_async_remote_copy(src_ref=sq_all.at[slot], dst_ref=sq_all.at[slot], send_sem=sq_send.at[other], recv_sem=sq_recv.at[slot],
                                            device_id={"data": lax.div(other, 4), "stage": lax.rem(other, 4)}, device_id_type=MESH)

    sq_all[me] = acc

    def tell(d, _):
        sq_copy(lax.rem(me + d, 16), me).start()
        return 0
    lax.fori_loop(1, 16, tell, 0)
    for copy in loads[5:]:
        copy.wait()

    @pl.when(stage >= 2)
    def _():
        mean_begin()
        mean_relay()
        mean_finish()

    def hear(d, _):
        other = lax.rem(me + d, 16)
        sq_copy(other, other).wait_recv()
        return 0
    lax.fori_loop(1, 16, hear, 0)
    total = sq_all[0]
    for i in range(1, 16):
        total = total + sq_all[i]
    total = jnp.sum(jnp.sum(total, axis=0, keepdims=True), axis=1, keepdims=True)
    clip = jnp.minimum(1.0, norm_ref[0] / (jnp.sqrt(total) + NORM_EPS))

    rate = rate_ref[0]
    whole = jnp.where(stage >= 2, 1, 0)

    def renew(rows, master, moments, mean, weights, scale, first, full):
        new = adamw_update(master[rows, :], moments[0, rows, :], moments[1, rows, :], mean[rows, :], clip, rate)
        if first:
            weights[rows, :] = new[0].astype(BF16) * jnp.asarray(scale, BF16)

        @pl.when(full)
        def _():
            master[rows, :] = new[0]
            moments[0, rows, :] = new[1]
            moments[1, rows, :] = new[2]

    def renew_block(up_block, down_block, first, full):
        renew(pl.ds(pl.multiple_of(64 * up_block, 64), 64), up32, m_up, mean_up, up_own, 0.5, first, full)
        renew(pl.ds(pl.multiple_of(256 * down_block, 256), 256), down32, m_down, mean_down, down_own, 1.0, first, full)

    def renew_first(t, _):
        renew_block(whole * t + (1 - whole) * (2 * y + z), whole * t + (1 - whole) * (2 * z + y), True, whole == 1)
        return 0

    def renew_rest(t, _):
        renew_block(t, t, False, t >= 0)
        return 0

    new_stores = [pltpu.make_async_copy(src, dst, in_sem.at[i]) for i, (src, dst) in enumerate((
        (up32, new_up_hbm), (down32, new_down_hbm), (m_up.at[0], new_m1_up_hbm), (m_down.at[0], new_m1_down_hbm), (m_up.at[1], new_m2_up_hbm), (m_down.at[1], new_m2_down_hbm)))]
    lax.fori_loop(0, 1 + 3 * whole, renew_first, 0)

    def feed(p):
        parts = [(up_own, up_aux, up_rows(z, y, up_piece * p, up_piece)), (down_own, down_aux, down_rows(z, y, down_piece * p, down_piece))]
        return [pltpu.make_async_remote_copy(src_ref=own.at[rows], dst_ref=aux.at[rows], send_sem=aux_send.at[2 * p + i], recv_sem=aux_recv.at[2 * p + i], device_id={"stage": 3 - stage}, device_id_type=MESH)
                for i, (own, aux, rows) in enumerate(parts)]

    @pl.when(stage < 2)
    def _():
        for p in range(N_PIECE):
            for c in feed(p):
                c.start()
        own_begin()
        own_relay()
        mean_begin()

    @pl.when(stage >= 2)
    def _():
        for copy in new_stores:
            copy.start()
        aux_begin(feed)
        aux_relay()

    def relay_mean(now):
        @pl.when(now)
        def _():
            mean_relay()

    forward_part(stage, own_finish, aux_finish, relay_mean, nb_hbm, up_own, down_own, up_aux, down_aux, up_two, down_two, out_hbm, late_hbm, nbuf, xin, yout, nb_sem, out_sem, send_sem, recv_sem, two_send, two_recv)

    @pl.when(stage < 2)
    def _():
        mean_finish()
        lax.fori_loop(0, 4, renew_rest, 0)
        for copy in new_stores:
            copy.start()
    store_w_up = pltpu.make_async_copy(up_own, w_up_hbm, in_sem.at[6])
    store_w_down = pltpu.make_async_copy(down_own, w_down_hbm, in_sem.at[7])
    store_w_up.start()
    store_w_down.start()

    @pl.when(stage == 1)
    def _():
        def left(i, _):
            pltpu.make_async_remote_copy(src_ref=yout.at[i], dst_ref=xin.at[i], send_sem=send_sem.at[i], recv_sem=recv_sem.at[i], device_id={"stage": 2}, device_id_type=MESH).wait_send()
            return 0
        lax.fori_loop(nbuf.shape[0] - N_SENT, nbuf.shape[0], left, 0)

    @pl.when(stage > 0)
    def _():
        for k in range(N_CHUNK):
            pass_down(k).wait_send()
    for c in range(2):
        for sub in range(2):
            v_first(sub, c).wait_send()
            u_first(sub, c).wait_send()
        v_second(c).wait_send()
        u_second(c).wait_send()

    def told(d, _):
        sq_copy(lax.rem(me + d, 16), me).wait_send()
        return 0
    lax.fori_loop(1, 16, told, 0)
    mean_drain()

    @pl.when(stage < 2)
    def _():
        own_drain()
        for p in range(N_PIECE):
            for c in feed(p):
                c.wait_send()

    @pl.when(stage >= 2)
    def _():
        aux_drain()
    for copy in new_stores:
        copy.wait()
    store_w_up.wait()
    store_w_down.wait()


def fused_step(master_up, master_down, m1_up, m1_down, m2_up, m2_down, grad_up, grad_down, acts, loss_grad, next_batch, learn_rate, max_norm):
    n_micro = next_batch.shape[0]
    n_tok, width = acts.shape
    hidden = master_up.shape[1]
    hbm = pl.BlockSpec(memory_space=pl.ANY)
    smem = pl.BlockSpec(memory_space=pltpu.SMEM)
    vmem = pltpu.VMEM
    dma = pltpu.SemaphoreType.DMA
    return pl.pallas_call(
        step_kernel,
        name="pipeline_step",
        out_shape=[jax.ShapeDtypeStruct(next_batch.shape, BF16)] + [jax.ShapeDtypeStruct((width, hidden), F32), jax.ShapeDtypeStruct((hidden, width), F32)] * 3 + [
            jax.ShapeDtypeStruct((N_LATE,) + next_batch.shape[1:], BF16), jax.ShapeDtypeStruct((width, hidden), BF16), jax.ShapeDtypeStruct((hidden, width), BF16)],
        in_specs=[hbm] * 11 + [smem] * 2,
        out_specs=[hbm] * 10,
        scratch_shapes=[
            vmem((width, hidden), F32), vmem((hidden, width), F32),
            vmem((width, hidden), F32), vmem((hidden, width), F32),
            vmem((width, hidden), F32), vmem((hidden, width), F32),
            vmem((n_tok, width), BF16), vmem((n_tok, width), BF16), vmem((n_tok, width), BF16),
            vmem((n_tok, hidden), BF16), vmem((n_tok, hidden), F32), vmem((n_tok, hidden), BF16),
            vmem((width, hidden), BF16), vmem((hidden, width), BF16),
            vmem((2, width // 4, hidden), F32), vmem((2, hidden // 4, width), F32),
            vmem((width // 4, hidden), F32), vmem((hidden // 4, width), F32),
            vmem((2, width, hidden), F32), vmem((2, hidden, width), F32),
            vmem((width, hidden), BF16), vmem((hidden, width), BF16),
            vmem((width, hidden), BF16), vmem((hidden, width), BF16),
            vmem((width, hidden), BF16), vmem((hidden, width), BF16),
            vmem((16, 8, 128), F32),
            vmem(next_batch.shape, BF16), vmem(next_batch.shape, BF16), vmem(next_batch.shape, BF16),
            dma((10,)), dma((N_CHUNK,)), dma((N_CHUNK,)), dma((12,)), dma((12,)), dma((16,)), dma((16,)), dma((18 * N_PIECE,)), dma((18 * N_PIECE,)), dma((2 * N_PIECE,)), dma((2 * N_PIECE,)),
            dma((n_micro,)), dma((n_micro,)), dma((n_micro,)), dma((n_micro,)), dma((2,)), dma((2,)),
        ],
        compiler_params=pltpu.CompilerParams(collective_id=1, has_side_effects=True, vmem_limit_bytes=63 * 1024 * 1024),
    )(master_up, master_down, m1_up, m1_down, m2_up, m2_down, grad_up, grad_down, acts, loss_grad, next_batch, learn_rate, max_norm)


def finish_kernel(outs_in, late_in, w_up_in, w_down_in, *refs):
    news_in, outs, news_out = refs[:6], refs[6], refs[7:13]
    obuf, late, w_up, w_down, upd_up, upd_down, load_sem, store_sem, micro_load, micro_store, late_load = refs[13:]
    stage = lax.axis_index("stage")
    n_micro = obuf.shape[0]
    last = stage == 3
    n_copied = jnp.where(last, n_micro - N_LATE, n_micro)
    per_late = -(-(n_micro - N_LATE) // (N_LATE - 2))
    slots = [buf.at[i] for i in range(3) for buf in (upd_up, upd_down)]
    loads = [pltpu.make_async_copy(src, slot, load_sem.at[i]) for i, (src, slot) in enumerate(zip(news_in, slots))]
    stores = [pltpu.make_async_copy(slot, dst, store_sem.at[i]) for i, (slot, dst) in enumerate(zip(slots, news_out))]
    w_loads = [pltpu.make_async_copy(w_up_in, w_up, load_sem.at[6]), pltpu.make_async_copy(w_down_in, w_down, load_sem.at[7])]

    def place(k):
        return mixed(k, n_micro)[1]

    def load_micro(k):
        i = place(k)
        return pltpu.make_async_copy(outs_in.at[i], obuf.at[i], micro_load.at[i])

    def store_micro(k):
        i = place(k)
        return pltpu.make_async_copy(obuf.at[i], outs.at[i], micro_store.at[i])

    def load_late(n):
        return pltpu.make_async_copy(late_in.at[n], late.at[n], late_load.at[n])

    def start_micro(k, _):
        load_micro(k).start()
        return 0

    def turn_micro(k, _):
        load_micro(k).wait()
        store_micro(k).start()
        return 0

    def start_late(n, _):
        load_late(n).start()
        return 0

    @pl.when(last)
    def _():
        for copy in w_loads:
            copy.start()
        lax.fori_loop(0, N_LATE, start_late, 0)
    for copy in loads:
        copy.start()
    lax.fori_loop(0, n_copied, start_micro, 0)

    @pl.when(last)
    def _():
        for copy in w_loads:
            copy.wait()

        def body(n, _):
            load_late(n).wait()
            k = n_micro - N_LATE + n
            stage_rows(late.at[n], w_up, w_down, obuf.at[place(k)])
            store_micro(k).start()

            @pl.when(n == 1)
            def _():
                for load, store in zip(loads, stores):
                    load.wait()
                    store.start()
            for j in range(per_late):
                k = per_late * (n - 2) + j

                @pl.when((k >= 0) & (k < n_micro - N_LATE))
                def _():
                    turn_micro(k, 0)
            return 0
        lax.fori_loop(0, N_LATE, body, 0)

    @pl.when(jnp.logical_not(last))
    def _():
        for load, store in zip(loads, stores):
            load.wait()
            store.start()
        lax.fori_loop(0, n_micro, turn_micro, 0)

    def stored(k, _):
        store_micro(k).wait()
        return 0
    lax.fori_loop(0, n_micro, stored, 0)
    for copy in stores:
        copy.wait()


def finish_step(outs, late, w_up, w_down, *news):
    n_micro = outs.shape[0]
    hbm = pl.BlockSpec(memory_space=pl.ANY)
    vmem = pltpu.VMEM
    dma = pltpu.SemaphoreType.DMA
    return pl.pallas_call(
        finish_kernel,
        name="finish_step",
        out_shape=[jax.ShapeDtypeStruct(outs.shape, BF16)] + [jax.ShapeDtypeStruct(new.shape, F32) for new in news],
        in_specs=[hbm] * 10,
        out_specs=[hbm] * 7,
        scratch_shapes=[
            vmem(outs.shape, BF16), vmem(late.shape, BF16), vmem(w_up.shape, BF16), vmem(w_down.shape, BF16),
            vmem((3,) + news[0].shape, F32), vmem((3,) + news[1].shape, F32),
            dma((8,)), dma((6,)), dma((n_micro,)), dma((n_micro,)), dma((N_LATE,)),
        ],
        compiler_params=pltpu.CompilerParams(vmem_limit_bytes=56 * 1024 * 1024),
    )(outs, late, w_up, w_down, *news)


def solution(mesh):
    def local_step(master_up, master_down, mom1_up, mom1_down, mom2_up, mom2_down, grad_up, grad_down, stage_acts, loss_grad, next_batch, learn_rate, max_norm):
        stage_outs, *news, late, w_up, w_down = fused_step(
            master_up[0], master_down[0], mom1_up[0], mom1_down[0], mom2_up[0], mom2_down[0], grad_up[0, 0], grad_down[0, 0],
            stage_acts[0], loss_grad, next_batch, learn_rate.reshape(1), max_norm.reshape(1))
        stage_outs, new_up, new_down, new_m1_up, new_m1_down, new_m2_up, new_m2_down = finish_step(stage_outs, late, w_up, w_down, *news)
        return (new_up[None], new_down[None], new_m1_up[None], new_m1_down[None], new_m2_up[None], new_m2_down[None], stage_outs[None])

    w_spec = P('stage', None, None)
    g_spec = P('data', 'stage', None, None)
    in_specs = (w_spec, w_spec, w_spec, w_spec, w_spec, w_spec, g_spec, g_spec, P('stage', 'data', None), P('data', None), P(None, 'data', None), P(), P())
    out_specs = (w_spec, w_spec, w_spec, w_spec, w_spec, w_spec, P('stage', None, 'data', None))
    return jax.shard_map(local_step, mesh=mesh, in_specs=in_specs, out_specs=out_specs, check_vma=False)
```

```python
import jax
import jax.numpy as jnp
from jax import lax
from jax.experimental import pallas as pl
from jax.experimental.pallas import tpu as pltpu
from jax.sharding import PartitionSpec as P

BETA1 = 0.9
BETA2 = 0.95
ADAM_EPS = 1e-8
WEIGHT_DECAY = 0.1
NORM_EPS = 1e-6
ADAM_STEP = 8
SQRT_TWO_PI = 0.7978845608028654
GELU_CUBIC = 0.044715

N_SENT = 5
N_CHUNK = 4
N_LATE = 6
N_TWICE = 4
N_PIECE = 1
MESH = pl.DeviceIdType.MESH
BF16 = jnp.bfloat16
F32 = jnp.float32


def mat_tn(left, right):
    return lax.dot_general(left, right, (((0,), (0,)), ((), ())), preferred_element_type=F32)


def mat_nt(left, right):
    return lax.dot_general(left, right, (((1,), (1,)), ((), ())), preferred_element_type=F32)


def adamw_update(master, first_mom, second_mom, grad_avg, clip_scale, learn_rate):
    scaled = clip_scale * grad_avg
    new_first = BETA1 * first_mom + (1.0 - BETA1) * scaled
    new_second = BETA2 * second_mom + (1.0 - BETA2) * scaled * scaled
    first_hat = new_first * (1.0 / (1.0 - BETA1 ** ADAM_STEP))
    second_hat = new_second * (1.0 / (1.0 - BETA2 ** ADAM_STEP))
    new_master = master - learn_rate * (first_hat / (jnp.sqrt(second_hat) + ADAM_EPS) + WEIGHT_DECAY * master)
    return new_master, new_first, new_second


def gelu_of_half(half):
    t = jnp.tanh(half * (2.0 * SQRT_TWO_PI + (8.0 * SQRT_TWO_PI * GELU_CUBIC) * (half * half)))
    return half + half * t


def stage_rows(src, up_half, down, dst):
    x = src[...]
    half = jnp.dot(x, up_half[...], preferred_element_type=F32)
    hidden = gelu_of_half(half).astype(BF16)
    y = jnp.dot(hidden, down[...], preferred_element_type=F32)
    dst[...] = (x.astype(F32) + y).astype(BF16)


def mixed(k, n_micro):
    before = lax.div(k * N_SENT, n_micro)
    is_sent = lax.div((k + 1) * N_SENT, n_micro) - before
    return is_sent, is_sent * (n_micro - N_SENT + before) + (1 - is_sent) * (k - before)


def forward_part(stage, own_ready, aux_ready, relay_mean, nb_hbm, up_own, down_own, up_aux, down_aux, up_two, down_two, out_hbm, late_hbm, nbuf, xin, yout, nb_sem, out_sem, send_sem, recv_sem, two_send, two_recv):
    n_micro = nbuf.shape[0]
    n_kept = n_micro - N_SENT

    def load(i):
        return pltpu.make_async_copy(nb_hbm.at[i], nbuf.at[i], nb_sem.at[i])

    def store(i):
        return pltpu.make_async_copy(yout.at[i], out_hbm.at[i], out_sem.at[i])

    def push(src, i, peer):
        return pltpu.make_async_remote_copy(src_ref=src.at[i], dst_ref=xin.at[i], send_sem=send_sem.at[i], recv_sem=recv_sem.at[i], device_id={"stage": peer}, device_id_type=MESH)

    def arrived(i):
        push(yout, i, stage).wait_recv()

    def rotated(j):
        return lax.rem(j + n_kept, n_micro)

    def finish_stores():
        def body(i, _):
            store(i).wait()
            return 0
        lax.fori_loop(0, n_micro, body, 0)

    def hand_over():
        return [pltpu.make_async_remote_copy(src_ref=aux, dst_ref=two, send_sem=two_send.at[i], recv_sem=two_recv.at[i], device_id={"stage": 3}, device_id_type=MESH)
                for i, (aux, two) in enumerate([(up_aux, up_two), (down_aux, down_two)])]

    def finish_sends(first, count):
        def body(i, _):
            push(yout, first + i, stage).wait_send()
            return 0
        lax.fori_loop(0, count, body, 0)

    @pl.when(stage == 0)
    def _():
        own_ready()

        def body(j, _):
            i = rotated(j)
            load(i).wait()
            stage_rows(nbuf.at[i], up_own, down_own, yout.at[i])
            push(yout, i, 1).start()
            store(i).start()
            relay_mean(j == 7)
            return 0
        lax.fori_loop(0, n_micro, body, 0)
        finish_sends(0, n_micro)
        finish_stores()

    @pl.when(stage == 1)
    def _():
        own_ready()

        def body(j, _):
            i = rotated(j)
            arrived(i)
            stage_rows(xin.at[i], up_own, down_own, yout.at[i])

            @pl.when(j < N_SENT)
            def _():
                push(yout, i, 2).start()
            store(i).start()
            relay_mean(j == 7)
            return 0
        lax.fori_loop(0, n_micro, body, 0)
        finish_stores()

    @pl.when(stage == 2)
    def _():
        aux_ready()
        for copy in hand_over():
            copy.start()

        def body(k, _):
            _, i = mixed(k, n_micro)
            arrived(i)

            @pl.when(i < n_kept - N_TWICE)
            def _():
                stage_rows(xin.at[i], up_aux, down_aux, xin.at[i])
            stage_rows(xin.at[i], up_own, down_own, yout.at[i])
            push(yout, i, 3).start()
            store(i).start()
            return 0
        lax.fori_loop(0, n_micro, body, 0)
        finish_sends(0, n_micro)
        finish_stores()
        for copy in hand_over():
            copy.wait_send()

    @pl.when(stage == 3)
    def _():
        aux_ready()

        def first(j, _):
            load(j).wait()
            stage_rows(nbuf.at[j], up_aux, down_aux, nbuf.at[j])

            @pl.when(j == n_kept - N_TWICE)
            def _():
                for copy in hand_over():
                    copy.wait_recv()

            @pl.when(j >= n_kept - N_TWICE)
            def _():
                stage_rows(nbuf.at[j], up_two, down_two, nbuf.at[j])
            push(nbuf, j, 2).start()
            return 0
        lax.fori_loop(0, n_kept, first, 0)

        def body(k, _):
            _, i = mixed(k, n_micro)
            arrived(i)
            stage_rows(xin.at[i], up_own, down_own, yout.at[i])
            store(i).start()
            return 0
        lax.fori_loop(0, n_micro - N_LATE, body, 0)

        def late(k):
            _, i = mixed(k, n_micro)
            return i, pltpu.make_async_copy(xin.at[i], late_hbm.at[k - (n_micro - N_LATE)], out_sem.at[i])

        def save(k, _):
            i, copy = late(k)
            arrived(i)
            copy.start()
            return 0
        lax.fori_loop(n_micro - N_LATE, n_micro, save, 0)

        def stored(k, _):
            _, i = mixed(k, n_micro)
            store(i).wait()
            return 0
        lax.fori_loop(0, n_micro - N_LATE, stored, 0)

        def saved(k, _):
            late(k)[1].wait()
            return 0
        lax.fori_loop(n_micro - N_LATE, n_micro, saved, 0)
        finish_sends(0, n_kept)


def start_loads(stage, nb_hbm, nbuf, nb_sem):
    n_micro = nbuf.shape[0]
    n_kept = n_micro - N_SENT

    def body(j, _):
        i = lax.rem(j + n_kept, n_micro)
        pltpu.make_async_copy(nb_hbm.at[i], nbuf.at[i], nb_sem.at[i]).start()
        return 0

    @pl.when(stage == 0)
    def _():
        lax.fori_loop(0, n_micro, body, 0)

    @pl.when(stage == 3)
    def _():
        lax.fori_loop(N_SENT, n_micro, body, 0)


def step_kernel(up_hbm, down_hbm, m1_up_hbm, m1_down_hbm, m2_up_hbm, m2_down_hbm, gu_hbm, gv_hbm, acts_hbm, loss_hbm, nb_hbm, rate_ref, norm_ref,
                out_hbm, new_up_hbm, new_down_hbm, new_m1_up_hbm, new_m1_down_hbm, new_m2_up_hbm, new_m2_down_hbm, late_hbm, w_up_hbm, w_down_hbm,
                up32, down32, gu, gv, mean_up, mean_down, acts, gbuf, dxbuf, hid, slope, dpre, up_bf, down_bf,
                ru1, rv1, ru2, rv2, m_up, m_down, up_own, down_own, up_aux, down_aux, up_two, down_two, sq_all, nbuf, xin, yout,
                in_sem, g_send, g_recv, rs_send, rs_recv, sq_send, sq_recv, ag_send, ag_recv, aux_send, aux_recv,
                nb_sem, out_sem, send_sem, recv_sem, two_send, two_recv):
    stage = lax.axis_index("stage")
    data = lax.axis_index("data")
    z = lax.div(data, 2)
    y = lax.rem(data, 2)
    me = data * 4 + stage
    z_peer = 2 * (1 - z) + y
    y_peer = 2 * z + (1 - y)
    n_tok = acts.shape[0]
    chunk = n_tok // N_CHUNK

    def up_rows(zz, yy, first=0, count=64):
        return pl.ds(pl.multiple_of(128 * yy + 64 * zz + first, 32), count)

    def down_rows(zz, yy, first=0, count=256):
        return pl.ds(pl.multiple_of(512 * zz + 256 * yy + first, 128), count)

    own_up, own_down = up_rows(z, y), down_rows(z, y)
    loads = [
        pltpu.make_async_copy(acts_hbm, acts, in_sem.at[0]),
        pltpu.make_async_copy(up_hbm, up32, in_sem.at[1]),
        pltpu.make_async_copy(down_hbm, down32, in_sem.at[2]),
        pltpu.make_async_copy(gv_hbm, gv, in_sem.at[3]),
        pltpu.make_async_copy(gu_hbm, gu, in_sem.at[4]),
        pltpu.make_async_copy(m1_up_hbm, m_up.at[0], in_sem.at[5]),
        pltpu.make_async_copy(m2_up_hbm, m_up.at[1], in_sem.at[6]),
        pltpu.make_async_copy(m1_down_hbm, m_down.at[0], in_sem.at[7]),
        pltpu.make_async_copy(m2_down_hbm, m_down.at[1], in_sem.at[8]),
    ]
    load_loss = pltpu.make_async_copy(loss_hbm, gbuf, in_sem.at[9])
    for copy in loads[:2]:
        copy.start()

    @pl.when(stage == 3)
    def _():
        load_loss.start()
    loads[2].start()

    barrier = pltpu.get_barrier_semaphore()

    def greet(d, _):
        other = lax.rem(me + d, 16)
        pl.semaphore_signal(barrier, inc=1, device_id={"data": lax.div(other, 4), "stage": lax.rem(other, 4)}, device_id_type=MESH)
        return 0
    lax.fori_loop(1, 16, greet, 0)

    def chunk_rows(k):
        return pl.ds(pl.multiple_of(k * chunk, chunk), chunk)

    def pass_down(k):
        rows = chunk_rows(k)
        return pltpu.make_async_remote_copy(src_ref=dxbuf.at[rows], dst_ref=gbuf.at[rows], send_sem=g_send.at[k], recv_sem=g_recv.at[k],
                                            device_id={"stage": jnp.maximum(stage - 1, 0)}, device_id_type=MESH)

    def prepare(k):
        rows = chunk_rows(k)
        pre = jnp.dot(acts[rows, :], up_bf[...], preferred_element_type=F32)
        sq = pre * pre
        half_t = 0.5 * jnp.tanh(pre * (SQRT_TWO_PI + (SQRT_TWO_PI * GELU_CUBIC) * sq))
        prob = 0.5 + half_t
        rest = 0.5 - half_t
        hid[rows, :] = (pre * prob).astype(BF16)
        slope[rows, :] = prob + (prob * rest) * pre * (2.0 * SQRT_TWO_PI + (6.0 * SQRT_TWO_PI * GELU_CUBIC) * sq)

    def backward(k):
        rows = chunk_rows(k)

        @pl.when(stage < 3)
        def _():
            pass_down(k).wait_recv()
        grad = gbuf[rows, :]
        d_pre = (mat_nt(grad, down_bf[...]) * slope[rows, :]).astype(BF16)
        dpre[rows, :] = d_pre

        @pl.when(stage > 0)
        def _():
            dxbuf[rows, :] = (grad.astype(F32) + mat_nt(d_pre, up_bf[...])).astype(BF16)
            pass_down(k).start()

    def rs_copy(src, dst, sem, peer):
        return pltpu.make_async_remote_copy(src_ref=src, dst_ref=dst, send_sem=rs_send.at[sem], recv_sem=rs_recv.at[sem], device_id={"data": peer}, device_id_type=MESH)

    def v_first(sub, c):
        yy = (1 - y) if sub == 0 else y
        return rs_copy(gv.at[down_rows(1 - z, yy, 128 * c, 128)], rv1.at[sub, pl.ds(128 * c, 128)], 2 * sub + c, z_peer)

    def u_first(sub, c):
        zz = (1 - z) if sub == 0 else z
        return rs_copy(gu.at[up_rows(zz, 1 - y, 32 * c, 32)], ru1.at[sub, pl.ds(32 * c, 32)], 4 + 2 * sub + c, y_peer)

    def v_second(c):
        return rs_copy(gv.at[down_rows(z, 1 - y, 128 * c, 128)], rv2.at[pl.ds(128 * c, 128)], 8 + c, y_peer)

    def u_second(c):
        return rs_copy(gu.at[up_rows(1 - z, y, 32 * c, 32)], ru2.at[pl.ds(32 * c, 32)], 10 + c, z_peer)

    def add_grads(k):
        rows = chunk_rows(k)

        @pl.when(k == 0)
        def _():
            loads[3].wait()
            loads[4].wait()

        def half(h, _):
            zz = h * z + (1 - h) * (1 - z)
            yy = h * y + (1 - h) * (1 - y)
            send = (k == N_CHUNK - 1) & (h == 0)
            out = pl.ds(pl.multiple_of(512 * zz, 512), 512)
            gv[out, :] += mat_tn(hid[rows, out], gbuf[rows, :])

            @pl.when(send)
            def _():
                for sub in range(2):
                    for c in range(2):
                        v_first(sub, c).start()
            out = pl.ds(pl.multiple_of(128 * yy, 128), 128)
            gu[out, :] += mat_tn(acts[rows, out], dpre[rows, :])

            @pl.when(send)
            def _():
                for sub in range(2):
                    for c in range(2):
                        u_first(sub, c).start()
            return 0
        lax.fori_loop(0, 2, half, 0)

    def tick(t, _):
        upper = jnp.where(stage >= 2, 1, 0)
        even = 1 - lax.rem(t, 2)
        early = jnp.where(t < N_CHUNK, 1, 0)
        late = jnp.where(t >= 2 * N_CHUNK, 1, 0)
        is_prep = upper * even * (1 - late) + (1 - upper) * early
        is_grad = upper * late + (1 - upper) * (1 - early) * (1 - even)
        k = upper * (late * (t - 2 * N_CHUNK) + (1 - late) * lax.div(t, 2)) + (1 - upper) * (early * t + (1 - early) * lax.div(t - N_CHUNK, 2))

        @pl.when(is_prep == 1)
        def _():
            prepare(k)

        @pl.when(is_prep + is_grad == 0)
        def _():
            backward(k)

        @pl.when(is_grad == 1)
        def _():
            add_grads(k)
        return 0

    loads[0].wait()
    loads[1].wait()
    up_bf[...] = up32[...].astype(BF16)
    prepare(0)
    loads[2].wait()
    for copy in loads[3:]:
        copy.start()
    start_loads(stage, nb_hbm, nbuf, nb_sem)
    down_bf[...] = down32[...].astype(BF16)
    pl.semaphore_wait(barrier, 15)

    @pl.when(stage == 3)
    def _():
        load_loss.wait()
    lax.fori_loop(1, 3 * N_CHUNK, tick, 0)

    for c in range(2):
        v_first(0, c).wait_recv()
        rows = down_rows(z, 1 - y, 128 * c, 128)
        gv[rows, :] += rv1[0, 128 * c:128 * (c + 1), :]
        v_second(c).start()
        u_first(0, c).wait_recv()
        rows = up_rows(1 - z, y, 32 * c, 32)
        gu[rows, :] += ru1[0, 32 * c:32 * (c + 1), :]
        u_second(c).start()
    acc = jnp.zeros((8, 128), F32)

    def fold(tile, acc):
        sq = tile * tile
        sq = jnp.sum(sq.reshape(sq.shape[0] // 8, 8, sq.shape[1]), axis=0)
        for i in range(0, sq.shape[1], 128):
            acc = acc + sq[:, i:i + 128]
        return acc

    for c in range(2):
        v_first(1, c).wait_recv()
        v_second(c).wait_recv()
        rows = down_rows(z, y, 128 * c, 128)
        mean = (gv[rows, :] + rv1[1, 128 * c:128 * (c + 1), :] + rv2[128 * c:128 * (c + 1), :]) * 0.25
        mean_down[rows, :] = mean
        acc = fold(mean, acc)
        u_first(1, c).wait_recv()
        u_second(c).wait_recv()
        rows = up_rows(z, y, 32 * c, 32)
        mean = (gu[rows, :] + ru1[1, 32 * c:32 * (c + 1), :] + ru2[32 * c:32 * (c + 1), :]) * 0.25
        mean_up[rows, :] = mean
        acc = fold(mean, acc)

    up_piece, down_piece = 64 // N_PIECE, 256 // N_PIECE

    def gather(which, up, down):
        def copy(ref, rows, sem, piece, peer):
            sem = (which * 6 + sem) * N_PIECE + piece
            return pltpu.make_async_remote_copy(src_ref=ref.at[rows], dst_ref=ref.at[rows], send_sem=ag_send.at[sem], recv_sem=ag_recv.at[sem],
                                                device_id={"data": peer}, device_id_type=MESH)

        def up_copy(zz, yy, sem, p, peer):
            return copy(up, up_rows(zz, yy, up_piece * p, up_piece), sem, p, peer)

        def down_copy(zz, yy, sem, p, peer):
            return copy(down, down_rows(zz, yy, down_piece * p, down_piece), sem, p, peer)

        def up_sends(p):
            return [up_copy(z, y, 0, p, z_peer), up_copy(z, y, 1, p, y_peer)]

        def down_sends(p):
            return [down_copy(z, y, 3, p, y_peer), down_copy(z, y, 4, p, z_peer)]

        def relays(p):
            return [(up_copy(1 - z, y, 0, p, z_peer), up_copy(1 - z, y, 2, p, y_peer)), (down_copy(z, 1 - y, 3, p, y_peer), down_copy(z, 1 - y, 5, p, z_peer))]

        def begin(matrix):
            for p in range(N_PIECE):
                for c in (up_sends, down_sends)[matrix](p):
                    c.start()

        def relay():
            for p in range(N_PIECE):
                for arrived, onward in relays(p):
                    arrived.wait_recv()
                    onward.start()

        def finish():
            for p in range(N_PIECE):
                for c in (up_copy(z, 1 - y, 1, p, y_peer), down_copy(1 - z, y, 4, p, z_peer), up_copy(1 - z, 1 - y, 2, p, y_peer), down_copy(1 - z, 1 - y, 5, p, z_peer)):
                    c.wait_recv()

        def drain():
            for p in range(N_PIECE):
                for c in up_sends(p) + down_sends(p) + [onward for _, onward in relays(p)]:
                    c.wait_send()
        return begin, relay, finish, drain

    own_begin, own_relay, own_finish, own_drain = gather(0, up_own, down_own)
    aux_begin, aux_relay, aux_finish, aux_drain = gather(1, up_aux, down_aux)
    mean_begin, mean_relay, mean_finish, mean_drain = gather(2, mean_up, mean_down)

    def sq_copy(other, slot):
        return pltpu.make_async_remote_copy(src_ref=sq_all.at[slot], dst_ref=sq_all.at[slot], send_sem=sq_send.at[other], recv_sem=sq_recv.at[slot],
                                            device_id={"data": lax.div(other, 4), "stage": lax.rem(other, 4)}, device_id_type=MESH)

    sq_all[me] = acc

    def tell(d, _):
        sq_copy(lax.rem(me + d, 16), me).start()
        return 0
    lax.fori_loop(1, 16, tell, 0)
    for copy in loads[5:]:
        copy.wait()

    @pl.when(stage >= 2)
    def _():
        mean_begin(0)
        mean_begin(1)
        mean_relay()
        mean_finish()

    def hear(d, _):
        other = lax.rem(me + d, 16)
        sq_copy(other, other).wait_recv()
        return 0
    lax.fori_loop(1, 16, hear, 0)
    total = sq_all[0]
    for i in range(1, 16):
        total = total + sq_all[i]
    total = jnp.sum(jnp.sum(total, axis=0, keepdims=True), axis=1, keepdims=True)
    clip = jnp.minimum(1.0, norm_ref[0] / (jnp.sqrt(total) + NORM_EPS))

    rate = rate_ref[0]

    def renew(rows, master, moments, mean, weights, scale, first, full):
        new = adamw_update(master[rows, :], moments[0, rows, :], moments[1, rows, :], mean[rows, :], clip, rate)
        if first:
            weights[rows, :] = new[0].astype(BF16) * jnp.asarray(scale, BF16)

        if full:
            master[rows, :] = new[0]
            moments[0, rows, :] = new[1]
            moments[1, rows, :] = new[2]

    def renew_up(block, first, full):
        renew(pl.ds(pl.multiple_of(64 * block, 64), 64), up32, m_up, mean_up, up_own, 0.5, first, full)

    def renew_down(block, first, full):
        renew(pl.ds(pl.multiple_of(256 * block, 256), 256), down32, m_down, mean_down, down_own, 1.0, first, full)

    def renew_all(first):
        def body(t, _):
            renew_up(t, first, True)
            renew_down(t, first, True)
            return 0
        lax.fori_loop(0, 4, body, 0)

    new_stores = [pltpu.make_async_copy(src, dst, in_sem.at[i]) for i, (src, dst) in enumerate((
        (up32, new_up_hbm), (down32, new_down_hbm), (m_up.at[0], new_m1_up_hbm), (m_down.at[0], new_m1_down_hbm), (m_up.at[1], new_m2_up_hbm), (m_down.at[1], new_m2_down_hbm)))]
    def feed(p):
        parts = [(up_own, up_aux, up_rows(z, y, up_piece * p, up_piece)), (down_own, down_aux, down_rows(z, y, down_piece * p, down_piece))]
        return [pltpu.make_async_remote_copy(src_ref=own.at[rows], dst_ref=aux.at[rows], send_sem=aux_send.at[2 * p + i], recv_sem=aux_recv.at[2 * p + i], device_id={"stage": 3 - stage}, device_id_type=MESH)
                for i, (own, aux, rows) in enumerate(parts)]

    @pl.when(stage < 2)
    def _():
        renew_up(2 * y + z, True, False)
        for p in range(N_PIECE):
            feed(p)[0].start()
        own_begin(0)
        renew_down(2 * z + y, True, False)
        for p in range(N_PIECE):
            feed(p)[1].start()
        own_begin(1)
        own_relay()
        mean_begin(0)
        mean_begin(1)

    @pl.when(stage >= 2)
    def _():
        for matrix in range(2):
            for p in range(N_PIECE):
                feed(p)[matrix].wait_recv()
            aux_begin(matrix)
        renew_all(True)
        for copy in new_stores:
            copy.start()
        aux_relay()

    def relay_mean(now):
        @pl.when(now)
        def _():
            mean_relay()

    forward_part(stage, own_finish, aux_finish, relay_mean, nb_hbm, up_own, down_own, up_aux, down_aux, up_two, down_two, out_hbm, late_hbm, nbuf, xin, yout, nb_sem, out_sem, send_sem, recv_sem, two_send, two_recv)

    @pl.when(stage < 2)
    def _():
        mean_finish()
        renew_all(False)
        for copy in new_stores:
            copy.start()
    store_w_up = pltpu.make_async_copy(up_own, w_up_hbm, in_sem.at[6])
    store_w_down = pltpu.make_async_copy(down_own, w_down_hbm, in_sem.at[7])
    store_w_up.start()
    store_w_down.start()

    @pl.when(stage == 1)
    def _():
        def left(i, _):
            pltpu.make_async_remote_copy(src_ref=yout.at[i], dst_ref=xin.at[i], send_sem=send_sem.at[i], recv_sem=recv_sem.at[i], device_id={"stage": 2}, device_id_type=MESH).wait_send()
            return 0
        lax.fori_loop(nbuf.shape[0] - N_SENT, nbuf.shape[0], left, 0)

    @pl.when(stage > 0)
    def _():
        for k in range(N_CHUNK):
            pass_down(k).wait_send()
    for c in range(2):
        for sub in range(2):
            v_first(sub, c).wait_send()
            u_first(sub, c).wait_send()
        v_second(c).wait_send()
        u_second(c).wait_send()

    def told(d, _):
        sq_copy(lax.rem(me + d, 16), me).wait_send()
        return 0
    lax.fori_loop(1, 16, told, 0)
    mean_drain()

    @pl.when(stage < 2)
    def _():
        own_drain()
        for p in range(N_PIECE):
            for c in feed(p):
                c.wait_send()

    @pl.when(stage >= 2)
    def _():
        aux_drain()
    for copy in new_stores:
        copy.wait()
    store_w_up.wait()
    store_w_down.wait()


def fused_step(master_up, master_down, m1_up, m1_down, m2_up, m2_down, grad_up, grad_down, acts, loss_grad, next_batch, learn_rate, max_norm):
    n_micro = next_batch.shape[0]
    n_tok, width = acts.shape
    hidden = master_up.shape[1]
    hbm = pl.BlockSpec(memory_space=pl.ANY)
    smem = pl.BlockSpec(memory_space=pltpu.SMEM)
    vmem = pltpu.VMEM
    dma = pltpu.SemaphoreType.DMA
    return pl.pallas_call(
        step_kernel,
        name="pipeline_step",
        out_shape=[jax.ShapeDtypeStruct(next_batch.shape, BF16)] + [jax.ShapeDtypeStruct((width, hidden), F32), jax.ShapeDtypeStruct((hidden, width), F32)] * 3 + [
            jax.ShapeDtypeStruct((N_LATE,) + next_batch.shape[1:], BF16), jax.ShapeDtypeStruct((width, hidden), BF16), jax.ShapeDtypeStruct((hidden, width), BF16)],
        in_specs=[hbm] * 11 + [smem] * 2,
        out_specs=[hbm] * 10,
        scratch_shapes=[
            vmem((width, hidden), F32), vmem((hidden, width), F32),
            vmem((width, hidden), F32), vmem((hidden, width), F32),
            vmem((width, hidden), F32), vmem((hidden, width), F32),
            vmem((n_tok, width), BF16), vmem((n_tok, width), BF16), vmem((n_tok, width), BF16),
            vmem((n_tok, hidden), BF16), vmem((n_tok, hidden), F32), vmem((n_tok, hidden), BF16),
            vmem((width, hidden), BF16), vmem((hidden, width), BF16),
            vmem((2, width // 4, hidden), F32), vmem((2, hidden // 4, width), F32),
            vmem((width // 4, hidden), F32), vmem((hidden // 4, width), F32),
            vmem((2, width, hidden), F32), vmem((2, hidden, width), F32),
            vmem((width, hidden), BF16), vmem((hidden, width), BF16),
            vmem((width, hidden), BF16), vmem((hidden, width), BF16),
            vmem((width, hidden), BF16), vmem((hidden, width), BF16),
            vmem((16, 8, 128), F32),
            vmem(next_batch.shape, BF16), vmem(next_batch.shape, BF16), vmem(next_batch.shape, BF16),
            dma((10,)), dma((N_CHUNK,)), dma((N_CHUNK,)), dma((12,)), dma((12,)), dma((16,)), dma((16,)), dma((18 * N_PIECE,)), dma((18 * N_PIECE,)), dma((2 * N_PIECE,)), dma((2 * N_PIECE,)),
            dma((n_micro,)), dma((n_micro,)), dma((n_micro,)), dma((n_micro,)), dma((2,)), dma((2,)),
        ],
        compiler_params=pltpu.CompilerParams(collective_id=1, has_side_effects=True, vmem_limit_bytes=63 * 1024 * 1024),
    )(master_up, master_down, m1_up, m1_down, m2_up, m2_down, grad_up, grad_down, acts, loss_grad, next_batch, learn_rate, max_norm)


def finish_kernel(outs_in, late_in, w_up_in, w_down_in, *refs):
    news_in, outs, news_out = refs[:6], refs[6], refs[7:13]
    obuf, late, w_up, w_down, upd_up, upd_down, load_sem, store_sem, micro_load, micro_store, late_load = refs[13:]
    stage = lax.axis_index("stage")
    n_micro = obuf.shape[0]
    last = stage == 3
    n_copied = jnp.where(last, n_micro - N_LATE, n_micro)
    per_late = -(-(n_micro - N_LATE) // (N_LATE - 2))
    slots = [buf.at[i] for i in range(3) for buf in (upd_up, upd_down)]
    loads = [pltpu.make_async_copy(src, slot, load_sem.at[i]) for i, (src, slot) in enumerate(zip(news_in, slots))]
    stores = [pltpu.make_async_copy(slot, dst, store_sem.at[i]) for i, (slot, dst) in enumerate(zip(slots, news_out))]
    w_loads = [pltpu.make_async_copy(w_up_in, w_up, load_sem.at[6]), pltpu.make_async_copy(w_down_in, w_down, load_sem.at[7])]

    def place(k):
        return mixed(k, n_micro)[1]

    def load_micro(k):
        i = place(k)
        return pltpu.make_async_copy(outs_in.at[i], obuf.at[i], micro_load.at[i])

    def store_micro(k):
        i = place(k)
        return pltpu.make_async_copy(obuf.at[i], outs.at[i], micro_store.at[i])

    def load_late(n):
        return pltpu.make_async_copy(late_in.at[n], late.at[n], late_load.at[n])

    def start_micro(k, _):
        load_micro(k).start()
        return 0

    def turn_micro(k, _):
        load_micro(k).wait()
        store_micro(k).start()
        return 0

    def start_late(n, _):
        load_late(n).start()
        return 0

    @pl.when(last)
    def _():
        for copy in w_loads:
            copy.start()
        lax.fori_loop(0, N_LATE, start_late, 0)
    for copy in loads:
        copy.start()
    lax.fori_loop(0, n_copied, start_micro, 0)

    @pl.when(last)
    def _():
        for copy in w_loads:
            copy.wait()

        def body(n, _):
            load_late(n).wait()
            k = n_micro - N_LATE + n
            stage_rows(late.at[n], w_up, w_down, obuf.at[place(k)])
            store_micro(k).start()

            @pl.when(n == 1)
            def _():
                for load, store in zip(loads, stores):
                    load.wait()
                    store.start()
            for j in range(per_late):
                k = per_late * (n - 2) + j

                @pl.when((k >= 0) & (k < n_micro - N_LATE))
                def _():
                    turn_micro(k, 0)
            return 0
        lax.fori_loop(0, N_LATE, body, 0)

    @pl.when(jnp.logical_not(last))
    def _():
        for load, store in zip(loads, stores):
            load.wait()
            store.start()
        lax.fori_loop(0, n_micro, turn_micro, 0)

    def stored(k, _):
        store_micro(k).wait()
        return 0
    lax.fori_loop(0, n_micro, stored, 0)
    for copy in stores:
        copy.wait()


def finish_step(outs, late, w_up, w_down, *news):
    n_micro = outs.shape[0]
    hbm = pl.BlockSpec(memory_space=pl.ANY)
    vmem = pltpu.VMEM
    dma = pltpu.SemaphoreType.DMA
    return pl.pallas_call(
        finish_kernel,
        name="finish_step",
        out_shape=[jax.ShapeDtypeStruct(outs.shape, BF16)] + [jax.ShapeDtypeStruct(new.shape, F32) for new in news],
        in_specs=[hbm] * 10,
        out_specs=[hbm] * 7,
        scratch_shapes=[
            vmem(outs.shape, BF16), vmem(late.shape, BF16), vmem(w_up.shape, BF16), vmem(w_down.shape, BF16),
            vmem((3,) + news[0].shape, F32), vmem((3,) + news[1].shape, F32),
            dma((8,)), dma((6,)), dma((n_micro,)), dma((n_micro,)), dma((N_LATE,)),
        ],
        compiler_params=pltpu.CompilerParams(vmem_limit_bytes=56 * 1024 * 1024),
    )(outs, late, w_up, w_down, *news)


def solution(mesh):
    def local_step(master_up, master_down, mom1_up, mom1_down, mom2_up, mom2_down, grad_up, grad_down, stage_acts, loss_grad, next_batch, learn_rate, max_norm):
        stage_outs, *news, late, w_up, w_down = fused_step(
            master_up[0], master_down[0], mom1_up[0], mom1_down[0], mom2_up[0], mom2_down[0], grad_up[0, 0], grad_down[0, 0],
            stage_acts[0], loss_grad, next_batch, learn_rate.reshape(1), max_norm.reshape(1))
        stage_outs, new_up, new_down, new_m1_up, new_m1_down, new_m2_up, new_m2_down = finish_step(stage_outs, late, w_up, w_down, *news)
        return (new_up[None], new_down[None], new_m1_up[None], new_m1_down[None], new_m2_up[None], new_m2_down[None], stage_outs[None])

    w_spec = P('stage', None, None)
    g_spec = P('data', 'stage', None, None)
    in_specs = (w_spec, w_spec, w_spec, w_spec, w_spec, w_spec, g_spec, g_spec, P('stage', 'data', None), P('data', None), P(None, 'data', None), P(), P())
    out_specs = (w_spec, w_spec, w_spec, w_spec, w_spec, w_spec, P('stage', None, 'data', None))
    return jax.shard_map(local_step, mesh=mesh, in_specs=in_specs, out_specs=out_specs, check_vma=False)
```

```python
import jax
import jax.numpy as jnp
from jax import lax
from jax.experimental import pallas as pl
from jax.experimental.pallas import tpu as pltpu
from jax.sharding import PartitionSpec as P

BETA1 = 0.9
BETA2 = 0.95
ADAM_EPS = 1e-8
WEIGHT_DECAY = 0.1
NORM_EPS = 1e-6
ADAM_STEP = 8
SQRT_TWO_PI = 0.7978845608028654
GELU_CUBIC = 0.044715

N_SENT = 5
N_CHUNK = 4
N_LATE = 6
N_TWICE = 5
N_PIECE = 1
MESH = pl.DeviceIdType.MESH
BF16 = jnp.bfloat16
F32 = jnp.float32


def mat_tn(left, right):
    return lax.dot_general(left, right, (((0,), (0,)), ((), ())), preferred_element_type=F32)


def mat_nt(left, right):
    return lax.dot_general(left, right, (((1,), (1,)), ((), ())), preferred_element_type=F32)


def adamw_update(master, first_mom, second_mom, grad_avg, clip_scale, learn_rate):
    scaled = clip_scale * grad_avg
    new_first = BETA1 * first_mom + (1.0 - BETA1) * scaled
    new_second = BETA2 * second_mom + (1.0 - BETA2) * scaled * scaled
    first_hat = new_first * (1.0 / (1.0 - BETA1 ** ADAM_STEP))
    second_hat = new_second * (1.0 / (1.0 - BETA2 ** ADAM_STEP))
    new_master = master - learn_rate * (first_hat / (jnp.sqrt(second_hat) + ADAM_EPS) + WEIGHT_DECAY * master)
    return new_master, new_first, new_second


def gelu_of_half(half):
    t = jnp.tanh(half * (2.0 * SQRT_TWO_PI + (8.0 * SQRT_TWO_PI * GELU_CUBIC) * (half * half)))
    return half + half * t


def stage_rows(src, up_half, down, dst):
    x = src[...]
    half = jnp.dot(x, up_half[...], preferred_element_type=F32)
    hidden = gelu_of_half(half).astype(BF16)
    y = jnp.dot(hidden, down[...], preferred_element_type=F32)
    dst[...] = (x.astype(F32) + y).astype(BF16)


def mixed(k, n_micro):
    before = lax.div(k * N_SENT, n_micro)
    is_sent = lax.div((k + 1) * N_SENT, n_micro) - before
    return is_sent, is_sent * (n_micro - N_SENT + before) + (1 - is_sent) * (k - before)


def forward_part(stage, own_ready, aux_ready, relay_mean, nb_hbm, up_own, down_own, up_aux, down_aux, up_two, down_two, out_hbm, late_hbm, nbuf, xin, yout, nb_sem, out_sem, send_sem, recv_sem, two_send, two_recv):
    n_micro = nbuf.shape[0]
    n_kept = n_micro - N_SENT

    def load(i):
        return pltpu.make_async_copy(nb_hbm.at[i], nbuf.at[i], nb_sem.at[i])

    def store(i):
        return pltpu.make_async_copy(yout.at[i], out_hbm.at[i], out_sem.at[i])

    def push(src, i, peer):
        return pltpu.make_async_remote_copy(src_ref=src.at[i], dst_ref=xin.at[i], send_sem=send_sem.at[i], recv_sem=recv_sem.at[i], device_id={"stage": peer}, device_id_type=MESH)

    def arrived(i):
        push(yout, i, stage).wait_recv()

    def rotated(j):
        return lax.rem(j + n_kept, n_micro)

    def finish_stores():
        def body(i, _):
            store(i).wait()
            return 0
        lax.fori_loop(0, n_micro, body, 0)

    def hand_over():
        return [pltpu.make_async_remote_copy(src_ref=aux, dst_ref=two, send_sem=two_send.at[i], recv_sem=two_recv.at[i], device_id={"stage": 3}, device_id_type=MESH)
                for i, (aux, two) in enumerate([(up_aux, up_two), (down_aux, down_two)])]

    def finish_sends(first, count):
        def body(i, _):
            push(yout, first + i, stage).wait_send()
            return 0
        lax.fori_loop(0, count, body, 0)

    @pl.when(stage == 0)
    def _():
        own_ready()

        def body(j, _):
            i = rotated(j)
            load(i).wait()
            stage_rows(nbuf.at[i], up_own, down_own, yout.at[i])
            push(yout, i, 1).start()
            store(i).start()
            relay_mean(j == 7)
            return 0
        lax.fori_loop(0, n_micro, body, 0)
        finish_sends(0, n_micro)
        finish_stores()

    @pl.when(stage == 1)
    def _():
        own_ready()

        def body(j, _):
            i = rotated(j)
            arrived(i)
            stage_rows(xin.at[i], up_own, down_own, yout.at[i])

            @pl.when(j < N_SENT)
            def _():
                push(yout, i, 2).start()
            store(i).start()
            relay_mean(j == 7)
            return 0
        lax.fori_loop(0, n_micro, body, 0)
        finish_stores()

    @pl.when(stage == 2)
    def _():
        aux_ready()
        for copy in hand_over():
            copy.start()

        def body(k, _):
            _, i = mixed(k, n_micro)
            arrived(i)

            @pl.when(i < n_kept - N_TWICE)
            def _():
                stage_rows(xin.at[i], up_aux, down_aux, xin.at[i])
            stage_rows(xin.at[i], up_own, down_own, yout.at[i])
            push(yout, i, 3).start()
            store(i).start()
            return 0
        lax.fori_loop(0, n_micro, body, 0)
        finish_sends(0, n_micro)
        finish_stores()
        for copy in hand_over():
            copy.wait_send()

    @pl.when(stage == 3)
    def _():
        aux_ready()

        def first(j, _):
            load(j).wait()
            stage_rows(nbuf.at[j], up_aux, down_aux, nbuf.at[j])

            @pl.when(j == n_kept - N_TWICE)
            def _():
                for copy in hand_over():
                    copy.wait_recv()

            @pl.when(j >= n_kept - N_TWICE)
            def _():
                stage_rows(nbuf.at[j], up_two, down_two, nbuf.at[j])
            push(nbuf, j, 2).start()
            return 0
        lax.fori_loop(0, n_kept, first, 0)

        def body(k, _):
            _, i = mixed(k, n_micro)
            arrived(i)
            stage_rows(xin.at[i], up_own, down_own, yout.at[i])
            store(i).start()
            return 0
        lax.fori_loop(0, n_micro - N_LATE, body, 0)

        def late(k):
            _, i = mixed(k, n_micro)
            return i, pltpu.make_async_copy(xin.at[i], late_hbm.at[k - (n_micro - N_LATE)], out_sem.at[i])

        def save(k, _):
            i, copy = late(k)
            arrived(i)
            copy.start()
            return 0
        lax.fori_loop(n_micro - N_LATE, n_micro, save, 0)

        def stored(k, _):
            _, i = mixed(k, n_micro)
            store(i).wait()
            return 0
        lax.fori_loop(0, n_micro - N_LATE, stored, 0)

        def saved(k, _):
            late(k)[1].wait()
            return 0
        lax.fori_loop(n_micro - N_LATE, n_micro, saved, 0)
        finish_sends(0, n_kept)


def start_loads(stage, nb_hbm, nbuf, nb_sem):
    n_micro = nbuf.shape[0]
    n_kept = n_micro - N_SENT

    def body(j, _):
        i = lax.rem(j + n_kept, n_micro)
        pltpu.make_async_copy(nb_hbm.at[i], nbuf.at[i], nb_sem.at[i]).start()
        return 0

    @pl.when(stage == 0)
    def _():
        lax.fori_loop(0, n_micro, body, 0)

    @pl.when(stage == 3)
    def _():
        lax.fori_loop(N_SENT, n_micro, body, 0)


def step_kernel(up_hbm, down_hbm, m1_up_hbm, m1_down_hbm, m2_up_hbm, m2_down_hbm, gu_hbm, gv_hbm, acts_hbm, loss_hbm, nb_hbm, rate_ref, norm_ref,
                out_hbm, new_up_hbm, new_down_hbm, new_m1_up_hbm, new_m1_down_hbm, new_m2_up_hbm, new_m2_down_hbm, late_hbm, w_up_hbm, w_down_hbm,
                up32, down32, gu, gv, mean_up, mean_down, acts, gbuf, dxbuf, hid, slope, dpre, up_bf, down_bf,
                ru1, rv1, ru2, rv2, m_up, m_down, up_own, down_own, up_aux, down_aux, up_two, down_two, sq_all, nbuf, xin, yout,
                in_sem, g_send, g_recv, rs_send, rs_recv, sq_send, sq_recv, ag_send, ag_recv, aux_send, aux_recv,
                nb_sem, out_sem, send_sem, recv_sem, two_send, two_recv):
    stage = lax.axis_index("stage")
    data = lax.axis_index("data")
    z = lax.div(data, 2)
    y = lax.rem(data, 2)
    me = data * 4 + stage
    z_peer = 2 * (1 - z) + y
    y_peer = 2 * z + (1 - y)
    n_tok = acts.shape[0]
    chunk = n_tok // N_CHUNK

    def up_rows(zz, yy, first=0, count=64):
        return pl.ds(pl.multiple_of(128 * yy + 64 * zz + first, 32), count)

    def down_rows(zz, yy, first=0, count=256):
        return pl.ds(pl.multiple_of(512 * zz + 256 * yy + first, 128), count)

    own_up, own_down = up_rows(z, y), down_rows(z, y)
    loads = [
        pltpu.make_async_copy(acts_hbm, acts, in_sem.at[0]),
        pltpu.make_async_copy(up_hbm, up32, in_sem.at[1]),
        pltpu.make_async_copy(down_hbm, down32, in_sem.at[2]),
        pltpu.make_async_copy(gv_hbm, gv, in_sem.at[3]),
        pltpu.make_async_copy(gu_hbm, gu, in_sem.at[4]),
        pltpu.make_async_copy(m1_up_hbm, m_up.at[0], in_sem.at[5]),
        pltpu.make_async_copy(m2_up_hbm, m_up.at[1], in_sem.at[6]),
        pltpu.make_async_copy(m1_down_hbm, m_down.at[0], in_sem.at[7]),
        pltpu.make_async_copy(m2_down_hbm, m_down.at[1], in_sem.at[8]),
    ]
    load_loss = pltpu.make_async_copy(loss_hbm, gbuf, in_sem.at[9])
    for copy in loads[:2]:
        copy.start()

    @pl.when(stage == 3)
    def _():
        load_loss.start()
    loads[2].start()

    barrier = pltpu.get_barrier_semaphore()

    def greet(d, _):
        other = lax.rem(me + d, 16)
        pl.semaphore_signal(barrier, inc=1, device_id={"data": lax.div(other, 4), "stage": lax.rem(other, 4)}, device_id_type=MESH)
        return 0
    lax.fori_loop(1, 16, greet, 0)

    def chunk_rows(k):
        return pl.ds(pl.multiple_of(k * chunk, chunk), chunk)

    def pass_down(k):
        rows = chunk_rows(k)
        return pltpu.make_async_remote_copy(src_ref=dxbuf.at[rows], dst_ref=gbuf.at[rows], send_sem=g_send.at[k], recv_sem=g_recv.at[k],
                                            device_id={"stage": jnp.maximum(stage - 1, 0)}, device_id_type=MESH)

    def prepare(k):
        rows = chunk_rows(k)
        pre = jnp.dot(acts[rows, :], up_bf[...], preferred_element_type=F32)
        sq = pre * pre
        half_t = 0.5 * jnp.tanh(pre * (SQRT_TWO_PI + (SQRT_TWO_PI * GELU_CUBIC) * sq))
        prob = 0.5 + half_t
        rest = 0.5 - half_t
        hid[rows, :] = (pre * prob).astype(BF16)
        slope[rows, :] = prob + (prob * rest) * pre * (2.0 * SQRT_TWO_PI + (6.0 * SQRT_TWO_PI * GELU_CUBIC) * sq)

    def backward(k):
        rows = chunk_rows(k)

        @pl.when(stage < 3)
        def _():
            pass_down(k).wait_recv()
        grad = gbuf[rows, :]
        d_pre = (mat_nt(grad, down_bf[...]) * slope[rows, :]).astype(BF16)
        dpre[rows, :] = d_pre

        @pl.when(stage > 0)
        def _():
            dxbuf[rows, :] = (grad.astype(F32) + mat_nt(d_pre, up_bf[...])).astype(BF16)
            pass_down(k).start()

    def rs_copy(src, dst, sem, peer):
        return pltpu.make_async_remote_copy(src_ref=src, dst_ref=dst, send_sem=rs_send.at[sem], recv_sem=rs_recv.at[sem], device_id={"data": peer}, device_id_type=MESH)

    def v_first(sub, c):
        yy = (1 - y) if sub == 0 else y
        return rs_copy(gv.at[down_rows(1 - z, yy, 128 * c, 128)], rv1.at[sub, pl.ds(128 * c, 128)], 2 * sub + c, z_peer)

    def u_first(sub, c):
        zz = (1 - z) if sub == 0 else z
        return rs_copy(gu.at[up_rows(zz, 1 - y, 32 * c, 32)], ru1.at[sub, pl.ds(32 * c, 32)], 4 + 2 * sub + c, y_peer)

    def v_second(c):
        return rs_copy(gv.at[down_rows(z, 1 - y, 128 * c, 128)], rv2.at[pl.ds(128 * c, 128)], 8 + c, y_peer)

    def u_second(c):
        return rs_copy(gu.at[up_rows(1 - z, y, 32 * c, 32)], ru2.at[pl.ds(32 * c, 32)], 10 + c, z_peer)

    def add_grads(k):
        rows = chunk_rows(k)

        @pl.when(k == 0)
        def _():
            loads[3].wait()
            loads[4].wait()

        def half(h, _):
            zz = h * z + (1 - h) * (1 - z)
            yy = h * y + (1 - h) * (1 - y)
            send = (k == N_CHUNK - 1) & (h == 0)
            out = pl.ds(pl.multiple_of(512 * zz, 512), 512)
            gv[out, :] += mat_tn(hid[rows, out], gbuf[rows, :])

            @pl.when(send)
            def _():
                for sub in range(2):
                    for c in range(2):
                        v_first(sub, c).start()
            out = pl.ds(pl.multiple_of(128 * yy, 128), 128)
            gu[out, :] += mat_tn(acts[rows, out], dpre[rows, :])

            @pl.when(send)
            def _():
                for sub in range(2):
                    for c in range(2):
                        u_first(sub, c).start()
            return 0
        lax.fori_loop(0, 2, half, 0)

    def tick(t, _):
        upper = jnp.where(stage >= 2, 1, 0)
        even = 1 - lax.rem(t, 2)
        early = jnp.where(t < N_CHUNK, 1, 0)
        late = jnp.where(t >= 2 * N_CHUNK, 1, 0)
        is_prep = upper * even * (1 - late) + (1 - upper) * early
        is_grad = upper * late + (1 - upper) * (1 - early) * (1 - even)
        k = upper * (late * (t - 2 * N_CHUNK) + (1 - late) * lax.div(t, 2)) + (1 - upper) * (early * t + (1 - early) * lax.div(t - N_CHUNK, 2))

        @pl.when(is_prep == 1)
        def _():
            prepare(k)

        @pl.when(is_prep + is_grad == 0)
        def _():
            backward(k)

        @pl.when(is_grad == 1)
        def _():
            add_grads(k)
        return 0

    loads[0].wait()
    loads[1].wait()
    up_bf[...] = up32[...].astype(BF16)
    prepare(0)
    loads[2].wait()
    for copy in loads[3:]:
        copy.start()
    start_loads(stage, nb_hbm, nbuf, nb_sem)
    down_bf[...] = down32[...].astype(BF16)
    pl.semaphore_wait(barrier, 15)

    @pl.when(stage == 3)
    def _():
        load_loss.wait()
    lax.fori_loop(1, 3 * N_CHUNK, tick, 0)

    for c in range(2):
        v_first(0, c).wait_recv()
        rows = down_rows(z, 1 - y, 128 * c, 128)
        gv[rows, :] += rv1[0, 128 * c:128 * (c + 1), :]
        v_second(c).start()
        u_first(0, c).wait_recv()
        rows = up_rows(1 - z, y, 32 * c, 32)
        gu[rows, :] += ru1[0, 32 * c:32 * (c + 1), :]
        u_second(c).start()
    acc = jnp.zeros((8, 128), F32)

    def fold(tile, acc):
        sq = tile * tile
        sq = jnp.sum(sq.reshape(sq.shape[0] // 8, 8, sq.shape[1]), axis=0)
        for i in range(0, sq.shape[1], 128):
            acc = acc + sq[:, i:i + 128]
        return acc

    for c in range(2):
        v_first(1, c).wait_recv()
        v_second(c).wait_recv()
        rows = down_rows(z, y, 128 * c, 128)
        mean = (gv[rows, :] + rv1[1, 128 * c:128 * (c + 1), :] + rv2[128 * c:128 * (c + 1), :]) * 0.25
        mean_down[rows, :] = mean
        acc = fold(mean, acc)
        u_first(1, c).wait_recv()
        u_second(c).wait_recv()
        rows = up_rows(z, y, 32 * c, 32)
        mean = (gu[rows, :] + ru1[1, 32 * c:32 * (c + 1), :] + ru2[32 * c:32 * (c + 1), :]) * 0.25
        mean_up[rows, :] = mean
        acc = fold(mean, acc)

    up_piece, down_piece = 64 // N_PIECE, 256 // N_PIECE

    def gather(which, up, down):
        def copy(ref, rows, sem, piece, peer):
            sem = (which * 6 + sem) * N_PIECE + piece
            return pltpu.make_async_remote_copy(src_ref=ref.at[rows], dst_ref=ref.at[rows], send_sem=ag_send.at[sem], recv_sem=ag_recv.at[sem],
                                                device_id={"data": peer}, device_id_type=MESH)

        def up_copy(zz, yy, sem, p, peer):
            return copy(up, up_rows(zz, yy, up_piece * p, up_piece), sem, p, peer)

        def down_copy(zz, yy, sem, p, peer):
            return copy(down, down_rows(zz, yy, down_piece * p, down_piece), sem, p, peer)

        def up_sends(p):
            return [up_copy(z, y, 0, p, z_peer), up_copy(z, y, 1, p, y_peer)]

        def down_sends(p):
            return [down_copy(z, y, 3, p, y_peer), down_copy(z, y, 4, p, z_peer)]

        def relays(p):
            return [(up_copy(1 - z, y, 0, p, z_peer), up_copy(1 - z, y, 2, p, y_peer)), (down_copy(z, 1 - y, 3, p, y_peer), down_copy(z, 1 - y, 5, p, z_peer))]

        def begin(matrix, hops=(0, 1)):
            for p in range(N_PIECE):
                for hop in hops:
                    (up_sends, down_sends)[matrix](p)[hop].start()

        def relay():
            for p in range(N_PIECE):
                for arrived, onward in relays(p):
                    arrived.wait_recv()
                    onward.start()

        def finish():
            for p in range(N_PIECE):
                for c in (up_copy(z, 1 - y, 1, p, y_peer), down_copy(1 - z, y, 4, p, z_peer), up_copy(1 - z, 1 - y, 2, p, y_peer), down_copy(1 - z, 1 - y, 5, p, z_peer)):
                    c.wait_recv()

        def drain():
            for p in range(N_PIECE):
                for c in up_sends(p) + down_sends(p) + [onward for _, onward in relays(p)]:
                    c.wait_send()
        return begin, relay, finish, drain

    own_begin, own_relay, own_finish, own_drain = gather(0, up_own, down_own)
    aux_begin, aux_relay, aux_finish, aux_drain = gather(1, up_aux, down_aux)
    mean_begin, mean_relay, mean_finish, mean_drain = gather(2, mean_up, mean_down)

    def sq_copy(other, slot):
        return pltpu.make_async_remote_copy(src_ref=sq_all.at[slot], dst_ref=sq_all.at[slot], send_sem=sq_send.at[other], recv_sem=sq_recv.at[slot],
                                            device_id={"data": lax.div(other, 4), "stage": lax.rem(other, 4)}, device_id_type=MESH)

    sq_all[me] = acc

    def tell(d, _):
        sq_copy(lax.rem(me + d, 16), me).start()
        return 0
    lax.fori_loop(1, 16, tell, 0)
    for copy in loads[5:]:
        copy.wait()

    @pl.when(stage >= 2)
    def _():
        mean_begin(0)
        mean_begin(1)
        mean_relay()
        mean_finish()

    def hear(d, _):
        other = lax.rem(me + d, 16)
        sq_copy(other, other).wait_recv()
        return 0
    lax.fori_loop(1, 16, hear, 0)
    total = sq_all[0]
    for i in range(1, 16):
        total = total + sq_all[i]
    total = jnp.sum(jnp.sum(total, axis=0, keepdims=True), axis=1, keepdims=True)
    clip = jnp.minimum(1.0, norm_ref[0] / (jnp.sqrt(total) + NORM_EPS))

    rate = rate_ref[0]

    def renew(rows, master, moments, mean, weights, scale, first, full):
        new = adamw_update(master[rows, :], moments[0, rows, :], moments[1, rows, :], mean[rows, :], clip, rate)
        if first:
            weights[rows, :] = new[0].astype(BF16) * jnp.asarray(scale, BF16)

        if full:
            master[rows, :] = new[0]
            moments[0, rows, :] = new[1]
            moments[1, rows, :] = new[2]

    def renew_up(block, first, full):
        renew(pl.ds(pl.multiple_of(64 * block, 64), 64), up32, m_up, mean_up, up_own, 0.5, first, full)

    def renew_down(block, first, full):
        renew(pl.ds(pl.multiple_of(256 * block, 256), 256), down32, m_down, mean_down, down_own, 1.0, first, full)

    def renew_all(first):
        def body(t, _):
            renew_up(t, first, True)
            renew_down(t, first, True)
            return 0
        lax.fori_loop(0, 4, body, 0)

    new_stores = [pltpu.make_async_copy(src, dst, in_sem.at[i]) for i, (src, dst) in enumerate((
        (up32, new_up_hbm), (down32, new_down_hbm), (m_up.at[0], new_m1_up_hbm), (m_down.at[0], new_m1_down_hbm), (m_up.at[1], new_m2_up_hbm), (m_down.at[1], new_m2_down_hbm)))]
    def feed(p):
        parts = [(up_own, up_aux, up_rows(z, y, up_piece * p, up_piece)), (down_own, down_aux, down_rows(z, y, down_piece * p, down_piece))]
        return [pltpu.make_async_remote_copy(src_ref=own.at[rows], dst_ref=aux.at[rows], send_sem=aux_send.at[2 * p + i], recv_sem=aux_recv.at[2 * p + i], device_id={"stage": 3 - stage}, device_id_type=MESH)
                for i, (own, aux, rows) in enumerate(parts)]

    @pl.when(stage < 2)
    def _():
        renew_up(2 * y + z, True, False)
        for p in range(N_PIECE):
            feed(p)[0].start()
        own_begin(0, (0,))
        renew_down(2 * z + y, True, False)
        for p in range(N_PIECE):
            feed(p)[1].start()
        own_begin(1, (0,))
        own_begin(0, (1,))
        own_begin(1, (1,))
        own_relay()
        mean_begin(0)
        mean_begin(1)

    @pl.when(stage >= 2)
    def _():
        for matrix in range(2):
            for p in range(N_PIECE):
                feed(p)[matrix].wait_recv()
            aux_begin(matrix)
        renew_all(True)
        for copy in new_stores:
            copy.start()
        aux_relay()

    def relay_mean(now):
        @pl.when(now)
        def _():
            mean_relay()

    forward_part(stage, own_finish, aux_finish, relay_mean, nb_hbm, up_own, down_own, up_aux, down_aux, up_two, down_two, out_hbm, late_hbm, nbuf, xin, yout, nb_sem, out_sem, send_sem, recv_sem, two_send, two_recv)

    @pl.when(stage < 2)
    def _():
        mean_finish()
        renew_all(False)
        for copy in new_stores:
            copy.start()
    store_w_up = pltpu.make_async_copy(up_own, w_up_hbm, in_sem.at[6])
    store_w_down = pltpu.make_async_copy(down_own, w_down_hbm, in_sem.at[7])
    store_w_up.start()
    store_w_down.start()

    @pl.when(stage == 1)
    def _():
        def left(i, _):
            pltpu.make_async_remote_copy(src_ref=yout.at[i], dst_ref=xin.at[i], send_sem=send_sem.at[i], recv_sem=recv_sem.at[i], device_id={"stage": 2}, device_id_type=MESH).wait_send()
            return 0
        lax.fori_loop(nbuf.shape[0] - N_SENT, nbuf.shape[0], left, 0)

    @pl.when(stage > 0)
    def _():
        for k in range(N_CHUNK):
            pass_down(k).wait_send()
    for c in range(2):
        for sub in range(2):
            v_first(sub, c).wait_send()
            u_first(sub, c).wait_send()
        v_second(c).wait_send()
        u_second(c).wait_send()

    def told(d, _):
        sq_copy(lax.rem(me + d, 16), me).wait_send()
        return 0
    lax.fori_loop(1, 16, told, 0)
    mean_drain()

    @pl.when(stage < 2)
    def _():
        own_drain()
        for p in range(N_PIECE):
            for c in feed(p):
                c.wait_send()

    @pl.when(stage >= 2)
    def _():
        aux_drain()
    for copy in new_stores:
        copy.wait()
    store_w_up.wait()
    store_w_down.wait()


def fused_step(master_up, master_down, m1_up, m1_down, m2_up, m2_down, grad_up, grad_down, acts, loss_grad, next_batch, learn_rate, max_norm):
    n_micro = next_batch.shape[0]
    n_tok, width = acts.shape
    hidden = master_up.shape[1]
    hbm = pl.BlockSpec(memory_space=pl.ANY)
    smem = pl.BlockSpec(memory_space=pltpu.SMEM)
    vmem = pltpu.VMEM
    dma = pltpu.SemaphoreType.DMA
    return pl.pallas_call(
        step_kernel,
        name="pipeline_step",
        out_shape=[jax.ShapeDtypeStruct(next_batch.shape, BF16)] + [jax.ShapeDtypeStruct((width, hidden), F32), jax.ShapeDtypeStruct((hidden, width), F32)] * 3 + [
            jax.ShapeDtypeStruct((N_LATE,) + next_batch.shape[1:], BF16), jax.ShapeDtypeStruct((width, hidden), BF16), jax.ShapeDtypeStruct((hidden, width), BF16)],
        in_specs=[hbm] * 11 + [smem] * 2,
        out_specs=[hbm] * 10,
        scratch_shapes=[
            vmem((width, hidden), F32), vmem((hidden, width), F32),
            vmem((width, hidden), F32), vmem((hidden, width), F32),
            vmem((width, hidden), F32), vmem((hidden, width), F32),
            vmem((n_tok, width), BF16), vmem((n_tok, width), BF16), vmem((n_tok, width), BF16),
            vmem((n_tok, hidden), BF16), vmem((n_tok, hidden), F32), vmem((n_tok, hidden), BF16),
            vmem((width, hidden), BF16), vmem((hidden, width), BF16),
            vmem((2, width // 4, hidden), F32), vmem((2, hidden // 4, width), F32),
            vmem((width // 4, hidden), F32), vmem((hidden // 4, width), F32),
            vmem((2, width, hidden), F32), vmem((2, hidden, width), F32),
            vmem((width, hidden), BF16), vmem((hidden, width), BF16),
            vmem((width, hidden), BF16), vmem((hidden, width), BF16),
            vmem((width, hidden), BF16), vmem((hidden, width), BF16),
            vmem((16, 8, 128), F32),
            vmem(next_batch.shape, BF16), vmem(next_batch.shape, BF16), vmem(next_batch.shape, BF16),
            dma((10,)), dma((N_CHUNK,)), dma((N_CHUNK,)), dma((12,)), dma((12,)), dma((16,)), dma((16,)), dma((18 * N_PIECE,)), dma((18 * N_PIECE,)), dma((2 * N_PIECE,)), dma((2 * N_PIECE,)),
            dma((n_micro,)), dma((n_micro,)), dma((n_micro,)), dma((n_micro,)), dma((2,)), dma((2,)),
        ],
        compiler_params=pltpu.CompilerParams(collective_id=1, has_side_effects=True, vmem_limit_bytes=63 * 1024 * 1024),
    )(master_up, master_down, m1_up, m1_down, m2_up, m2_down, grad_up, grad_down, acts, loss_grad, next_batch, learn_rate, max_norm)


def finish_kernel(outs_in, late_in, w_up_in, w_down_in, *refs):
    news_in, outs, news_out = refs[:6], refs[6], refs[7:13]
    obuf, late, w_up, w_down, upd_up, upd_down, load_sem, store_sem, micro_load, micro_store, late_load = refs[13:]
    stage = lax.axis_index("stage")
    n_micro = obuf.shape[0]
    last = stage == 3
    n_copied = jnp.where(last, n_micro - N_LATE, n_micro)
    per_late = -(-(n_micro - N_LATE) // (N_LATE - 2))
    slots = [buf.at[i] for i in range(3) for buf in (upd_up, upd_down)]
    loads = [pltpu.make_async_copy(src, slot, load_sem.at[i]) for i, (src, slot) in enumerate(zip(news_in, slots))]
    stores = [pltpu.make_async_copy(slot, dst, store_sem.at[i]) for i, (slot, dst) in enumerate(zip(slots, news_out))]
    w_loads = [pltpu.make_async_copy(w_up_in, w_up, load_sem.at[6]), pltpu.make_async_copy(w_down_in, w_down, load_sem.at[7])]

    def place(k):
        return mixed(k, n_micro)[1]

    def load_micro(k):
        i = place(k)
        return pltpu.make_async_copy(outs_in.at[i], obuf.at[i], micro_load.at[i])

    def store_micro(k):
        i = place(k)
        return pltpu.make_async_copy(obuf.at[i], outs.at[i], micro_store.at[i])

    def load_late(n):
        return pltpu.make_async_copy(late_in.at[n], late.at[n], late_load.at[n])

    def start_micro(k, _):
        load_micro(k).start()
        return 0

    def turn_micro(k, _):
        load_micro(k).wait()
        store_micro(k).start()
        return 0

    def start_late(n, _):
        load_late(n).start()
        return 0

    @pl.when(last)
    def _():
        for copy in w_loads:
            copy.start()
        lax.fori_loop(0, N_LATE, start_late, 0)
    for copy in loads:
        copy.start()
    lax.fori_loop(0, n_copied, start_micro, 0)

    @pl.when(last)
    def _():
        for copy in w_loads:
            copy.wait()

        def body(n, _):
            load_late(n).wait()
            k = n_micro - N_LATE + n
            stage_rows(late.at[n], w_up, w_down, obuf.at[place(k)])
            store_micro(k).start()

            @pl.when(n == 1)
            def _():
                for load, store in zip(loads, stores):
                    load.wait()
                    store.start()
            for j in range(per_late):
                k = per_late * (n - 2) + j

                @pl.when((k >= 0) & (k < n_micro - N_LATE))
                def _():
                    turn_micro(k, 0)
            return 0
        lax.fori_loop(0, N_LATE, body, 0)

    @pl.when(jnp.logical_not(last))
    def _():
        for load, store in zip(loads, stores):
            load.wait()
            store.start()
        lax.fori_loop(0, n_micro, turn_micro, 0)

    def stored(k, _):
        store_micro(k).wait()
        return 0
    lax.fori_loop(0, n_micro, stored, 0)
    for copy in stores:
        copy.wait()


def finish_step(outs, late, w_up, w_down, *news):
    n_micro = outs.shape[0]
    hbm = pl.BlockSpec(memory_space=pl.ANY)
    vmem = pltpu.VMEM
    dma = pltpu.SemaphoreType.DMA
    return pl.pallas_call(
        finish_kernel,
        name="finish_step",
        out_shape=[jax.ShapeDtypeStruct(outs.shape, BF16)] + [jax.ShapeDtypeStruct(new.shape, F32) for new in news],
        in_specs=[hbm] * 10,
        out_specs=[hbm] * 7,
        scratch_shapes=[
            vmem(outs.shape, BF16), vmem(late.shape, BF16), vmem(w_up.shape, BF16), vmem(w_down.shape, BF16),
            vmem((3,) + news[0].shape, F32), vmem((3,) + news[1].shape, F32),
            dma((8,)), dma((6,)), dma((n_micro,)), dma((n_micro,)), dma((N_LATE,)),
        ],
        compiler_params=pltpu.CompilerParams(vmem_limit_bytes=56 * 1024 * 1024),
    )(outs, late, w_up, w_down, *news)


def solution(mesh):
    def local_step(master_up, master_down, mom1_up, mom1_down, mom2_up, mom2_down, grad_up, grad_down, stage_acts, loss_grad, next_batch, learn_rate, max_norm):
        stage_outs, *news, late, w_up, w_down = fused_step(
            master_up[0], master_down[0], mom1_up[0], mom1_down[0], mom2_up[0], mom2_down[0], grad_up[0, 0], grad_down[0, 0],
            stage_acts[0], loss_grad, next_batch, learn_rate.reshape(1), max_norm.reshape(1))
        stage_outs, new_up, new_down, new_m1_up, new_m1_down, new_m2_up, new_m2_down = finish_step(stage_outs, late, w_up, w_down, *news)
        return (new_up[None], new_down[None], new_m1_up[None], new_m1_down[None], new_m2_up[None], new_m2_down[None], stage_outs[None])

    w_spec = P('stage', None, None)
    g_spec = P('data', 'stage', None, None)
    in_specs = (w_spec, w_spec, w_spec, w_spec, w_spec, w_spec, g_spec, g_spec, P('stage', 'data', None), P('data', None), P(None, 'data', None), P(), P())
    out_specs = (w_spec, w_spec, w_spec, w_spec, w_spec, w_spec, P('stage', None, 'data', None))
    return jax.shard_map(local_step, mesh=mesh, in_specs=in_specs, out_specs=out_specs, check_vma=False)
```

```python
import jax
import jax.numpy as jnp
from jax import lax
from jax.experimental import pallas as pl
from jax.experimental.pallas import tpu as pltpu
from jax.sharding import PartitionSpec as P

BETA1 = 0.9
BETA2 = 0.95
ADAM_EPS = 1e-8
WEIGHT_DECAY = 0.1
NORM_EPS = 1e-6
ADAM_STEP = 8
SQRT_TWO_PI = 0.7978845608028654
GELU_CUBIC = 0.044715

N_SENT = 5
N_CHUNK = 4
N_LATE = 6
N_TWICE = 6
N_PIECE = 2
MESH = pl.DeviceIdType.MESH
BF16 = jnp.bfloat16
F32 = jnp.float32


def repeat(first, end, body):
    def step(i, _):
        body(i)
        return 0
    lax.fori_loop(first, end, step, 0)


def mat_tn(left, right):
    return lax.dot_general(left, right, (((0,), (0,)), ((), ())), preferred_element_type=F32)


def mat_nt(left, right):
    return lax.dot_general(left, right, (((1,), (1,)), ((), ())), preferred_element_type=F32)


def adamw_update(master, first_mom, second_mom, grad_avg, clip_scale, learn_rate):
    scaled = clip_scale * grad_avg
    new_first = BETA1 * first_mom + (1.0 - BETA1) * scaled
    new_second = BETA2 * second_mom + (1.0 - BETA2) * scaled * scaled
    first_hat = new_first * (1.0 / (1.0 - BETA1 ** ADAM_STEP))
    second_hat = new_second * (1.0 / (1.0 - BETA2 ** ADAM_STEP))
    new_master = master - learn_rate * (first_hat / (jnp.sqrt(second_hat) + ADAM_EPS) + WEIGHT_DECAY * master)
    return new_master, new_first, new_second


def gelu_of_half(half):
    t = jnp.tanh(half * (2.0 * SQRT_TWO_PI + (8.0 * SQRT_TWO_PI * GELU_CUBIC) * (half * half)))
    return half + half * t


def stage_rows(src, up_half, down, dst):
    x = src[...]
    half = jnp.dot(x, up_half[...], preferred_element_type=F32)
    hidden = gelu_of_half(half).astype(BF16)
    y = jnp.dot(hidden, down[...], preferred_element_type=F32)
    dst[...] = (x.astype(F32) + y).astype(BF16)


def mixed(k, n_micro):
    before = lax.div(k * N_SENT, n_micro)
    is_sent = lax.div((k + 1) * N_SENT, n_micro) - before
    return is_sent, is_sent * (n_micro - N_SENT + before) + (1 - is_sent) * (k - before)


def forward_part(stage, own_ready, aux_ready, relay_mean, nb_hbm, up_own, down_own, up_aux, down_aux, up_two, down_two, out_hbm, late_hbm, nbuf, xin, yout, nb_sem, out_sem, send_sem, recv_sem, two_send, two_recv):
    n_micro = nbuf.shape[0]
    n_kept = n_micro - N_SENT

    def load(i):
        return pltpu.make_async_copy(nb_hbm.at[i], nbuf.at[i], nb_sem.at[i])

    def store(i):
        return pltpu.make_async_copy(yout.at[i], out_hbm.at[i], out_sem.at[i])

    def push(src, i, peer):
        return pltpu.make_async_remote_copy(src_ref=src.at[i], dst_ref=xin.at[i], send_sem=send_sem.at[i], recv_sem=recv_sem.at[i], device_id={"stage": peer}, device_id_type=MESH)

    def arrived(i):
        push(yout, i, stage).wait_recv()

    def rotated(j):
        return lax.rem(j + n_kept, n_micro)

    def finish_stores():
        def body(i):
            store(i).wait()
        repeat(0, n_micro, body)

    def hand_over():
        return [pltpu.make_async_remote_copy(src_ref=aux, dst_ref=two, send_sem=two_send.at[i], recv_sem=two_recv.at[i], device_id={"stage": 3}, device_id_type=MESH)
                for i, (aux, two) in enumerate([(up_aux, up_two), (down_aux, down_two)])]

    def finish_sends(first, count):
        def body(i):
            push(yout, first + i, stage).wait_send()
        repeat(0, count, body)

    @pl.when(stage == 0)
    def _():
        own_ready()

        def body(j):
            i = rotated(j)
            load(i).wait()
            stage_rows(nbuf.at[i], up_own, down_own, yout.at[i])
            push(yout, i, 1).start()
            store(i).start()
            relay_mean(j == 7)
        repeat(0, n_micro, body)
        finish_sends(0, n_micro)
        finish_stores()

    @pl.when(stage == 1)
    def _():
        own_ready()

        def body(j):
            i = rotated(j)
            arrived(i)
            stage_rows(xin.at[i], up_own, down_own, yout.at[i])

            @pl.when(j < N_SENT)
            def _():
                push(yout, i, 2).start()
            store(i).start()
            relay_mean(j == 7)
        repeat(0, n_micro, body)
        finish_stores()

    @pl.when(stage == 2)
    def _():
        aux_ready()
        for copy in hand_over():
            copy.start()

        def body(k):
            _, i = mixed(k, n_micro)
            arrived(i)

            @pl.when(i < n_kept - N_TWICE)
            def _():
                stage_rows(xin.at[i], up_aux, down_aux, xin.at[i])
            stage_rows(xin.at[i], up_own, down_own, yout.at[i])
            push(yout, i, 3).start()
            store(i).start()
        repeat(0, n_micro, body)
        finish_sends(0, n_micro)
        finish_stores()
        for copy in hand_over():
            copy.wait_send()

    @pl.when(stage == 3)
    def _():
        aux_ready()

        def first(j):
            load(j).wait()
            stage_rows(nbuf.at[j], up_aux, down_aux, nbuf.at[j])

            @pl.when(j == n_kept - N_TWICE)
            def _():
                for copy in hand_over():
                    copy.wait_recv()

            @pl.when(j >= n_kept - N_TWICE)
            def _():
                stage_rows(nbuf.at[j], up_two, down_two, nbuf.at[j])
            push(nbuf, j, 2).start()
        repeat(0, n_kept, first)

        def body(k):
            _, i = mixed(k, n_micro)
            arrived(i)
            stage_rows(xin.at[i], up_own, down_own, yout.at[i])
            store(i).start()
        repeat(0, n_micro - N_LATE, body)

        def late(k):
            _, i = mixed(k, n_micro)
            return i, pltpu.make_async_copy(xin.at[i], late_hbm.at[k - (n_micro - N_LATE)], out_sem.at[i])

        def save(k):
            i, copy = late(k)
            arrived(i)
            copy.start()
        repeat(n_micro - N_LATE, n_micro, save)

        def stored(k):
            _, i = mixed(k, n_micro)
            store(i).wait()
        repeat(0, n_micro - N_LATE, stored)

        def saved(k):
            late(k)[1].wait()
        repeat(n_micro - N_LATE, n_micro, saved)
        finish_sends(0, n_kept)


def start_loads(stage, nb_hbm, nbuf, nb_sem):
    n_micro = nbuf.shape[0]
    n_kept = n_micro - N_SENT

    def body(j):
        i = lax.rem(j + n_kept, n_micro)
        pltpu.make_async_copy(nb_hbm.at[i], nbuf.at[i], nb_sem.at[i]).start()

    @pl.when(stage == 0)
    def _():
        repeat(0, n_micro, body)

    @pl.when(stage == 3)
    def _():
        repeat(N_SENT, n_micro, body)


def step_kernel(up_hbm, down_hbm, m1_up_hbm, m1_down_hbm, m2_up_hbm, m2_down_hbm, gu_hbm, gv_hbm, acts_hbm, loss_hbm, nb_hbm, rate_ref, norm_ref,
                out_hbm, new_up_hbm, new_down_hbm, new_m1_up_hbm, new_m1_down_hbm, new_m2_up_hbm, new_m2_down_hbm, late_hbm, w_up_hbm, w_down_hbm,
                up32, down32, gu, gv, mean_up, mean_down, acts, gbuf, dxbuf, hid, slope, dpre, up_bf, down_bf,
                ru1, rv1, ru2, rv2, m_up, m_down, up_own, down_own, up_aux, down_aux, up_two, down_two, sq_all, nbuf, xin, yout,
                in_sem, g_send, g_recv, rs_send, rs_recv, sq_send, sq_recv, ag_send, ag_recv, aux_send, aux_recv,
                nb_sem, out_sem, send_sem, recv_sem, two_send, two_recv):
    stage = lax.axis_index("stage")
    data = lax.axis_index("data")
    z = lax.div(data, 2)
    y = lax.rem(data, 2)
    me = data * 4 + stage
    z_peer = 2 * (1 - z) + y
    y_peer = 2 * z + (1 - y)
    n_tok = acts.shape[0]
    chunk = n_tok // N_CHUNK

    def up_rows(zz, yy, first=0, count=64):
        return pl.ds(pl.multiple_of(128 * yy + 64 * zz + first, 32), count)

    def down_rows(zz, yy, first=0, count=256):
        return pl.ds(pl.multiple_of(512 * zz + 256 * yy + first, 128), count)

    own_up, own_down = up_rows(z, y), down_rows(z, y)
    loads = [pltpu.make_async_copy(src, dst, in_sem.at[i]) for i, (src, dst) in enumerate((
        (acts_hbm, acts), (up_hbm, up32), (down_hbm, down32), (gv_hbm, gv), (gu_hbm, gu),
        (m1_up_hbm, m_up.at[0]), (m2_up_hbm, m_up.at[1]), (m1_down_hbm, m_down.at[0]), (m2_down_hbm, m_down.at[1])))]
    load_loss = pltpu.make_async_copy(loss_hbm, gbuf, in_sem.at[9])
    for copy in loads[:2]:
        copy.start()

    @pl.when(stage == 3)
    def _():
        load_loss.start()
    loads[2].start()

    barrier = pltpu.get_barrier_semaphore()

    def greet(d):
        other = lax.rem(me + d, 16)
        pl.semaphore_signal(barrier, inc=1, device_id={"data": lax.div(other, 4), "stage": lax.rem(other, 4)}, device_id_type=MESH)
    repeat(1, 16, greet)

    def chunk_rows(k):
        return pl.ds(pl.multiple_of(k * chunk, chunk), chunk)

    def pass_down(k):
        rows = chunk_rows(k)
        return pltpu.make_async_remote_copy(src_ref=dxbuf.at[rows], dst_ref=gbuf.at[rows], send_sem=g_send.at[k], recv_sem=g_recv.at[k],
                                            device_id={"stage": jnp.maximum(stage - 1, 0)}, device_id_type=MESH)

    def prepare(k):
        rows = chunk_rows(k)
        pre = jnp.dot(acts[rows, :], up_bf[...], preferred_element_type=F32)
        sq = pre * pre
        half_t = 0.5 * jnp.tanh(pre * (SQRT_TWO_PI + (SQRT_TWO_PI * GELU_CUBIC) * sq))
        prob = 0.5 + half_t
        rest = 0.5 - half_t
        hid[rows, :] = (pre * prob).astype(BF16)
        slope[rows, :] = prob + (prob * rest) * pre * (2.0 * SQRT_TWO_PI + (6.0 * SQRT_TWO_PI * GELU_CUBIC) * sq)

    def backward(k):
        rows = chunk_rows(k)

        @pl.when(stage < 3)
        def _():
            pass_down(k).wait_recv()
        grad = gbuf[rows, :]
        d_pre = (mat_nt(grad, down_bf[...]) * slope[rows, :]).astype(BF16)
        dpre[rows, :] = d_pre

        @pl.when(stage > 0)
        def _():
            dxbuf[rows, :] = (grad.astype(F32) + mat_nt(d_pre, up_bf[...])).astype(BF16)
            pass_down(k).start()

    def rs_copy(src, dst, sem, peer):
        return pltpu.make_async_remote_copy(src_ref=src, dst_ref=dst, send_sem=rs_send.at[sem], recv_sem=rs_recv.at[sem], device_id={"data": peer}, device_id_type=MESH)

    def v_first(sub, c):
        yy = (1 - y) if sub == 0 else y
        return rs_copy(gv.at[down_rows(1 - z, yy, 128 * c, 128)], rv1.at[sub, pl.ds(128 * c, 128)], 2 * sub + c, z_peer)

    def u_first(sub, c):
        zz = (1 - z) if sub == 0 else z
        return rs_copy(gu.at[up_rows(zz, 1 - y, 32 * c, 32)], ru1.at[sub, pl.ds(32 * c, 32)], 4 + 2 * sub + c, y_peer)

    def v_second(c):
        return rs_copy(gv.at[down_rows(z, 1 - y, 128 * c, 128)], rv2.at[pl.ds(128 * c, 128)], 8 + c, y_peer)

    def u_second(c):
        return rs_copy(gu.at[up_rows(1 - z, y, 32 * c, 32)], ru2.at[pl.ds(32 * c, 32)], 10 + c, z_peer)

    def add_grads(k):
        rows = chunk_rows(k)

        @pl.when(k == 0)
        def _():
            loads[3].wait()
            loads[4].wait()

        def half(h):
            zz = h * z + (1 - h) * (1 - z)
            yy = h * y + (1 - h) * (1 - y)
            send = (k == N_CHUNK - 1) & (h == 0)
            out = pl.ds(pl.multiple_of(512 * zz, 512), 512)
            gv[out, :] += mat_tn(hid[rows, out], gbuf[rows, :])

            @pl.when(send)
            def _():
                for sub in range(2):
                    for c in range(2):
                        v_first(sub, c).start()
            out = pl.ds(pl.multiple_of(128 * yy, 128), 128)
            gu[out, :] += mat_tn(acts[rows, out], dpre[rows, :])

            @pl.when(send)
            def _():
                for sub in range(2):
                    for c in range(2):
                        u_first(sub, c).start()
        repeat(0, 2, half)

    def tick(t):
        upper = jnp.where(stage >= 2, 1, 0)
        even = 1 - lax.rem(t, 2)
        early = jnp.where(t < N_CHUNK, 1, 0)
        late = jnp.where(t >= 2 * N_CHUNK, 1, 0)
        is_prep = upper * even * (1 - late) + (1 - upper) * early
        is_grad = upper * late + (1 - upper) * (1 - early) * (1 - even)
        k = upper * (late * (t - 2 * N_CHUNK) + (1 - late) * lax.div(t, 2)) + (1 - upper) * (early * t + (1 - early) * lax.div(t - N_CHUNK, 2))

        @pl.when(is_prep == 1)
        def _():
            prepare(k)

        @pl.when(is_prep + is_grad == 0)
        def _():
            backward(k)

        @pl.when(is_grad == 1)
        def _():
            add_grads(k)

    loads[0].wait()
    loads[1].wait()
    up_bf[...] = up32[...].astype(BF16)
    prepare(0)
    loads[2].wait()
    for copy in loads[3:]:
        copy.start()
    start_loads(stage, nb_hbm, nbuf, nb_sem)
    down_bf[...] = down32[...].astype(BF16)
    pl.semaphore_wait(barrier, 15)

    @pl.when(stage == 3)
    def _():
        load_loss.wait()
    repeat(1, 3 * N_CHUNK, tick)

    for c in range(2):
        v_first(0, c).wait_recv()
        rows = down_rows(z, 1 - y, 128 * c, 128)
        gv[rows, :] += rv1[0, 128 * c:128 * (c + 1), :]
        v_second(c).start()
        u_first(0, c).wait_recv()
        rows = up_rows(1 - z, y, 32 * c, 32)
        gu[rows, :] += ru1[0, 32 * c:32 * (c + 1), :]
        u_second(c).start()
    acc = jnp.zeros((8, 128), F32)

    def fold(tile, acc):
        sq = tile * tile
        sq = jnp.sum(sq.reshape(sq.shape[0] // 8, 8, sq.shape[1]), axis=0)
        for i in range(0, sq.shape[1], 128):
            acc = acc + sq[:, i:i + 128]
        return acc

    for c in range(2):
        v_first(1, c).wait_recv()
        v_second(c).wait_recv()
        rows = down_rows(z, y, 128 * c, 128)
        mean = (gv[rows, :] + rv1[1, 128 * c:128 * (c + 1), :] + rv2[128 * c:128 * (c + 1), :]) * 0.25
        mean_down[rows, :] = mean
        acc = fold(mean, acc)
        u_first(1, c).wait_recv()
        u_second(c).wait_recv()
        rows = up_rows(z, y, 32 * c, 32)
        mean = (gu[rows, :] + ru1[1, 32 * c:32 * (c + 1), :] + ru2[32 * c:32 * (c + 1), :]) * 0.25
        mean_up[rows, :] = mean
        acc = fold(mean, acc)

    up_piece, down_piece = 64 // N_PIECE, 256 // N_PIECE

    def gather(which, up, down):
        def copy(ref, rows, sem, piece, peer):
            sem = (which * 6 + sem) * N_PIECE + piece
            return pltpu.make_async_remote_copy(src_ref=ref.at[rows], dst_ref=ref.at[rows], send_sem=ag_send.at[sem], recv_sem=ag_recv.at[sem],
                                                device_id={"data": peer}, device_id_type=MESH)

        def up_copy(zz, yy, sem, p, peer):
            return copy(up, up_rows(zz, yy, up_piece * p, up_piece), sem, p, peer)

        def down_copy(zz, yy, sem, p, peer):
            return copy(down, down_rows(zz, yy, down_piece * p, down_piece), sem, p, peer)

        def up_sends(p):
            return [up_copy(z, y, 0, p, z_peer), up_copy(z, y, 1, p, y_peer)]

        def down_sends(p):
            return [down_copy(z, y, 3, p, y_peer), down_copy(z, y, 4, p, z_peer)]

        def relays(p):
            return [(up_copy(1 - z, y, 0, p, z_peer), up_copy(1 - z, y, 2, p, y_peer)), (down_copy(z, 1 - y, 3, p, y_peer), down_copy(z, 1 - y, 5, p, z_peer))]

        def begin(matrix, hops=(0, 1)):
            for p in range(N_PIECE):
                for hop in hops:
                    (up_sends, down_sends)[matrix](p)[hop].start()

        def relay():
            for p in range(N_PIECE):
                for arrived, onward in relays(p):
                    arrived.wait_recv()
                    onward.start()

        def finish():
            for p in range(N_PIECE):
                for c in (up_copy(z, 1 - y, 1, p, y_peer), down_copy(1 - z, y, 4, p, z_peer), up_copy(1 - z, 1 - y, 2, p, y_peer), down_copy(1 - z, 1 - y, 5, p, z_peer)):
                    c.wait_recv()

        def drain():
            for p in range(N_PIECE):
                for c in up_sends(p) + down_sends(p) + [onward for _, onward in relays(p)]:
                    c.wait_send()
        return begin, relay, finish, drain

    own_begin, own_relay, own_finish, own_drain = gather(0, up_own, down_own)
    aux_begin, aux_relay, aux_finish, aux_drain = gather(1, up_aux, down_aux)
    mean_begin, mean_relay, mean_finish, mean_drain = gather(2, mean_up, mean_down)

    def sq_copy(other, slot):
        return pltpu.make_async_remote_copy(src_ref=sq_all.at[slot], dst_ref=sq_all.at[slot], send_sem=sq_send.at[other], recv_sem=sq_recv.at[slot],
                                            device_id={"data": lax.div(other, 4), "stage": lax.rem(other, 4)}, device_id_type=MESH)

    sq_all[me] = acc

    def tell(d):
        sq_copy(lax.rem(me + d, 16), me).start()
    repeat(1, 16, tell)
    for copy in loads[5:]:
        copy.wait()

    @pl.when(stage >= 2)
    def _():
        mean_begin(0)
        mean_begin(1)
        mean_relay()
        mean_finish()

    def hear(d):
        other = lax.rem(me + d, 16)
        sq_copy(other, other).wait_recv()
    repeat(1, 16, hear)
    total = sq_all[0]
    for i in range(1, 16):
        total = total + sq_all[i]
    total = jnp.sum(jnp.sum(total, axis=0, keepdims=True), axis=1, keepdims=True)
    clip = jnp.minimum(1.0, norm_ref[0] / (jnp.sqrt(total) + NORM_EPS))

    rate = rate_ref[0]

    def renew(rows, master, moments, mean, weights, scale, first, full):
        new = adamw_update(master[rows, :], moments[0, rows, :], moments[1, rows, :], mean[rows, :], clip, rate)
        if first:
            weights[rows, :] = new[0].astype(BF16) * jnp.asarray(scale, BF16)

        if full:
            master[rows, :] = new[0]
            moments[0, rows, :] = new[1]
            moments[1, rows, :] = new[2]

    def renew_up(block, first, full):
        renew(pl.ds(pl.multiple_of(64 * block, 64), 64), up32, m_up, mean_up, up_own, 0.5, first, full)

    def renew_down(block, first, full):
        renew(pl.ds(pl.multiple_of(256 * block, 256), 256), down32, m_down, mean_down, down_own, 1.0, first, full)

    def renew_all(first):
        def body(t):
            renew_up(t, first, True)
            renew_down(t, first, True)
        repeat(0, 4, body)

    new_stores = [pltpu.make_async_copy(src, dst, in_sem.at[i]) for i, (src, dst) in enumerate((
        (up32, new_up_hbm), (down32, new_down_hbm), (m_up.at[0], new_m1_up_hbm), (m_down.at[0], new_m1_down_hbm), (m_up.at[1], new_m2_up_hbm), (m_down.at[1], new_m2_down_hbm)))]
    def feed(p):
        parts = [(up_own, up_aux, up_rows(z, y, up_piece * p, up_piece)), (down_own, down_aux, down_rows(z, y, down_piece * p, down_piece))]
        return [pltpu.make_async_remote_copy(src_ref=own.at[rows], dst_ref=aux.at[rows], send_sem=aux_send.at[2 * p + i], recv_sem=aux_recv.at[2 * p + i], device_id={"stage": 3 - stage}, device_id_type=MESH)
                for i, (own, aux, rows) in enumerate(parts)]

    @pl.when(stage < 2)
    def _():
        renew_up(2 * y + z, True, False)
        for p in range(N_PIECE):
            feed(p)[0].start()
        own_begin(0, (0,))
        renew_down(2 * z + y, True, False)
        for p in range(N_PIECE):
            feed(p)[1].start()
        own_begin(1, (0,))
        own_begin(0, (1,))
        own_begin(1, (1,))
        own_relay()
        mean_begin(0)
        mean_begin(1)

    @pl.when(stage >= 2)
    def _():
        for matrix in range(2):
            for p in range(N_PIECE):
                feed(p)[matrix].wait_recv()
            aux_begin(matrix)
        renew_all(True)
        for copy in new_stores:
            copy.start()
        aux_relay()

    def relay_mean(now):
        @pl.when(now)
        def _():
            mean_relay()

    forward_part(stage, own_finish, aux_finish, relay_mean, nb_hbm, up_own, down_own, up_aux, down_aux, up_two, down_two, out_hbm, late_hbm, nbuf, xin, yout, nb_sem, out_sem, send_sem, recv_sem, two_send, two_recv)

    @pl.when(stage < 2)
    def _():
        mean_finish()
        renew_all(False)
        for copy in new_stores:
            copy.start()
    store_w_up = pltpu.make_async_copy(up_own, w_up_hbm, in_sem.at[6])
    store_w_down = pltpu.make_async_copy(down_own, w_down_hbm, in_sem.at[7])
    store_w_up.start()
    store_w_down.start()

    @pl.when(stage == 1)
    def _():
        def left(i):
            pltpu.make_async_remote_copy(src_ref=yout.at[i], dst_ref=xin.at[i], send_sem=send_sem.at[i], recv_sem=recv_sem.at[i], device_id={"stage": 2}, device_id_type=MESH).wait_send()
        repeat(nbuf.shape[0] - N_SENT, nbuf.shape[0], left)

    @pl.when(stage > 0)
    def _():
        for k in range(N_CHUNK):
            pass_down(k).wait_send()
    for c in range(2):
        for sub in range(2):
            v_first(sub, c).wait_send()
            u_first(sub, c).wait_send()
        v_second(c).wait_send()
        u_second(c).wait_send()

    def told(d):
        sq_copy(lax.rem(me + d, 16), me).wait_send()
    repeat(1, 16, told)
    mean_drain()

    @pl.when(stage < 2)
    def _():
        own_drain()
        for p in range(N_PIECE):
            for c in feed(p):
                c.wait_send()

    @pl.when(stage >= 2)
    def _():
        aux_drain()
    for copy in new_stores:
        copy.wait()
    store_w_up.wait()
    store_w_down.wait()


def fused_step(master_up, master_down, m1_up, m1_down, m2_up, m2_down, grad_up, grad_down, acts, loss_grad, next_batch, learn_rate, max_norm):
    n_micro = next_batch.shape[0]
    n_tok, width = acts.shape
    hidden = master_up.shape[1]
    hbm = pl.BlockSpec(memory_space=pl.ANY)
    smem = pl.BlockSpec(memory_space=pltpu.SMEM)
    vmem = pltpu.VMEM
    dma = pltpu.SemaphoreType.DMA
    return pl.pallas_call(
        step_kernel,
        name="pipeline_step",
        out_shape=[jax.ShapeDtypeStruct(next_batch.shape, BF16)] + [jax.ShapeDtypeStruct((width, hidden), F32), jax.ShapeDtypeStruct((hidden, width), F32)] * 3 + [
            jax.ShapeDtypeStruct((N_LATE,) + next_batch.shape[1:], BF16), jax.ShapeDtypeStruct((width, hidden), BF16), jax.ShapeDtypeStruct((hidden, width), BF16)],
        in_specs=[hbm] * 11 + [smem] * 2,
        out_specs=[hbm] * 10,
        scratch_shapes=[
            vmem((width, hidden), F32), vmem((hidden, width), F32),
            vmem((width, hidden), F32), vmem((hidden, width), F32),
            vmem((width, hidden), F32), vmem((hidden, width), F32),
            vmem((n_tok, width), BF16), vmem((n_tok, width), BF16), vmem((n_tok, width), BF16),
            vmem((n_tok, hidden), BF16), vmem((n_tok, hidden), F32), vmem((n_tok, hidden), BF16),
            vmem((width, hidden), BF16), vmem((hidden, width), BF16),
            vmem((2, width // 4, hidden), F32), vmem((2, hidden // 4, width), F32),
            vmem((width // 4, hidden), F32), vmem((hidden // 4, width), F32),
            vmem((2, width, hidden), F32), vmem((2, hidden, width), F32),
            vmem((width, hidden), BF16), vmem((hidden, width), BF16),
            vmem((width, hidden), BF16), vmem((hidden, width), BF16),
            vmem((width, hidden), BF16), vmem((hidden, width), BF16),
            vmem((16, 8, 128), F32),
            vmem(next_batch.shape, BF16), vmem(next_batch.shape, BF16), vmem(next_batch.shape, BF16),
            *(dma((n,)) for n in (10, N_CHUNK, N_CHUNK, 12, 12, 16, 16, 18 * N_PIECE, 18 * N_PIECE, 2 * N_PIECE, 2 * N_PIECE, n_micro, n_micro, n_micro, n_micro, 2, 2)),
        ],
        compiler_params=pltpu.CompilerParams(collective_id=1, has_side_effects=True, vmem_limit_bytes=63 * 1024 * 1024),
    )(master_up, master_down, m1_up, m1_down, m2_up, m2_down, grad_up, grad_down, acts, loss_grad, next_batch, learn_rate, max_norm)


def finish_kernel(outs_in, late_in, w_up_in, w_down_in, *refs):
    news_in, outs, news_out = refs[:6], refs[6], refs[7:13]
    obuf, late, w_up, w_down, upd_up, upd_down, load_sem, store_sem, micro_load, micro_store, late_load = refs[13:]
    stage = lax.axis_index("stage")
    n_micro = obuf.shape[0]
    last = stage == 3
    n_copied = jnp.where(last, n_micro - N_LATE, n_micro)
    per_late = -(-(n_micro - N_LATE) // (N_LATE - 2))
    slots = [buf.at[i] for i in range(3) for buf in (upd_up, upd_down)]
    loads = [pltpu.make_async_copy(src, slot, load_sem.at[i]) for i, (src, slot) in enumerate(zip(news_in, slots))]
    stores = [pltpu.make_async_copy(slot, dst, store_sem.at[i]) for i, (slot, dst) in enumerate(zip(slots, news_out))]
    w_loads = [pltpu.make_async_copy(w_up_in, w_up, load_sem.at[6]), pltpu.make_async_copy(w_down_in, w_down, load_sem.at[7])]

    def place(k):
        return mixed(k, n_micro)[1]

    def load_micro(k):
        i = place(k)
        return pltpu.make_async_copy(outs_in.at[i], obuf.at[i], micro_load.at[i])

    def store_micro(k):
        i = place(k)
        return pltpu.make_async_copy(obuf.at[i], outs.at[i], micro_store.at[i])

    def load_late(n):
        return pltpu.make_async_copy(late_in.at[n], late.at[n], late_load.at[n])

    def start_micro(k):
        load_micro(k).start()

    def turn_micro(k):
        load_micro(k).wait()
        store_micro(k).start()

    def start_late(n):
        load_late(n).start()

    @pl.when(last)
    def _():
        for copy in w_loads:
            copy.start()
        repeat(0, N_LATE, start_late)
    for copy in loads:
        copy.start()
    repeat(0, n_copied, start_micro)

    @pl.when(last)
    def _():
        for copy in w_loads:
            copy.wait()

        def body(n):
            load_late(n).wait()
            k = n_micro - N_LATE + n
            stage_rows(late.at[n], w_up, w_down, obuf.at[place(k)])
            store_micro(k).start()

            @pl.when(n == 1)
            def _():
                for load, store in zip(loads, stores):
                    load.wait()
                    store.start()
            for j in range(per_late):
                k = per_late * (n - 2) + j

                @pl.when((k >= 0) & (k < n_micro - N_LATE))
                def _():
                    turn_micro(k)
        repeat(0, N_LATE, body)

    @pl.when(jnp.logical_not(last))
    def _():
        for load, store in zip(loads, stores):
            load.wait()
            store.start()
        repeat(0, n_micro, turn_micro)

    def stored(k):
        store_micro(k).wait()
    repeat(0, n_micro, stored)
    for copy in stores:
        copy.wait()


def finish_step(outs, late, w_up, w_down, *news):
    n_micro = outs.shape[0]
    hbm = pl.BlockSpec(memory_space=pl.ANY)
    vmem = pltpu.VMEM
    dma = pltpu.SemaphoreType.DMA
    return pl.pallas_call(
        finish_kernel,
        name="finish_step",
        out_shape=[jax.ShapeDtypeStruct(outs.shape, BF16)] + [jax.ShapeDtypeStruct(new.shape, F32) for new in news],
        in_specs=[hbm] * 10,
        out_specs=[hbm] * 7,
        scratch_shapes=[
            vmem(outs.shape, BF16), vmem(late.shape, BF16), vmem(w_up.shape, BF16), vmem(w_down.shape, BF16),
            vmem((3,) + news[0].shape, F32), vmem((3,) + news[1].shape, F32),
            dma((8,)), dma((6,)), dma((n_micro,)), dma((n_micro,)), dma((N_LATE,)),
        ],
        compiler_params=pltpu.CompilerParams(vmem_limit_bytes=56 * 1024 * 1024),
    )(outs, late, w_up, w_down, *news)


def solution(mesh):
    def local_step(master_up, master_down, mom1_up, mom1_down, mom2_up, mom2_down, grad_up, grad_down, stage_acts, loss_grad, next_batch, learn_rate, max_norm):
        stage_outs, *news, late, w_up, w_down = fused_step(
            master_up[0], master_down[0], mom1_up[0], mom1_down[0], mom2_up[0], mom2_down[0], grad_up[0, 0], grad_down[0, 0],
            stage_acts[0], loss_grad, next_batch, learn_rate.reshape(1), max_norm.reshape(1))
        stage_outs, new_up, new_down, new_m1_up, new_m1_down, new_m2_up, new_m2_down = finish_step(stage_outs, late, w_up, w_down, *news)
        return (new_up[None], new_down[None], new_m1_up[None], new_m1_down[None], new_m2_up[None], new_m2_down[None], stage_outs[None])

    w_spec = P('stage', None, None)
    g_spec = P('data', 'stage', None, None)
    in_specs = (w_spec, w_spec, w_spec, w_spec, w_spec, w_spec, g_spec, g_spec, P('stage', 'data', None), P('data', None), P(None, 'data', None), P(), P())
    out_specs = (w_spec, w_spec, w_spec, w_spec, w_spec, w_spec, P('stage', None, 'data', None))
    return jax.shard_map(local_step, mesh=mesh, in_specs=in_specs, out_specs=out_specs, check_vma=False)
```

```python
import jax
import jax.numpy as jnp
from jax import lax
from jax.experimental import pallas as pl
from jax.experimental.pallas import tpu as pltpu
from jax.sharding import PartitionSpec as P

BETA1 = 0.9
BETA2 = 0.95
ADAM_EPS = 1e-8
WEIGHT_DECAY = 0.1
NORM_EPS = 1e-6
ADAM_STEP = 8
SQRT_TWO_PI = 0.7978845608028654
GELU_CUBIC = 0.044715

N_SENT = 5
N_CHUNK = 4
N_LATE = 6
N_TWICE = 5
N_PIECE = 2
MESH = pl.DeviceIdType.MESH
BF16 = jnp.bfloat16
F32 = jnp.float32


def repeat(first, end, body):
    def step(i, _):
        body(i)
        return 0
    lax.fori_loop(first, end, step, 0)


def mat_tn(left, right):
    return lax.dot_general(left, right, (((0,), (0,)), ((), ())), preferred_element_type=F32)


def mat_nt(left, right):
    return lax.dot_general(left, right, (((1,), (1,)), ((), ())), preferred_element_type=F32)


def adamw_update(master, first_mom, second_mom, grad_avg, clip_scale, learn_rate):
    scaled = clip_scale * grad_avg
    new_first = BETA1 * first_mom + (1.0 - BETA1) * scaled
    new_second = BETA2 * second_mom + (1.0 - BETA2) * scaled * scaled
    first_hat = new_first * (1.0 / (1.0 - BETA1 ** ADAM_STEP))
    second_hat = new_second * (1.0 / (1.0 - BETA2 ** ADAM_STEP))
    new_master = master - learn_rate * (first_hat / (jnp.sqrt(second_hat) + ADAM_EPS) + WEIGHT_DECAY * master)
    return new_master, new_first, new_second


def gelu_of_half(half):
    t = jnp.tanh(half * (2.0 * SQRT_TWO_PI + (8.0 * SQRT_TWO_PI * GELU_CUBIC) * (half * half)))
    return half + half * t


def stage_rows(src, up_half, down, dst):
    x = src[...]
    half = jnp.dot(x, up_half[...], preferred_element_type=F32)
    hidden = gelu_of_half(half).astype(BF16)
    y = jnp.dot(hidden, down[...], preferred_element_type=F32)
    dst[...] = (x.astype(F32) + y).astype(BF16)


def mixed(k, n_micro):
    before = lax.div(k * N_SENT, n_micro)
    is_sent = lax.div((k + 1) * N_SENT, n_micro) - before
    return is_sent, is_sent * (n_micro - N_SENT + before) + (1 - is_sent) * (k - before)


def forward_part(stage, own_ready, aux_ready, relay_mean, nb_hbm, up_own, down_own, up_aux, down_aux, up_two, down_two, out_hbm, late_hbm, nbuf, xin, yout, nb_sem, out_sem, send_sem, recv_sem, two_send, two_recv):
    n_micro = nbuf.shape[0]
    n_kept = n_micro - N_SENT

    def load(i):
        return pltpu.make_async_copy(nb_hbm.at[i], nbuf.at[i], nb_sem.at[i])

    def store(i):
        return pltpu.make_async_copy(yout.at[i], out_hbm.at[i], out_sem.at[i])

    def push(src, i, peer):
        return pltpu.make_async_remote_copy(src_ref=src.at[i], dst_ref=xin.at[i], send_sem=send_sem.at[i], recv_sem=recv_sem.at[i], device_id={"stage": peer}, device_id_type=MESH)

    def arrived(i):
        push(yout, i, stage).wait_recv()

    def rotated(j):
        return lax.rem(j + n_kept, n_micro)

    def finish_stores():
        def body(i):
            store(i).wait()
        repeat(0, n_micro, body)

    def hand_over():
        return [pltpu.make_async_remote_copy(src_ref=aux, dst_ref=two, send_sem=two_send.at[i], recv_sem=two_recv.at[i], device_id={"stage": 3}, device_id_type=MESH)
                for i, (aux, two) in enumerate([(up_aux, up_two), (down_aux, down_two)])]

    def finish_sends(first, count):
        def body(i):
            push(yout, first + i, stage).wait_send()
        repeat(0, count, body)

    @pl.when(stage == 0)
    def _():
        own_ready()

        def body(j):
            i = rotated(j)
            load(i).wait()
            stage_rows(nbuf.at[i], up_own, down_own, yout.at[i])
            push(yout, i, 1).start()
            store(i).start()
            relay_mean(j == 7)
        repeat(0, n_micro, body)
        finish_sends(0, n_micro)
        finish_stores()

    @pl.when(stage == 1)
    def _():
        own_ready()

        def body(j):
            i = rotated(j)
            arrived(i)
            stage_rows(xin.at[i], up_own, down_own, yout.at[i])

            @pl.when(j < N_SENT)
            def _():
                push(yout, i, 2).start()
            store(i).start()
            relay_mean(j == 7)
        repeat(0, n_micro, body)
        finish_stores()

    @pl.when(stage == 2)
    def _():
        aux_ready()
        for copy in hand_over():
            copy.start()

        def body(k):
            _, i = mixed(k, n_micro)
            arrived(i)

            @pl.when(i < n_kept - N_TWICE)
            def _():
                stage_rows(xin.at[i], up_aux, down_aux, xin.at[i])
            stage_rows(xin.at[i], up_own, down_own, yout.at[i])
            push(yout, i, 3).start()
            store(i).start()
        repeat(0, n_micro, body)
        finish_sends(0, n_micro)
        finish_stores()
        for copy in hand_over():
            copy.wait_send()

    @pl.when(stage == 3)
    def _():
        aux_ready()

        def first(j):
            load(j).wait()
            stage_rows(nbuf.at[j], up_aux, down_aux, nbuf.at[j])

            @pl.when(j == n_kept - N_TWICE)
            def _():
                for copy in hand_over():
                    copy.wait_recv()

            @pl.when(j >= n_kept - N_TWICE)
            def _():
                stage_rows(nbuf.at[j], up_two, down_two, nbuf.at[j])
            push(nbuf, j, 2).start()
        repeat(0, n_kept, first)

        def body(k):
            _, i = mixed(k, n_micro)
            arrived(i)
            stage_rows(xin.at[i], up_own, down_own, yout.at[i])
            store(i).start()
        repeat(0, n_micro - N_LATE, body)

        def late(k):
            _, i = mixed(k, n_micro)
            return i, pltpu.make_async_copy(xin.at[i], late_hbm.at[k - (n_micro - N_LATE)], out_sem.at[i])

        def save(k):
            i, copy = late(k)
            arrived(i)
            copy.start()
        repeat(n_micro - N_LATE, n_micro, save)

        def stored(k):
            _, i = mixed(k, n_micro)
            store(i).wait()
        repeat(0, n_micro - N_LATE, stored)

        def saved(k):
            late(k)[1].wait()
        repeat(n_micro - N_LATE, n_micro, saved)
        finish_sends(0, n_kept)


def start_loads(stage, nb_hbm, nbuf, nb_sem):
    n_micro = nbuf.shape[0]
    n_kept = n_micro - N_SENT

    def body(j):
        i = lax.rem(j + n_kept, n_micro)
        pltpu.make_async_copy(nb_hbm.at[i], nbuf.at[i], nb_sem.at[i]).start()

    @pl.when(stage == 0)
    def _():
        repeat(0, n_micro, body)

    @pl.when(stage == 3)
    def _():
        repeat(N_SENT, n_micro, body)


def step_kernel(up_hbm, down_hbm, m1_up_hbm, m1_down_hbm, m2_up_hbm, m2_down_hbm, gu_hbm, gv_hbm, acts_hbm, loss_hbm, nb_hbm, rate_ref, norm_ref,
                out_hbm, new_up_hbm, new_down_hbm, new_m1_up_hbm, new_m1_down_hbm, new_m2_up_hbm, new_m2_down_hbm, late_hbm, w_up_hbm, w_down_hbm,
                up32, down32, gu, gv, mean_up, mean_down, acts, gbuf, dxbuf, hid, slope, dpre, up_bf, down_bf,
                ru1, rv1, ru2, rv2, m_up, m_down, up_own, down_own, up_aux, down_aux, up_two, down_two, sq_all, nbuf, xin, yout,
                in_sem, g_send, g_recv, rs_send, rs_recv, sq_send, sq_recv, ag_send, ag_recv, aux_send, aux_recv,
                nb_sem, out_sem, send_sem, recv_sem, two_send, two_recv):
    stage = lax.axis_index("stage")
    data = lax.axis_index("data")
    z = lax.div(data, 2)
    y = lax.rem(data, 2)
    me = data * 4 + stage
    z_peer = 2 * (1 - z) + y
    y_peer = 2 * z + (1 - y)
    n_tok = acts.shape[0]
    chunk = n_tok // N_CHUNK

    def up_rows(zz, yy, first=0, count=64):
        return pl.ds(pl.multiple_of(128 * yy + 64 * zz + first, 32), count)

    def down_rows(zz, yy, first=0, count=256):
        return pl.ds(pl.multiple_of(512 * zz + 256 * yy + first, 128), count)

    own_up, own_down = up_rows(z, y), down_rows(z, y)
    loads = [pltpu.make_async_copy(src, dst, in_sem.at[i]) for i, (src, dst) in enumerate((
        (acts_hbm, acts), (up_hbm, up32), (down_hbm, down32), (gv_hbm, gv), (gu_hbm, gu),
        (m1_up_hbm, m_up.at[0]), (m2_up_hbm, m_up.at[1]), (m1_down_hbm, m_down.at[0]), (m2_down_hbm, m_down.at[1])))]
    load_loss = pltpu.make_async_copy(loss_hbm, gbuf, in_sem.at[9])
    for copy in loads[:2]:
        copy.start()

    @pl.when(stage == 3)
    def _():
        load_loss.start()
    loads[2].start()

    barrier = pltpu.get_barrier_semaphore()

    def greet(d):
        other = lax.rem(me + d, 16)
        pl.semaphore_signal(barrier, inc=1, device_id={"data": lax.div(other, 4), "stage": lax.rem(other, 4)}, device_id_type=MESH)
    repeat(1, 16, greet)

    def chunk_rows(k):
        return pl.ds(pl.multiple_of(k * chunk, chunk), chunk)

    def pass_down(k):
        rows = chunk_rows(k)
        return pltpu.make_async_remote_copy(src_ref=dxbuf.at[rows], dst_ref=gbuf.at[rows], send_sem=g_send.at[k], recv_sem=g_recv.at[k],
                                            device_id={"stage": jnp.maximum(stage - 1, 0)}, device_id_type=MESH)

    def prepare(k):
        rows = chunk_rows(k)
        pre = jnp.dot(acts[rows, :], up_bf[...], preferred_element_type=F32)
        sq = pre * pre
        half_t = 0.5 * jnp.tanh(pre * (SQRT_TWO_PI + (SQRT_TWO_PI * GELU_CUBIC) * sq))
        prob = 0.5 + half_t
        rest = 0.5 - half_t
        hid[rows, :] = (pre * prob).astype(BF16)
        slope[rows, :] = prob + (prob * rest) * pre * (2.0 * SQRT_TWO_PI + (6.0 * SQRT_TWO_PI * GELU_CUBIC) * sq)

    def backward(k):
        rows = chunk_rows(k)

        @pl.when(stage < 3)
        def _():
            pass_down(k).wait_recv()
        grad = gbuf[rows, :]
        d_pre = (mat_nt(grad, down_bf[...]) * slope[rows, :]).astype(BF16)
        dpre[rows, :] = d_pre

        @pl.when(stage > 0)
        def _():
            dxbuf[rows, :] = (grad.astype(F32) + mat_nt(d_pre, up_bf[...])).astype(BF16)
            pass_down(k).start()

    def rs_copy(src, dst, sem, peer):
        return pltpu.make_async_remote_copy(src_ref=src, dst_ref=dst, send_sem=rs_send.at[sem], recv_sem=rs_recv.at[sem], device_id={"data": peer}, device_id_type=MESH)

    def v_first(sub, c):
        yy = (1 - y) if sub == 0 else y
        return rs_copy(gv.at[down_rows(1 - z, yy, 128 * c, 128)], rv1.at[sub, pl.ds(128 * c, 128)], 2 * sub + c, z_peer)

    def u_first(sub, c):
        zz = (1 - z) if sub == 0 else z
        return rs_copy(gu.at[up_rows(zz, 1 - y, 32 * c, 32)], ru1.at[sub, pl.ds(32 * c, 32)], 4 + 2 * sub + c, y_peer)

    def v_second(c):
        return rs_copy(gv.at[down_rows(z, 1 - y, 128 * c, 128)], rv2.at[pl.ds(128 * c, 128)], 8 + c, y_peer)

    def u_second(c):
        return rs_copy(gu.at[up_rows(1 - z, y, 32 * c, 32)], ru2.at[pl.ds(32 * c, 32)], 10 + c, z_peer)

    def add_grads(k):
        rows = chunk_rows(k)

        @pl.when(k == 0)
        def _():
            loads[3].wait()
            loads[4].wait()

        def half(h):
            zz = h * z + (1 - h) * (1 - z)
            yy = h * y + (1 - h) * (1 - y)
            send = (k == N_CHUNK - 1) & (h == 0)
            out = pl.ds(pl.multiple_of(512 * zz, 512), 512)
            gv[out, :] += mat_tn(hid[rows, out], gbuf[rows, :])

            @pl.when(send)
            def _():
                for sub in range(2):
                    for c in range(2):
                        v_first(sub, c).start()
            out = pl.ds(pl.multiple_of(128 * yy, 128), 128)
            gu[out, :] += mat_tn(acts[rows, out], dpre[rows, :])

            @pl.when(send)
            def _():
                for sub in range(2):
                    for c in range(2):
                        u_first(sub, c).start()
        repeat(0, 2, half)

    def tick(t):
        upper = jnp.where(stage >= 2, 1, 0)
        even = 1 - lax.rem(t, 2)
        early = jnp.where(t < N_CHUNK, 1, 0)
        late = jnp.where(t >= 2 * N_CHUNK, 1, 0)
        is_prep = upper * even * (1 - late) + (1 - upper) * early
        is_grad = upper * late + (1 - upper) * (1 - early) * (1 - even)
        k = upper * (late * (t - 2 * N_CHUNK) + (1 - late) * lax.div(t, 2)) + (1 - upper) * (early * t + (1 - early) * lax.div(t - N_CHUNK, 2))

        @pl.when(is_prep == 1)
        def _():
            prepare(k)

        @pl.when(is_prep + is_grad == 0)
        def _():
            backward(k)

        @pl.when(is_grad == 1)
        def _():
            add_grads(k)

    loads[0].wait()
    loads[1].wait()
    up_bf[...] = up32[...].astype(BF16)
    prepare(0)
    loads[2].wait()
    for copy in loads[3:]:
        copy.start()
    start_loads(stage, nb_hbm, nbuf, nb_sem)
    down_bf[...] = down32[...].astype(BF16)
    pl.semaphore_wait(barrier, 15)

    @pl.when(stage == 3)
    def _():
        load_loss.wait()
    repeat(1, 3 * N_CHUNK, tick)

    for c in range(2):
        v_first(0, c).wait_recv()
        rows = down_rows(z, 1 - y, 128 * c, 128)
        gv[rows, :] += rv1[0, 128 * c:128 * (c + 1), :]
        v_second(c).start()
        u_first(0, c).wait_recv()
        rows = up_rows(1 - z, y, 32 * c, 32)
        gu[rows, :] += ru1[0, 32 * c:32 * (c + 1), :]
        u_second(c).start()
    acc = jnp.zeros((8, 128), F32)

    def fold(tile, acc):
        sq = tile * tile
        sq = jnp.sum(sq.reshape(sq.shape[0] // 8, 8, sq.shape[1]), axis=0)
        for i in range(0, sq.shape[1], 128):
            acc = acc + sq[:, i:i + 128]
        return acc

    for c in range(2):
        v_first(1, c).wait_recv()
        v_second(c).wait_recv()
        rows = down_rows(z, y, 128 * c, 128)
        mean = (gv[rows, :] + rv1[1, 128 * c:128 * (c + 1), :] + rv2[128 * c:128 * (c + 1), :]) * 0.25
        mean_down[rows, :] = mean
        acc = fold(mean, acc)
        u_first(1, c).wait_recv()
        u_second(c).wait_recv()
        rows = up_rows(z, y, 32 * c, 32)
        mean = (gu[rows, :] + ru1[1, 32 * c:32 * (c + 1), :] + ru2[32 * c:32 * (c + 1), :]) * 0.25
        mean_up[rows, :] = mean
        acc = fold(mean, acc)

    up_piece, down_piece = 64 // N_PIECE, 256 // N_PIECE

    def gather(which, up, down):
        def copy(ref, rows, sem, piece, peer):
            sem = (which * 6 + sem) * N_PIECE + piece
            return pltpu.make_async_remote_copy(src_ref=ref.at[rows], dst_ref=ref.at[rows], send_sem=ag_send.at[sem], recv_sem=ag_recv.at[sem],
                                                device_id={"data": peer}, device_id_type=MESH)

        def up_copy(zz, yy, sem, p, peer):
            return copy(up, up_rows(zz, yy, up_piece * p, up_piece), sem, p, peer)

        def down_copy(zz, yy, sem, p, peer):
            return copy(down, down_rows(zz, yy, down_piece * p, down_piece), sem, p, peer)

        def up_sends(p):
            return [up_copy(z, y, 0, p, z_peer), up_copy(z, y, 1, p, y_peer)]

        def down_sends(p):
            return [down_copy(z, y, 3, p, y_peer), down_copy(z, y, 4, p, z_peer)]

        def relays(p):
            return [(up_copy(1 - z, y, 0, p, z_peer), up_copy(1 - z, y, 2, p, y_peer)), (down_copy(z, 1 - y, 3, p, y_peer), down_copy(z, 1 - y, 5, p, z_peer))]

        def begin(matrix, hops=(0, 1)):
            for p in range(N_PIECE):
                for hop in hops:
                    (up_sends, down_sends)[matrix](p)[hop].start()

        def relay():
            for p in range(N_PIECE):
                for arrived, onward in relays(p):
                    arrived.wait_recv()
                    onward.start()

        def finish():
            for p in range(N_PIECE):
                for c in (up_copy(z, 1 - y, 1, p, y_peer), down_copy(1 - z, y, 4, p, z_peer), up_copy(1 - z, 1 - y, 2, p, y_peer), down_copy(1 - z, 1 - y, 5, p, z_peer)):
                    c.wait_recv()

        def drain():
            for p in range(N_PIECE):
                for c in up_sends(p) + down_sends(p) + [onward for _, onward in relays(p)]:
                    c.wait_send()
        return begin, relay, finish, drain

    own_begin, own_relay, own_finish, own_drain = gather(0, up_own, down_own)
    aux_begin, aux_relay, aux_finish, aux_drain = gather(1, up_aux, down_aux)
    mean_begin, mean_relay, mean_finish, mean_drain = gather(2, mean_up, mean_down)

    def sq_copy(other, slot):
        return pltpu.make_async_remote_copy(src_ref=sq_all.at[slot], dst_ref=sq_all.at[slot], send_sem=sq_send.at[other], recv_sem=sq_recv.at[slot],
                                            device_id={"data": lax.div(other, 4), "stage": lax.rem(other, 4)}, device_id_type=MESH)

    sq_all[me] = acc

    def tell(d):
        sq_copy(lax.rem(me + d, 16), me).start()
    repeat(1, 16, tell)
    for copy in loads[5:]:
        copy.wait()

    @pl.when(stage >= 2)
    def _():
        mean_begin(0)
        mean_begin(1)
        mean_relay()
        mean_finish()

    def hear(d):
        other = lax.rem(me + d, 16)
        sq_copy(other, other).wait_recv()
    repeat(1, 16, hear)
    total = sq_all[0]
    for i in range(1, 16):
        total = total + sq_all[i]
    total = jnp.sum(jnp.sum(total, axis=0, keepdims=True), axis=1, keepdims=True)
    clip = jnp.minimum(1.0, norm_ref[0] / (jnp.sqrt(total) + NORM_EPS))

    rate = rate_ref[0]

    def renew(rows, master, moments, mean, weights, scale, first, full):
        new = adamw_update(master[rows, :], moments[0, rows, :], moments[1, rows, :], mean[rows, :], clip, rate)
        if first:
            weights[rows, :] = new[0].astype(BF16) * jnp.asarray(scale, BF16)

        if full:
            master[rows, :] = new[0]
            moments[0, rows, :] = new[1]
            moments[1, rows, :] = new[2]

    def renew_up(block, first, full):
        renew(pl.ds(pl.multiple_of(64 * block, 64), 64), up32, m_up, mean_up, up_own, 0.5, first, full)

    def renew_down(block, first, full):
        renew(pl.ds(pl.multiple_of(256 * block, 256), 256), down32, m_down, mean_down, down_own, 1.0, first, full)

    def renew_all(first):
        def body(t):
            renew_up(t, first, True)
            renew_down(t, first, True)
        repeat(0, 4, body)

    new_stores = [pltpu.make_async_copy(src, dst, in_sem.at[i]) for i, (src, dst) in enumerate((
        (up32, new_up_hbm), (down32, new_down_hbm), (m_up.at[0], new_m1_up_hbm), (m_down.at[0], new_m1_down_hbm), (m_up.at[1], new_m2_up_hbm), (m_down.at[1], new_m2_down_hbm)))]
    def feed(p):
        parts = [(up_own, up_aux, up_rows(z, y, up_piece * p, up_piece)), (down_own, down_aux, down_rows(z, y, down_piece * p, down_piece))]
        return [pltpu.make_async_remote_copy(src_ref=own.at[rows], dst_ref=aux.at[rows], send_sem=aux_send.at[2 * p + i], recv_sem=aux_recv.at[2 * p + i], device_id={"stage": 3 - stage}, device_id_type=MESH)
                for i, (own, aux, rows) in enumerate(parts)]

    @pl.when(stage < 2)
    def _():
        renew_up(2 * y + z, True, False)
        for p in range(N_PIECE):
            feed(p)[0].start()
        own_begin(0, (0,))
        renew_down(2 * z + y, True, False)
        for p in range(N_PIECE):
            feed(p)[1].start()
        own_begin(1, (0,))
        own_begin(0, (1,))
        own_begin(1, (1,))
        own_relay()
        mean_begin(0)
        mean_begin(1)

    @pl.when(stage >= 2)
    def _():
        for matrix in range(2):
            for p in range(N_PIECE):
                feed(p)[matrix].wait_recv()
            aux_begin(matrix)
        renew_all(True)
        for copy in new_stores:
            copy.start()
        aux_relay()

    def relay_mean(now):
        @pl.when(now)
        def _():
            mean_relay()

    forward_part(stage, own_finish, aux_finish, relay_mean, nb_hbm, up_own, down_own, up_aux, down_aux, up_two, down_two, out_hbm, late_hbm, nbuf, xin, yout, nb_sem, out_sem, send_sem, recv_sem, two_send, two_recv)

    @pl.when(stage < 2)
    def _():
        mean_finish()
        renew_all(False)
        for copy in new_stores:
            copy.start()
    store_w_up = pltpu.make_async_copy(up_own, w_up_hbm, in_sem.at[6])
    store_w_down = pltpu.make_async_copy(down_own, w_down_hbm, in_sem.at[7])
    store_w_up.start()
    store_w_down.start()

    @pl.when(stage == 1)
    def _():
        def left(i):
            pltpu.make_async_remote_copy(src_ref=yout.at[i], dst_ref=xin.at[i], send_sem=send_sem.at[i], recv_sem=recv_sem.at[i], device_id={"stage": 2}, device_id_type=MESH).wait_send()
        repeat(nbuf.shape[0] - N_SENT, nbuf.shape[0], left)

    @pl.when(stage > 0)
    def _():
        for k in range(N_CHUNK):
            pass_down(k).wait_send()
    for c in range(2):
        for sub in range(2):
            v_first(sub, c).wait_send()
            u_first(sub, c).wait_send()
        v_second(c).wait_send()
        u_second(c).wait_send()

    def told(d):
        sq_copy(lax.rem(me + d, 16), me).wait_send()
    repeat(1, 16, told)
    mean_drain()

    @pl.when(stage < 2)
    def _():
        own_drain()
        for p in range(N_PIECE):
            for c in feed(p):
                c.wait_send()

    @pl.when(stage >= 2)
    def _():
        aux_drain()
    for copy in new_stores:
        copy.wait()
    store_w_up.wait()
    store_w_down.wait()


def fused_step(master_up, master_down, m1_up, m1_down, m2_up, m2_down, grad_up, grad_down, acts, loss_grad, next_batch, learn_rate, max_norm):
    n_micro = next_batch.shape[0]
    n_tok, width = acts.shape
    hidden = master_up.shape[1]
    hbm = pl.BlockSpec(memory_space=pl.ANY)
    smem = pl.BlockSpec(memory_space=pltpu.SMEM)
    vmem = pltpu.VMEM
    dma = pltpu.SemaphoreType.DMA
    return pl.pallas_call(
        step_kernel,
        name="pipeline_step",
        out_shape=[jax.ShapeDtypeStruct(next_batch.shape, BF16)] + [jax.ShapeDtypeStruct((width, hidden), F32), jax.ShapeDtypeStruct((hidden, width), F32)] * 3 + [
            jax.ShapeDtypeStruct((N_LATE,) + next_batch.shape[1:], BF16), jax.ShapeDtypeStruct((width, hidden), BF16), jax.ShapeDtypeStruct((hidden, width), BF16)],
        in_specs=[hbm] * 11 + [smem] * 2,
        out_specs=[hbm] * 10,
        scratch_shapes=[
            vmem((width, hidden), F32), vmem((hidden, width), F32),
            vmem((width, hidden), F32), vmem((hidden, width), F32),
            vmem((width, hidden), F32), vmem((hidden, width), F32),
            vmem((n_tok, width), BF16), vmem((n_tok, width), BF16), vmem((n_tok, width), BF16),
            vmem((n_tok, hidden), BF16), vmem((n_tok, hidden), F32), vmem((n_tok, hidden), BF16),
            vmem((width, hidden), BF16), vmem((hidden, width), BF16),
            vmem((2, width // 4, hidden), F32), vmem((2, hidden // 4, width), F32),
            vmem((width // 4, hidden), F32), vmem((hidden // 4, width), F32),
            vmem((2, width, hidden), F32), vmem((2, hidden, width), F32),
            vmem((width, hidden), BF16), vmem((hidden, width), BF16),
            vmem((width, hidden), BF16), vmem((hidden, width), BF16),
            vmem((width, hidden), BF16), vmem((hidden, width), BF16),
            vmem((16, 8, 128), F32),
            vmem(next_batch.shape, BF16), vmem(next_batch.shape, BF16), vmem(next_batch.shape, BF16),
            *(dma((n,)) for n in (10, N_CHUNK, N_CHUNK, 12, 12, 16, 16, 18 * N_PIECE, 18 * N_PIECE, 2 * N_PIECE, 2 * N_PIECE, n_micro, n_micro, n_micro, n_micro, 2, 2)),
        ],
        compiler_params=pltpu.CompilerParams(collective_id=1, has_side_effects=True, vmem_limit_bytes=63 * 1024 * 1024),
    )(master_up, master_down, m1_up, m1_down, m2_up, m2_down, grad_up, grad_down, acts, loss_grad, next_batch, learn_rate, max_norm)


def finish_kernel(outs_in, late_in, w_up_in, w_down_in, *refs):
    news_in, outs, news_out = refs[:6], refs[6], refs[7:13]
    obuf, late, w_up, w_down, upd_up, upd_down, load_sem, store_sem, micro_load, micro_store, late_load = refs[13:]
    stage = lax.axis_index("stage")
    n_micro = obuf.shape[0]
    last = stage == 3
    n_copied = jnp.where(last, n_micro - N_LATE, n_micro)
    per_late = -(-(n_micro - N_LATE) // (N_LATE - 2))
    slots = [buf.at[i] for i in range(3) for buf in (upd_up, upd_down)]
    loads = [pltpu.make_async_copy(src, slot, load_sem.at[i]) for i, (src, slot) in enumerate(zip(news_in, slots))]
    stores = [pltpu.make_async_copy(slot, dst, store_sem.at[i]) for i, (slot, dst) in enumerate(zip(slots, news_out))]
    w_loads = [pltpu.make_async_copy(w_up_in, w_up, load_sem.at[6]), pltpu.make_async_copy(w_down_in, w_down, load_sem.at[7])]

    def place(k):
        return mixed(k, n_micro)[1]

    def load_micro(k):
        i = place(k)
        return pltpu.make_async_copy(outs_in.at[i], obuf.at[i], micro_load.at[i])

    def store_micro(k):
        i = place(k)
        return pltpu.make_async_copy(obuf.at[i], outs.at[i], micro_store.at[i])

    def load_late(n):
        return pltpu.make_async_copy(late_in.at[n], late.at[n], late_load.at[n])

    def start_micro(k):
        load_micro(k).start()

    def turn_micro(k):
        load_micro(k).wait()
        store_micro(k).start()

    def start_late(n):
        load_late(n).start()

    @pl.when(last)
    def _():
        for copy in w_loads:
            copy.start()
        repeat(0, N_LATE, start_late)
    for copy in loads:
        copy.start()
    repeat(0, n_copied, start_micro)

    @pl.when(last)
    def _():
        for copy in w_loads:
            copy.wait()

        def body(n):
            load_late(n).wait()
            k = n_micro - N_LATE + n
            stage_rows(late.at[n], w_up, w_down, obuf.at[place(k)])
            store_micro(k).start()

            @pl.when(n == 1)
            def _():
                for load, store in zip(loads, stores):
                    load.wait()
                    store.start()
            for j in range(per_late):
                k = per_late * (n - 2) + j

                @pl.when((k >= 0) & (k < n_micro - N_LATE))
                def _():
                    turn_micro(k)
        repeat(0, N_LATE, body)

    @pl.when(jnp.logical_not(last))
    def _():
        for load, store in zip(loads, stores):
            load.wait()
            store.start()
        repeat(0, n_micro, turn_micro)

    def stored(k):
        store_micro(k).wait()
    repeat(0, n_micro, stored)
    for copy in stores:
        copy.wait()


def finish_step(outs, late, w_up, w_down, *news):
    n_micro = outs.shape[0]
    hbm = pl.BlockSpec(memory_space=pl.ANY)
    vmem = pltpu.VMEM
    dma = pltpu.SemaphoreType.DMA
    return pl.pallas_call(
        finish_kernel,
        name="finish_step",
        out_shape=[jax.ShapeDtypeStruct(outs.shape, BF16)] + [jax.ShapeDtypeStruct(new.shape, F32) for new in news],
        in_specs=[hbm] * 10,
        out_specs=[hbm] * 7,
        scratch_shapes=[
            vmem(outs.shape, BF16), vmem(late.shape, BF16), vmem(w_up.shape, BF16), vmem(w_down.shape, BF16),
            vmem((3,) + news[0].shape, F32), vmem((3,) + news[1].shape, F32),
            dma((8,)), dma((6,)), dma((n_micro,)), dma((n_micro,)), dma((N_LATE,)),
        ],
        compiler_params=pltpu.CompilerParams(vmem_limit_bytes=56 * 1024 * 1024),
    )(outs, late, w_up, w_down, *news)


def solution(mesh):
    def local_step(master_up, master_down, mom1_up, mom1_down, mom2_up, mom2_down, grad_up, grad_down, stage_acts, loss_grad, next_batch, learn_rate, max_norm):
        stage_outs, *news, late, w_up, w_down = fused_step(
            master_up[0], master_down[0], mom1_up[0], mom1_down[0], mom2_up[0], mom2_down[0], grad_up[0, 0], grad_down[0, 0],
            stage_acts[0], loss_grad, next_batch, learn_rate.reshape(1), max_norm.reshape(1))
        stage_outs, new_up, new_down, new_m1_up, new_m1_down, new_m2_up, new_m2_down = finish_step(stage_outs, late, w_up, w_down, *news)
        return (new_up[None], new_down[None], new_m1_up[None], new_m1_down[None], new_m2_up[None], new_m2_down[None], stage_outs[None])

    w_spec = P('stage', None, None)
    g_spec = P('data', 'stage', None, None)
    in_specs = (w_spec, w_spec, w_spec, w_spec, w_spec, w_spec, g_spec, g_spec, P('stage', 'data', None), P('data', None), P(None, 'data', None), P(), P())
    out_specs = (w_spec, w_spec, w_spec, w_spec, w_spec, w_spec, P('stage', None, 'data', None))
    return jax.shard_map(local_step, mesh=mesh, in_specs=in_specs, out_specs=out_specs, check_vma=False)
```
